32 devices in a mesh: fsdp: 4 (over y, x), ctx: 4 (over z), tp: 2 (over core).
Axes of the slice: x: 2, y: 2, z: 4, core: 2. Of those that a mesh axis runs over, the one named last changes fastest.
Arguments:
- tokens: bfloat16 [4, 512, 2560], P('fsdp', 'ctx'), may hold values from -6 to 6
- segment_ids: int32 [4, 512], P('fsdp'), may hold values from 0 to 1, never falling along the last dimension, each value on 1 to 511 neighbouring positions
- w_query: bfloat16 [2560, 2560], P('fsdp', 'tp'), may hold values from -0.125 to 0.125
- w_keyval: bfloat16 [2560, 512], P('fsdp'), may hold values from -0.125 to 0.125
- w_out: bfloat16 [2560, 2560], P('tp', 'fsdp'), may hold values from -1 to 1
- w_gate: bfloat16 [2560, 7680], P('fsdp', 'tp'), may hold values from -0.125 to 0.125
- w_up: bfloat16 [2560, 7680], P('fsdp', 'tp'), may hold values from -0.125 to 0.125
- w_down: bfloat16 [7680, 2560], P('tp', 'fsdp'), may hold values from -0.0625 to 0.0625
- gain_attn: bfloat16 [2560], P('fsdp'), may hold values from 0.5 to 1.5
- gain_ffn: bfloat16 [2560], P('fsdp'), may hold values from 0.5 to 1.5
- cotangent: bfloat16 [4, 512, 2560], P('fsdp', 'ctx'), may hold values from -6 to 6
Outputs:
- out: bfloat16 [4, 512, 2560], P('fsdp', 'ctx')
- grad_tokens: float32 [4, 512, 2560], P('fsdp', 'ctx')
- grad_w_query: float32 [2560, 2560], P('fsdp', 'tp')
- grad_w_keyval: float32 [2560, 512], P('fsdp')
- grad_w_out: float32 [2560, 2560], P('tp', 'fsdp')
- grad_w_gate: float32 [2560, 7680], P('fsdp', 'tp')
- grad_w_up: float32 [2560, 7680], P('fsdp', 'tp')
- grad_w_down: float32 [7680, 2560], P('tp', 'fsdp')
- grad_gain_attn: float32 [2560], P('fsdp')
- grad_gain_ffn: float32 [2560], P('fsdp')
The draws below stay inside these ranges and needn't reach their ends.
Inputs may be any that keep to these rules, and one draw needn't show every extreme that they name: `segment_ids`: in each packed row the segment numbers never fall and start at 0; every number up to 1 is used; a segment has 1 to 511 tokens.
All inputs are finite; a program needn't handle non-finite values.
Results may differ from the reference program's by a relative error of at most 0.023.
Values may be sent and summed in bfloat16 or wider, within the bound.
A program may use at most 384 MiB of HBM per device.

```python
import math
import jax
import jax.numpy as jnp
import numpy as np
from jax import lax

D = 2560
HEADS = 10
HD = 256
FF = 7680
BATCH = 4
GROUP_TOK = 512
SEGS = 2
SEGMOST = 511


def steps_of(key, shape, shards, least, top_value):
    def one(axis_at, shards_of):
        steps = jax.random.uniform(jax.random.fold_in(jax.random.fold_in(key, 6), axis_at), (shards_of,), jnp.float32, least / len(shards), top_value / len(shards))
        return jnp.repeat(jnp.exp(steps), shape[axis_at] // shards_of).reshape((-1,) + (1,) * (len(shape) - axis_at - 1))

    level = one(*shards[0])
    for cut in shards[1:]:
        level = level * one(*cut)
    return level


def length_profile(count, total, bound, skew):
    loads = [(1 << 20) // math.isqrt(grade ** skew) + 1 for grade in range(2, count + 1)]
    surplus, counts = total - bound - (count - 1), [1] * (count - 1)
    while surplus > 0:
        free = [i for i in range(count - 1) if counts[i] < bound]
        pool, remaining = sum([loads[i] for i in free]), surplus
        for i in free:
            addition = min(bound - counts[i], max(1, remaining * loads[i] // pool), surplus)
            counts[i] = counts[i] + addition
            surplus = surplus - addition
    return np.array([bound] + counts)


def ragged(own_key, amount, total, limit, skew):
    if amount == 2:
        one = jax.random.randint(own_key, (), max(1, total - limit), min(limit, total - 1) + 1)
        return jnp.stack([one, total - one])
    lengths = jnp.asarray(length_profile(amount, total, limit, skew), jnp.int32)
    twos = (amount - 1) // 2
    giver, taker = lengths[1:1 + 2 * twos:2], lengths[2:2 + 2 * twos:2]
    margin = jnp.minimum(giver - 1, limit - taker)
    passed = jax.random.randint(jax.random.fold_in(own_key, 1), (twos,), 0, 1 << 20) % (margin + 1)
    lengths = lengths.at[1:1 + 2 * twos:2].set(giver - passed).at[2:2 + 2 * twos:2].set(taker + passed)
    return lengths[jax.random.permutation(jax.random.fold_in(own_key, 2), amount)]


def normal_values(stream_key, extent, scale, most, split=(), kind=jnp.bfloat16):
    values = scale * jax.random.normal(stream_key, extent, jnp.float32)
    if split:
        values = values * steps_of(stream_key, extent, split, -0.22, 0.18)
    return jnp.clip(values, -most, most).astype(kind)


def setup_inputs(seed: int = 0) -> dict:
    arg_keys = jax.random.split(jax.random.key(seed), 12)
    tokens = normal_values(arg_keys[0], (BATCH, GROUP_TOK, D), 1.0, 6.0, ((0, 4), (1, 4)))
    segment_ids = jax.vmap(lambda own: jnp.searchsorted(jnp.cumsum(ragged(own, SEGS, GROUP_TOK, SEGMOST, 2)), jnp.arange(GROUP_TOK), side="right"))(jax.random.split(arg_keys[1], BATCH)).reshape((BATCH, GROUP_TOK)).astype(jnp.int32)
    w_query = normal_values(arg_keys[2], (D, HEADS * HD), D ** -0.5, 0.125, ((0, 4), (1, 2)))
    w_keyval = normal_values(arg_keys[3], (D, 2 * HD), D ** -0.5, 0.125, ((0, 4),))
    w_out = normal_values(arg_keys[4], (HEADS * HD, D), (max(8, HEADS * HD // 80)) ** -0.5, 1.0, ((0, 2), (1, 4)))
    w_gate = normal_values(arg_keys[5], (D, FF), D ** -0.5, 0.125, ((0, 4), (1, 2)))
    w_up = normal_values(arg_keys[6], (D, FF), D ** -0.5, 0.125, ((0, 4), (1, 2)))
    w_down = normal_values(arg_keys[7], (FF, D), FF ** -0.5, 0.0625, ((0, 2), (1, 4)))
    gain_attn = jnp.clip(1.0 + 0.1 * jax.random.normal(arg_keys[8], (D,), jnp.float32), 0.5, 1.5).astype(jnp.bfloat16)
    gain_ffn = jnp.clip(1.0 + 0.1 * jax.random.normal(arg_keys[9], (D,), jnp.float32), 0.5, 1.5).astype(jnp.bfloat16)
    cotangent = normal_values(arg_keys[10], (BATCH, GROUP_TOK, D), 1.0, 6.0, ((0, 4), (1, 4)))
    return dict(tokens=tokens, segment_ids=segment_ids, w_query=w_query, w_keyval=w_keyval, w_out=w_out, w_gate=w_gate, w_up=w_up, w_down=w_down, gain_attn=gain_attn, gain_ffn=gain_ffn, cotangent=cotangent)


@jax.custom_vjp
def low(v):
    return lax.optimization_barrier(v.astype(jnp.bfloat16)).astype(jnp.float32)

@jax.custom_vjp
def low_back(v):
    return v

def low_keep(v):
    return (low(v), None)

def low_pass(kept, grad):
    return (grad,)

def back_keep(v):
    return (v, None)

def back_low(kept, grad):
    return (low(grad),)
low.defvjp(low_keep, low_pass)
low_back.defvjp(back_keep, back_low)

def rms_scale(value, gain):
    return value * lax.rsqrt(lax.optimization_barrier(jnp.mean(value * value, axis=-1, keepdims=True)) + 1e-06) * gain

def rotate(value, cosine, sine):
    quarter = value.shape[-1] // 4
    first = value[..., :quarter]
    second = value[..., quarter:2 * quarter]
    rest = value[..., 2 * quarter:]
    return jnp.concatenate([first * cosine - second * sine, second * cosine + first * sine, rest], axis=-1)

def matmul(left, right):
    return jnp.dot(left, right, precision=lax.Precision.HIGHEST, preferred_element_type=jnp.float32)

def row_forward(tokens_row, segment_row, weights):
    w_query, w_keyval, w_out, w_gate, w_up, w_down, gain_attn, gain_ffn = weights
    length = tokens_row.shape[0]
    index = jnp.arange(length, dtype=jnp.int32)
    change = jnp.concatenate([jnp.ones((1,), dtype=bool), segment_row[1:] != segment_row[:-1]])
    starts = lax.cummax(jnp.where(change, index, jnp.zeros_like(index)), axis=0)
    position = (index - starts).astype(jnp.float32)
    freqs = 10000.0 ** (-(jnp.arange(HD // 4, dtype=jnp.float32) * 2.0 / (HD // 2)))
    angle = position[:, None] * freqs[None, :]
    cosine = jnp.cos(angle)
    sine = jnp.sin(angle)
    normed = low(rms_scale(tokens_row, gain_attn))
    query = low_back(matmul(normed, w_query)).reshape(length, HEADS, HD)
    keyval = low_back(matmul(normed, w_keyval))
    query = low(rotate(query, cosine[:, None, :], sine[:, None, :]))
    keys = low(rotate(keyval[:, :HD], cosine, sine))
    values = low(keyval[:, HD:])
    block = min(512, length)
    count = length // block

    def attend(start):
        start = start.astype(jnp.int32)
        query_block = lax.dynamic_slice_in_dim(query, start, block, 0)
        query_index = start + jnp.arange(block, dtype=jnp.int32)
        query_segment = lax.dynamic_slice_in_dim(segment_row, start, block, 0)
        scores = jnp.einsum('qhd,kd->qhk', query_block, keys, precision=lax.Precision.HIGHEST) * HD ** (-0.5)
        mask = (query_segment[:, None] == segment_row[None, :]) & (index[None, :] <= query_index[:, None])
        scores = low_back(jnp.where(mask[:, None, :], scores, jnp.float32(-1e+30)))
        probs = jax.nn.softmax(scores, axis=-1)
        return jnp.einsum('qhk,kd->qhd', low(probs), values, precision=lax.Precision.HIGHEST)
    attended = lax.map(jax.checkpoint(attend), jnp.arange(count, dtype=jnp.int32) * block)
    attended = low_back(low(attended.reshape(length, HEADS * HD)))
    branch = low_back(matmul(attended, w_out))
    hidden_state = tokens_row + branch
    normed_ffn = low(rms_scale(hidden_state, gain_ffn))
    gate = low_back(matmul(normed_ffn, w_gate))
    upward = low_back(matmul(normed_ffn, w_up))
    hidden = low(jax.nn.gelu(gate, approximate=True) * upward)
    return hidden_state + matmul(hidden, w_down)

def reference(tokens, segment_ids, w_query, w_keyval, w_out, w_gate, w_up, w_down, gain_attn, gain_ffn, cotangent):

    def forward(tokens_f, wq_f, wkv_f, wo_f, wg_f, wu_f, wd_f, ga_f, gf_f):
        weights = (wq_f, wkv_f, wo_f, wg_f, wu_f, wd_f, ga_f, gf_f)

        def one_row(pair):
            return row_forward(pair[0], pair[1], weights)
        return lax.map(jax.checkpoint(one_row), (tokens_f, segment_ids))
    output, pullback = jax.vjp(forward, tokens.astype(jnp.float32), w_query.astype(jnp.float32), w_keyval.astype(jnp.float32), w_out.astype(jnp.float32), w_gate.astype(jnp.float32), w_up.astype(jnp.float32), w_down.astype(jnp.float32), gain_attn.astype(jnp.float32), gain_ffn.astype(jnp.float32))
    grads = pullback(cotangent.astype(jnp.float32))
    return (output.astype(jnp.bfloat16), grads[0], grads[1], grads[2], grads[3], grads[4], grads[5], grads[6], grads[7], grads[8])
```

```python
import jax
import jax.numpy as jnp
from jax import lax
from jax.sharding import PartitionSpec as P

HD = 256
NEGATIVE = -1e30
BF = jnp.bfloat16
F32 = jnp.float32


def rms_scale(value, gain):
    return value * lax.rsqrt(jnp.mean(value * value, axis=-1, keepdims=True) + 1e-06) * gain


def rotate(value, cosine, sine):
    quarter = value.shape[-1] // 4
    first = value[..., :quarter]
    second = value[..., quarter : 2 * quarter]
    rest = value[..., 2 * quarter :]
    return jnp.concatenate(
        [first * cosine - second * sine, second * cosine + first * sine, rest], axis=-1
    )


def unrotate(value, cosine, sine):
    return rotate(value, cosine, -sine)


def matmul(left, right):
    return jnp.dot(left, right, preferred_element_type=F32)


def times_transposed(left, right):
    return lax.dot_general(left, right, (((1,), (1,)), ((), ())), preferred_element_type=F32)


def transposed_times(left, right):
    return lax.dot_general(left, right, (((0,), (0,)), ((), ())), preferred_element_type=F32)


def geglu(gate_in, up_in):
    return jax.nn.gelu(gate_in, approximate=True) * up_in


def swap(value, axis, size, k):
    return lax.ppermute(value, axis, [(i, i ^ k) for i in range(size)])


def per_device(
    sizes,
    tokens,
    segment_ids,
    w_query,
    w_keyval,
    w_out,
    w_gate,
    w_up,
    w_down,
    gain_attn,
    gain_ffn,
    cotangent,
):
    nf, nc, nt = sizes
    fi, ci, ti = lax.axis_index("fsdp"), lax.axis_index("ctx"), lax.axis_index("tp")
    rows = tokens.shape[1]
    depth = tokens.shape[2]
    slab = depth // nf
    half = depth // nt
    heads = w_query.shape[1] // HD
    qcols = heads * HD
    units = w_gate.shape[1] // nc
    scale = HD ** (-0.5)

    def cut(value, start, size, axis):
        return lax.dynamic_slice_in_dim(value, start, size, axis)

    def all_to_all_blocks(blocks, axis, size):
        return [blocks[0]] + [swap(blocks[k], axis, size, k) for k in range(1, size)]

    def gather_blocks(value, axis, size):
        return [value] + [swap(value, axis, size, k) for k in range(1, size)]

    def absolute(blocks, index, axis):
        stacked = jnp.stack(blocks)
        size = len(blocks)
        return jnp.concatenate(
            [lax.dynamic_index_in_dim(stacked, j ^ index, 0, keepdims=False) for j in range(size)],
            axis=axis,
        )

    def rows_to_slabs(value):
        blocks = [cut(value, (fi ^ k) * slab, slab, 1) for k in range(nf)]
        return jnp.concatenate(all_to_all_blocks(blocks, "fsdp", nf), axis=0)

    def slabs_to_rows(value):
        blocks = list(value.reshape(nf, rows, slab))
        return absolute(all_to_all_blocks(blocks, "fsdp", nf), fi, 1)

    def reduce_rows(value, width):
        blocks = list(value.reshape(nf, rows, width))
        got = all_to_all_blocks(blocks, "fsdp", nf)
        return sum(block.astype(F32) for block in got)

    def gather_rows(value):
        return jnp.concatenate(gather_blocks(value, "fsdp", nf), axis=0)

    def both_halves(mine, axis):
        other = swap(mine, "tp", nt, 1)
        return jnp.where(
            ti == 0,
            jnp.concatenate([mine, other], axis=axis),
            jnp.concatenate([other, mine], axis=axis),
        )

    def tp_sum(value):
        low = value.astype(BF)
        return low.astype(F32) + swap(low, "tp", nt, 1).astype(F32)

    def gather_ctx(value):
        mine = cut(value, ti * half, half, 1)
        return both_halves(jnp.concatenate(gather_blocks(mine, "ctx", nc), axis=0), 1)

    def reduce_ctx(value):
        low = value.astype(BF)
        keep = cut(low, ti * half, half, 1)
        send = cut(low, (1 - ti) * half, half, 1)
        both = (keep.astype(F32) + swap(send, "tp", nt, 1).astype(F32)).astype(BF)
        got = all_to_all_blocks(list(both.reshape(nc, rows, half)), "ctx", nc)
        return sum(block.astype(F32) for block in got)

    gate_full = lax.all_gather(cut(w_gate, ci * units, units, 1), "fsdp", axis=0, tiled=True)
    up_full = lax.all_gather(cut(w_up, ci * units, units, 1), "fsdp", axis=0, tiled=True)
    down_full = lax.all_gather(
        cut(w_down, ci * units, units, 0).T, "fsdp", axis=0, tiled=True
    )

    gains = jnp.stack([gain_attn, gain_ffn])
    gains = absolute(gather_blocks(gains, "fsdp", nf), fi, 1).astype(F32)
    gain_one, gain_two = gains[0], gains[1]
    inputs = tokens[0].astype(F32)
    incoming = cotangent[0]

    segment_row = segment_ids[0]
    offset = ci * rows
    local_segment = lax.dynamic_slice_in_dim(segment_row, offset, rows, 0)
    local_index = offset + jnp.arange(rows, dtype=jnp.int32)
    earlier = jnp.sum((segment_row[None, :] < local_segment[:, None]).astype(jnp.int32), axis=1)
    position = (local_index - earlier).astype(F32)
    freqs = 10000.0 ** (-(jnp.arange(HD // 4, dtype=F32) * 2.0 / (HD // 2)))
    angle = position[:, None] * freqs[None, :]
    cosine = jnp.cos(angle)
    sine = jnp.sin(angle)

    normed_attn = rms_scale(inputs, gain_one).astype(BF)
    normed_slab = rows_to_slabs(normed_attn)
    kv_half = cut(w_keyval, ti * HD, HD, 1)
    partial = jnp.concatenate(
        [matmul(normed_slab, w_query).astype(BF), matmul(normed_slab, kv_half).astype(BF)], axis=1
    )
    projected = reduce_rows(partial, qcols + HD)
    query = projected[:, :qcols].reshape(rows, heads, HD)
    keyval = projected[:, qcols:]
    query_rows = (
        rotate(query, cosine[:, None, :], sine[:, None, :]).reshape(rows * heads, HD).astype(BF)
    )
    keyval = jnp.where(ti == 0, rotate(keyval, cosine, sine), keyval).astype(BF)
    kv_all = jnp.concatenate(gather_blocks(keyval, "ctx", nc), axis=0)
    kv_other = swap(kv_all, "tp", nt, 1)
    key_all = jnp.where(ti == 0, kv_all, kv_other)
    value_all = jnp.where(ti == 0, kv_other, kv_all)

    key_index = jnp.concatenate(
        [(ci ^ k) * rows + jnp.arange(rows, dtype=jnp.int32) for k in range(nc)]
    )
    key_segment = jnp.concatenate(
        [lax.dynamic_slice_in_dim(segment_row, (ci ^ k) * rows, rows, 0) for k in range(nc)]
    )
    row_index = jnp.repeat(local_index, heads)
    row_segment = jnp.repeat(local_segment, heads)
    mask = (row_segment[:, None] == key_segment[None, :]) & (
        key_index[None, :] <= row_index[:, None]
    )
    scores = jnp.where(mask, times_transposed(query_rows, key_all) * scale, NEGATIVE)
    peak = jnp.max(scores, axis=1, keepdims=True)
    terms = jnp.exp(scores - peak)
    probs = terms / jnp.sum(terms, axis=1, keepdims=True)
    probs_low = probs.astype(BF)
    attended = matmul(probs_low, value_all).reshape(rows, qcols).astype(BF)

    attended_plane = gather_rows(attended)
    branch = tp_sum(matmul(attended_plane, w_out)).astype(BF)
    hidden_state = inputs + slabs_to_rows(branch).astype(F32)
    normed_ffn = rms_scale(hidden_state, gain_two).astype(BF)

    normed_all = gather_ctx(normed_ffn)
    incoming_all = gather_ctx(incoming)
    gate = matmul(normed_all, gate_full)
    upward = matmul(normed_all, up_full)
    d_hidden = matmul(incoming_all, down_full)
    hidden, geglu_pull = jax.vjp(geglu, gate, upward)
    hidden = hidden.astype(BF)
    d_gate, d_up = geglu_pull(d_hidden)
    d_gate = d_gate.astype(BF)
    d_up = d_up.astype(BF)

    def finish(grad, axis):
        low = grad.astype(BF)
        blocks = [cut(low, (fi ^ k) * slab, slab, axis) for k in range(nf)]
        got = all_to_all_blocks(blocks, "fsdp", nf)
        return sum(block.astype(F32) for block in got).astype(BF)

    shard_down = finish(transposed_times(hidden, incoming_all), 1)
    grad_down = lax.all_gather(shard_down, "ctx", axis=0, tiled=True).astype(F32)
    shard_gate = finish(transposed_times(normed_all, d_gate), 0)
    grad_gate = lax.all_gather(shard_gate, "ctx", axis=0, tiled=False)
    shard_up = finish(transposed_times(normed_all, d_up), 0)
    grad_up = lax.all_gather(shard_up, "ctx", axis=0, tiled=False)

    def spread(value):
        return jnp.concatenate([value[j] for j in range(nc)], axis=1).astype(F32)

    grad_gate = spread(grad_gate)
    grad_up = spread(grad_up)

    d_normed_ffn = reduce_ctx(
        times_transposed(d_gate, gate_full) + times_transposed(d_up, up_full)
    ).astype(BF)
    d_normed_ffn = both_halves(d_normed_ffn, 1).astype(F32)
    feed = reduce_ctx(times_transposed(hidden, down_full))
    output = both_halves((cut(hidden_state, ti * half, half, 1) + feed).astype(BF), 1)

    unused, norm_pull = jax.vjp(rms_scale, hidden_state, gain_two)
    d_state_norm, grad_gain_two = norm_pull(d_normed_ffn)
    d_state = incoming.astype(F32) + d_state_norm
    d_branch_slab = rows_to_slabs(d_state.astype(BF))
    grad_out = transposed_times(attended_plane, d_branch_slab)
    d_attended = reduce_rows(times_transposed(d_branch_slab, w_out).astype(BF), qcols)
    d_attended = d_attended.astype(BF).reshape(rows * heads, HD)
    d_probs = times_transposed(d_attended, value_all)
    delta = jnp.sum(probs * d_probs, axis=1, keepdims=True)
    d_scores = (probs * (d_probs - delta)).astype(BF)
    d_rows = matmul(d_scores, key_all) * scale
    d_key = transposed_times(d_scores, query_rows) * scale
    d_value = transposed_times(probs_low, d_attended)
    d_key, d_value = d_key.astype(BF), d_value.astype(BF)
    keep = jnp.where(ti == 0, d_key, d_value)
    send = jnp.where(ti == 0, d_value, d_key)
    d_kv = (keep.astype(F32) + swap(send, "tp", nt, 1).astype(F32)).astype(BF)
    d_kv = sum(
        block.astype(F32)
        for block in all_to_all_blocks(list(d_kv.reshape(nc, rows, HD)), "ctx", nc)
    )
    d_kv = jnp.where(ti == 0, unrotate(d_kv, cosine, sine), d_kv).astype(BF)
    d_query = unrotate(d_rows.reshape(rows, heads, HD), cosine[:, None, :], sine[:, None, :])
    d_query = d_query.reshape(rows, qcols).astype(BF)
    d_plane = gather_rows(jnp.concatenate([d_query, d_kv], axis=1))
    d_query_plane = d_plane[:, :qcols]
    d_kv_plane = d_plane[:, qcols:]
    d_normed = tp_sum(
        times_transposed(d_query_plane, w_query) + times_transposed(d_kv_plane, kv_half)
    ).astype(BF)
    d_normed_attn = slabs_to_rows(d_normed).astype(F32)
    grad_query = transposed_times(normed_slab, d_query_plane)
    grad_kv = transposed_times(normed_slab, d_kv_plane)
    unused, norm_pull_one = jax.vjp(rms_scale, inputs, gain_one)
    d_input_norm, grad_gain_one = norm_pull_one(d_normed_attn)
    grad_inputs = d_state + d_input_norm

    grad_out = lax.psum(grad_out.astype(BF), "ctx").astype(F32)
    grad_query = lax.psum(grad_query.astype(BF), "ctx").astype(F32)
    grad_kv = lax.psum(grad_kv.astype(BF), "ctx")
    grad_kv = both_halves(grad_kv, 1).astype(F32)
    gain_grads = jnp.stack([grad_gain_one, grad_gain_two])
    gain_blocks = [cut(gain_grads, (fi ^ k) * slab, slab, 1) for k in range(nf)]
    gain_grads = sum(all_to_all_blocks(gain_blocks, "fsdp", nf))
    step = 1
    while step < nc:
        gain_grads = gain_grads + swap(gain_grads, "ctx", nc, step)
        step *= 2
    return (
        output[None],
        grad_inputs[None],
        grad_query,
        grad_kv,
        grad_out,
        grad_gate,
        grad_up,
        grad_down,
        gain_grads[0],
        gain_grads[1],
    )


def solution(mesh):
    sizes = (mesh.shape["fsdp"], mesh.shape["ctx"], mesh.shape["tp"])
    in_specs = (
        P("fsdp", "ctx", None),
        P("fsdp", None),
        P("fsdp", "tp"),
        P("fsdp", None),
        P("tp", "fsdp"),
        P("fsdp", "tp"),
        P("fsdp", "tp"),
        P("tp", "fsdp"),
        P("fsdp"),
        P("fsdp"),
        P("fsdp", "ctx", None),
    )
    out_specs = (
        P("fsdp", "ctx", None),
        P("fsdp", "ctx", None),
        P("fsdp", "tp"),
        P("fsdp", None),
        P("tp", "fsdp"),
        P("fsdp", "tp"),
        P("fsdp", "tp"),
        P("tp", "fsdp"),
        P("fsdp"),
        P("fsdp"),
    )

    def body(*args):
        return per_device(sizes, *args)

    return jax.shard_map(
        body, mesh=mesh, in_specs=in_specs, out_specs=out_specs, check_vma=False
    )
```

```python
import functools

import jax
import jax.numpy as jnp
from jax import lax
from jax.experimental import pallas as pl
from jax.experimental.pallas import tpu as pltpu
from jax.sharding import PartitionSpec as P


HD = 256
NEGATIVE = -1e30
BF = jnp.bfloat16
F32 = jnp.float32
MESH = pl.DeviceIdType.MESH


def rms_scale(value, gain):
    return value * lax.rsqrt(jnp.mean(value * value, axis=-1, keepdims=True) + 1e-06) * gain


def rotate(value, cosine, sine):
    quarter = value.shape[-1] // 4
    first = value[..., :quarter]
    second = value[..., quarter : 2 * quarter]
    rest = value[..., 2 * quarter :]
    return jnp.concatenate(
        [first * cosine - second * sine, second * cosine + first * sine, rest], axis=-1
    )


def unrotate(value, cosine, sine):
    return rotate(value, cosine, -sine)


def matmul(left, right):
    return jnp.dot(left, right, preferred_element_type=F32)


def times_transposed(left, right):
    return lax.dot_general(left, right, (((1,), (1,)), ((), ())), preferred_element_type=F32)


def transposed_times(left, right):
    return lax.dot_general(left, right, (((0,), (0,)), ((), ())), preferred_element_type=F32)


def geglu(gate_in, up_in):
    return jax.nn.gelu(gate_in, approximate=True) * up_in


def swap(value, axis, size, k):
    return lax.ppermute(value, axis, [(i, i ^ k) for i in range(size)])


def per_device(
    sizes,
    tokens,
    segment_ids,
    w_query,
    w_keyval,
    w_out,
    w_gate,
    w_up,
    w_down,
    gain_attn,
    gain_ffn,
    cotangent,
):
    nf, nc, nt = sizes
    fi, ci, ti = lax.axis_index("fsdp"), lax.axis_index("ctx"), lax.axis_index("tp")
    rows = tokens.shape[1]
    depth = tokens.shape[2]
    slab = depth // nf
    half = depth // nt
    heads = w_query.shape[1] // HD
    qcols = heads * HD
    units = w_gate.shape[1] // nc
    scale = HD ** (-0.5)

    def cut(value, start, size, axis):
        return lax.dynamic_slice_in_dim(value, start, size, axis)

    def all_to_all_blocks(blocks, axis, size):
        return [blocks[0]] + [swap(blocks[k], axis, size, k) for k in range(1, size)]

    def gather_blocks(value, axis, size):
        return [value] + [swap(value, axis, size, k) for k in range(1, size)]

    def absolute(blocks, index, axis):
        stacked = jnp.stack(blocks)
        size = len(blocks)
        return jnp.concatenate(
            [lax.dynamic_index_in_dim(stacked, j ^ index, 0, keepdims=False) for j in range(size)],
            axis=axis,
        )

    def rows_to_slabs(value):
        blocks = [cut(value, (fi ^ k) * slab, slab, 1) for k in range(nf)]
        return jnp.concatenate(all_to_all_blocks(blocks, "fsdp", nf), axis=0)

    def slabs_to_rows(value):
        blocks = list(value.reshape(nf, rows, slab))
        return absolute(all_to_all_blocks(blocks, "fsdp", nf), fi, 1)

    def reduce_rows(value, width):
        blocks = list(value.reshape(nf, rows, width))
        got = all_to_all_blocks(blocks, "fsdp", nf)
        return sum(block.astype(F32) for block in got)

    def gather_rows(value):
        return jnp.concatenate(gather_blocks(value, "fsdp", nf), axis=0)

    def both_halves(mine, axis):
        other = swap(mine, "tp", nt, 1)
        return jnp.where(
            ti == 0,
            jnp.concatenate([mine, other], axis=axis),
            jnp.concatenate([other, mine], axis=axis),
        )

    def tp_sum(value):
        low = value.astype(BF)
        return low.astype(F32) + swap(low, "tp", nt, 1).astype(F32)

    def gather_ctx(value):
        mine = cut(value, ti * half, half, 1)
        return both_halves(jnp.concatenate(gather_blocks(mine, "ctx", nc), axis=0), 1)

    def reduce_ctx(value):
        low = value.astype(BF)
        keep = cut(low, ti * half, half, 1)
        send = cut(low, (1 - ti) * half, half, 1)
        both = (keep.astype(F32) + swap(send, "tp", nt, 1).astype(F32)).astype(BF)
        got = all_to_all_blocks(list(both.reshape(nc, rows, half)), "ctx", nc)
        return sum(block.astype(F32) for block in got)

    gate_full = lax.all_gather(cut(w_gate, ci * units, units, 1), "fsdp", axis=0, tiled=True)
    up_full = lax.all_gather(cut(w_up, ci * units, units, 1), "fsdp", axis=0, tiled=True)
    down_full = lax.all_gather(
        cut(w_down, ci * units, units, 0).T, "fsdp", axis=0, tiled=True
    )

    gains = jnp.stack([gain_attn, gain_ffn])
    gains = absolute(gather_blocks(gains, "fsdp", nf), fi, 1).astype(F32)
    gain_one, gain_two = gains[0], gains[1]
    inputs = tokens[0].astype(F32)
    incoming = cotangent[0]

    segment_row = segment_ids[0]
    offset = ci * rows
    local_segment = lax.dynamic_slice_in_dim(segment_row, offset, rows, 0)
    local_index = offset + jnp.arange(rows, dtype=jnp.int32)
    earlier = jnp.sum((segment_row[None, :] < local_segment[:, None]).astype(jnp.int32), axis=1)
    position = (local_index - earlier).astype(F32)
    freqs = 10000.0 ** (-(jnp.arange(HD // 4, dtype=F32) * 2.0 / (HD // 2)))
    angle = position[:, None] * freqs[None, :]
    cosine = jnp.cos(angle)
    sine = jnp.sin(angle)

    normed_attn = rms_scale(inputs, gain_one).astype(BF)
    normed_slab = rows_to_slabs(normed_attn)
    kv_half = cut(w_keyval, ti * HD, HD, 1)
    partial = jnp.concatenate(
        [matmul(normed_slab, w_query).astype(BF), matmul(normed_slab, kv_half).astype(BF)], axis=1
    )
    projected = reduce_rows(partial, qcols + HD)
    query = projected[:, :qcols].reshape(rows, heads, HD)
    keyval = projected[:, qcols:]
    query_rows = (
        rotate(query, cosine[:, None, :], sine[:, None, :]).reshape(rows * heads, HD).astype(BF)
    )
    keyval = jnp.where(ti == 0, rotate(keyval, cosine, sine), keyval).astype(BF)
    kv_all = jnp.concatenate(gather_blocks(keyval, "ctx", nc), axis=0)
    kv_other = swap(kv_all, "tp", nt, 1)
    key_all = jnp.where(ti == 0, kv_all, kv_other)
    value_all = jnp.where(ti == 0, kv_other, kv_all)

    key_index = jnp.concatenate(
        [(ci ^ k) * rows + jnp.arange(rows, dtype=jnp.int32) for k in range(nc)]
    )
    key_segment = jnp.concatenate(
        [lax.dynamic_slice_in_dim(segment_row, (ci ^ k) * rows, rows, 0) for k in range(nc)]
    )
    row_index = jnp.repeat(local_index, heads)
    row_segment = jnp.repeat(local_segment, heads)
    mask = (row_segment[:, None] == key_segment[None, :]) & (
        key_index[None, :] <= row_index[:, None]
    )
    scores = jnp.where(mask, times_transposed(query_rows, key_all) * scale, NEGATIVE)
    peak = jnp.max(scores, axis=1, keepdims=True)
    terms = jnp.exp(scores - peak)
    probs = terms / jnp.sum(terms, axis=1, keepdims=True)
    probs_low = probs.astype(BF)
    attended = matmul(probs_low, value_all).reshape(rows, qcols).astype(BF)

    attended_plane = gather_rows(attended)
    branch = tp_sum(matmul(attended_plane, w_out)).astype(BF)
    hidden_state = inputs + slabs_to_rows(branch).astype(F32)
    normed_ffn = rms_scale(hidden_state, gain_two).astype(BF)

    normed_all = gather_ctx(normed_ffn)
    incoming_all = gather_ctx(incoming)
    gate = matmul(normed_all, gate_full)
    upward = matmul(normed_all, up_full)
    d_hidden = matmul(incoming_all, down_full)
    hidden, geglu_pull = jax.vjp(geglu, gate, upward)
    hidden = hidden.astype(BF)
    d_gate, d_up = geglu_pull(d_hidden)
    d_gate = d_gate.astype(BF)
    d_up = d_up.astype(BF)

    def finish(grad, axis):
        low = grad.astype(BF)
        blocks = [cut(low, (fi ^ k) * slab, slab, axis) for k in range(nf)]
        got = all_to_all_blocks(blocks, "fsdp", nf)
        return sum(block.astype(F32) for block in got).astype(BF)

    shard_down = finish(transposed_times(hidden, incoming_all), 1)
    grad_down = lax.all_gather(shard_down, "ctx", axis=0, tiled=True).astype(F32)
    shard_gate = finish(transposed_times(normed_all, d_gate), 0)
    grad_gate = lax.all_gather(shard_gate, "ctx", axis=0, tiled=False)
    shard_up = finish(transposed_times(normed_all, d_up), 0)
    grad_up = lax.all_gather(shard_up, "ctx", axis=0, tiled=False)

    def spread(value):
        return jnp.concatenate([value[j] for j in range(nc)], axis=1).astype(F32)

    grad_gate = spread(grad_gate)
    grad_up = spread(grad_up)

    d_normed_ffn = reduce_ctx(
        times_transposed(d_gate, gate_full) + times_transposed(d_up, up_full)
    ).astype(BF)
    d_normed_ffn = both_halves(d_normed_ffn, 1).astype(F32)
    feed = reduce_ctx(times_transposed(hidden, down_full))
    output = both_halves((cut(hidden_state, ti * half, half, 1) + feed).astype(BF), 1)

    unused, norm_pull = jax.vjp(rms_scale, hidden_state, gain_two)
    d_state_norm, grad_gain_two = norm_pull(d_normed_ffn)
    d_state = incoming.astype(F32) + d_state_norm
    d_branch_slab = rows_to_slabs(d_state.astype(BF))
    grad_out = transposed_times(attended_plane, d_branch_slab)
    d_attended = reduce_rows(times_transposed(d_branch_slab, w_out).astype(BF), qcols)
    d_attended = d_attended.astype(BF).reshape(rows * heads, HD)
    d_probs = times_transposed(d_attended, value_all)
    delta = jnp.sum(probs * d_probs, axis=1, keepdims=True)
    d_scores = (probs * (d_probs - delta)).astype(BF)
    d_rows = matmul(d_scores, key_all) * scale
    d_key = transposed_times(d_scores, query_rows) * scale
    d_value = transposed_times(probs_low, d_attended)
    d_key, d_value = d_key.astype(BF), d_value.astype(BF)
    keep = jnp.where(ti == 0, d_key, d_value)
    send = jnp.where(ti == 0, d_value, d_key)
    d_kv = (keep.astype(F32) + swap(send, "tp", nt, 1).astype(F32)).astype(BF)
    d_kv = sum(
        block.astype(F32)
        for block in all_to_all_blocks(list(d_kv.reshape(nc, rows, HD)), "ctx", nc)
    )
    d_kv = jnp.where(ti == 0, unrotate(d_kv, cosine, sine), d_kv).astype(BF)
    d_query = unrotate(d_rows.reshape(rows, heads, HD), cosine[:, None, :], sine[:, None, :])
    d_query = d_query.reshape(rows, qcols).astype(BF)
    d_plane = gather_rows(jnp.concatenate([d_query, d_kv], axis=1))
    d_query_plane = d_plane[:, :qcols]
    d_kv_plane = d_plane[:, qcols:]
    d_normed = tp_sum(
        times_transposed(d_query_plane, w_query) + times_transposed(d_kv_plane, kv_half)
    ).astype(BF)
    d_normed_attn = slabs_to_rows(d_normed).astype(F32)
    grad_query = transposed_times(normed_slab, d_query_plane)
    grad_kv = transposed_times(normed_slab, d_kv_plane)
    unused, norm_pull_one = jax.vjp(rms_scale, inputs, gain_one)
    d_input_norm, grad_gain_one = norm_pull_one(d_normed_attn)
    grad_inputs = d_state + d_input_norm

    grad_out = lax.psum(grad_out.astype(BF), "ctx").astype(F32)
    grad_query = lax.psum(grad_query.astype(BF), "ctx").astype(F32)
    grad_kv = lax.psum(grad_kv.astype(BF), "ctx")
    grad_kv = both_halves(grad_kv, 1).astype(F32)
    gain_grads = jnp.stack([grad_gain_one, grad_gain_two])
    gain_blocks = [cut(gain_grads, (fi ^ k) * slab, slab, 1) for k in range(nf)]
    gain_grads = sum(all_to_all_blocks(gain_blocks, "fsdp", nf))
    step = 1
    while step < nc:
        gain_grads = gain_grads + swap(gain_grads, "ctx", nc, step)
        step *= 2
    return (
        output[None],
        grad_inputs[None],
        grad_query,
        grad_kv,
        grad_out,
        grad_gate,
        grad_up,
        grad_down,
        gain_grads[0],
        gain_grads[1],
    )


def partners(axis, size):
    me = lax.axis_index(axis)
    flip = me + 1 - 2 * lax.rem(me, 2)
    return [me, flip, lax.rem(me + 2, size), size - 1 - me]


class Wire:
    def __init__(self, send, recv):
        self.send, self.recv, self.count, self.live = send, recv, 0, []

    def __call__(self, src, dst, axis, peer):
        slot = self.count
        self.count += 1
        copy = pltpu.make_async_remote_copy(
            src_ref=src,
            dst_ref=dst,
            send_sem=self.send.at[slot],
            recv_sem=self.recv.at[slot],
            device_id={axis: peer},
            device_id_type=MESH,
        )
        copy.start()
        self.live.append(copy)
        return copy

    def settle(self, copies):
        for copy in copies:
            copy.wait_send()
            self.live = [each for each in self.live if each is not copy]

    def finish(self):
        for copy in self.live:
            copy.wait_send()


def greet(peers):
    barrier = pltpu.get_barrier_semaphore()
    for axis, peer in peers:
        pl.semaphore_signal(barrier, inc=1, device_id={axis: peer}, device_id_type=MESH)
    pl.semaphore_wait(barrier, len(peers))


def wide(value, columns):
    return jnp.concatenate([value] * (columns // value.shape[1]), axis=1)


def nt_dot(left, right):
    return lax.dot_general(left, right, (((1,), (1,)), ((), ())), preferred_element_type=F32)


def tn_dot(left, right):
    return lax.dot_general(left, right, (((0,), (0,)), ((), ())), preferred_element_type=F32)


class Gather:
    def __init__(self, wire, fs, pieces, height, place, own=None):
        self.wire, self.fs, self.pieces, self.height = wire, fs, pieces, height
        self.place, self.own = place, own
        self.arrivals = {}

    def strip(self, p):
        return pl.ds(p * self.height, self.height)

    def send(self, m, p, k):
        target = self.place(m, self.fs[0], self.strip(p))
        source = self.own.at[self.strip(p), :] if self.own is not None else target
        self.arrivals[m, p, k] = self.wire(source, target, "fsdp", self.fs[k])

    def pass_on(self, m, p, k, to):
        self.arrivals.pop((m, p, k)).wait_recv()
        target = self.place(m, self.fs[k], self.strip(p))
        self.arrivals[m, p, 3] = self.wire(target, target, "fsdp", self.fs[to])

    def steps(self, which, prepare):
        half = self.pieces // 2
        for m in which:
            prepare(m)
            for i in range(half):
                self.send(m, i, 1)
                self.send(m, half + i, 2)
                yield
            for i in range(half):
                self.pass_on(m, half + i, 2, 1)
                self.pass_on(m, i, 1, 2)
                yield
            for i in range(half):
                self.send(m, half + i, 1)
                self.send(m, i, 2)
                yield

    def settle(self):
        for copy in self.arrivals.values():
            copy.wait_recv()


def gather_kernel(w_down, after, down_full, down_rows, own, send, recv, local):
    del after
    fs = partners("fsdp", 4)
    ci = lax.axis_index("ctx")
    units, slab = down_rows.shape
    load = pltpu.make_async_copy(
        w_down.at[pl.ds(pl.multiple_of(ci * units, 64), units), :], down_rows, local.at[0]
    )
    load.start()
    greet([("fsdp", fs[1]), ("fsdp", fs[2])])
    wire = Wire(send, recv)
    gather = Gather(
        wire, fs, 8, slab // 8, lambda m, index, at: down_full.at[index, at, :], own=own
    )
    keep = pltpu.make_async_copy(own, down_full.at[fs[0]], local.at[1])

    def prepare(m):
        load.wait()
        own[...] = down_rows[...].T
        keep.start()

    for _ in gather.steps((0,), prepare):
        pass
    gather.settle()
    keep.wait()
    wire.finish()


def call_gather(w_down, after):
    units, slab = w_down.shape[0] // 4, w_down.shape[1]
    hbm = pl.BlockSpec(memory_space=pl.ANY)
    return pl.pallas_call(
        gather_kernel,
        out_shape=jax.ShapeDtypeStruct((4, slab, units), BF),
        in_specs=[hbm] * 2,
        out_specs=hbm,
        scratch_shapes=[
            pltpu.VMEM((units, slab), BF),
            pltpu.VMEM((slab, units), BF),
            pltpu.SemaphoreType.DMA((24,)),
            pltpu.SemaphoreType.DMA((24,)),
            pltpu.SemaphoreType.DMA((2,)),
        ],
        compiler_params=pltpu.CompilerParams(collective_id=2, has_side_effects=True),
        cost_estimate=pl.CostEstimate(flops=0, bytes_accessed=120_000_000, transcendentals=0),
        name="gather_down",
    )(w_down, after)


def forward_kernel(
    heads,
    tok,
    cot,
    gains,
    cos,
    sin,
    keep,
    w_q,
    w_kv,
    w_o,
    w_gate,
    w_up,
    q_rot,
    kv_out,
    probs,
    state,
    gains_all,
    normed_all,
    cot_all,
    gate_full,
    up_full,
    normed_slab,
    att_plane,
    gate,
    upward,
    hidden,
    shard,
    xbuf,
    rbuf,
    part,
    precv,
    kvbuf,
    attbuf,
    obuf,
    orecv,
    bbuf,
    brecv,
    nown,
    grel,
    window,
    wfull,
    nall,
    call,
    parts,
    near,
    far,
    sums,
    send,
    recv,
    local,
):
    fs, cs = partners("fsdp", 4), partners("ctx", 4)
    ci, ti = lax.axis_index("ctx"), lax.axis_index("tp")
    other = 1 - ti
    rows, depth = tok.shape
    slab = depth // 4
    hrows = rows // 2
    qcols = heads * HD
    units = gate_full.shape[2]
    scale = HD ** (-0.5)
    wire = Wire(send, recv)
    locals_ = []

    def keep_local(src, dst):
        copy = pltpu.make_async_copy(src, dst, local.at[len(locals_)])
        copy.start()
        locals_.append(copy)
        return copy

    def lanes(index):
        return pl.ds(pl.multiple_of(index * slab, slab), slab)

    mine = pl.ds(pl.multiple_of(ti * hrows, hrows), hrows)
    first = pl.ds(pl.multiple_of(((ci * units) // 128) * 128, 128), window.shape[2])
    win = [
        keep_local(w_gate.at[:, first], window.at[0]),
        keep_local(w_up.at[:, first], window.at[1]),
    ]
    greet(
        [("fsdp", fs[k]) for k in (1, 2, 3)]
        + [("ctx", cs[k]) for k in (1, 2, 3)]
        + [("tp", other)]
    )

    x_in = [None] * 4
    for k in (1, 2, 3):
        x_in[k] = wire(tok.at[:, lanes(fs[k])], xbuf.at[k], "fsdp", fs[k])
    g_in = [None] * 4
    for k in (1, 2, 3):
        g_in[k] = wire(gains, grel.at[k], "fsdp", fs[k])
    grel[0] = gains[...]
    xbuf[0] = tok[:, lanes(fs[0])]
    x = tok[...].astype(F32)
    r = lax.rsqrt(jnp.sum(x * x, axis=1, keepdims=True) * (1.0 / depth) + 1e-06)
    rbuf[0] = jnp.broadcast_to(r, (rows, 128))
    r_in = [None] * 4
    for k in (1, 2, 3):
        r_in[k] = wire(rbuf.at[0], rbuf.at[k], "fsdp", fs[k])
    c_in = [None] * 4
    for k in (1, 2, 3):
        c_in[k] = wire(cot.at[mine, :], call.at[ci, ti], "ctx", cs[k])
    for half in (0, 1):
        call[ci, half] = cot[half * hrows : (half + 1) * hrows, :]

    odd = units % 128
    pieces = 8
    height = slab // pieces

    def prepare(m):
        win[m].wait()
        if odd:

            @pl.when(lax.rem(ci, 2) == 0)
            def _():
                wfull[m, fs[0]] = window[m, :, 0:units]

            @pl.when(lax.rem(ci, 2) == 1)
            def _():
                wfull[m, fs[0]] = window[m, :, odd : odd + units]
        else:
            wfull[m, fs[0]] = window[m, :, 0:units]

    gather = Gather(wire, fs, pieces, height, lambda m, index, at: wfull.at[m, index, at, :])
    schedule = gather.steps((0, 1), prepare)

    def bulk(count):
        for _ in range(count):
            next(schedule, None)

    bulk(BULK[0])
    gain_one = gains[0:1, :]
    kv_half = w_kv[:, pl.ds(pl.multiple_of(ti * HD, HD), HD)]
    p_in = [None] * 4
    for k in range(4):
        if k:
            x_in[k].wait_recv()
            r_in[k].wait_recv()
        normed = (xbuf[k].astype(F32) * wide(rbuf[k], slab) * gain_one).astype(BF)
        normed_slab[k] = normed
        part[k, :, 0:qcols] = jnp.dot(normed, w_q[...], preferred_element_type=F32).astype(BF)
        part[k, :, qcols:] = jnp.dot(normed, kv_half, preferred_element_type=F32).astype(BF)
        if k:
            p_in[k] = wire(part.at[k], precv.at[k], "fsdp", fs[k])
    bulk(BULK[1])
    for k in (1, 2, 3):
        p_in[k].wait_recv()

    def total(start, size):
        out = part[0, :, start : start + size].astype(F32)
        for k in (1, 2, 3):
            out += precv[k, :, start : start + size].astype(F32)
        return out

    c, s = cos[...], sin[...]
    zero = (1 - ti).astype(F32)
    kvbuf[ti, 0] = turn(total(qcols, HD), c * zero + (1.0 - zero), s * zero).astype(BF)
    kv_in = [None] * 4
    for k in (1, 2, 3):
        kv_in[k] = wire(kvbuf.at[ti, 0], kvbuf.at[ti, k], "ctx", cs[k])
    kv_side = [wire(kvbuf.at[ti, 0], kvbuf.at[ti, 0], "tp", other)]
    for h in range(heads):
        q_rot[:, h * HD : (h + 1) * HD] = turn(total(h * HD, HD), c, s).astype(BF)
    bulk(BULK[2])
    for k in (1, 2, 3):
        kv_in[k].wait_recv()
        kv_side.append(wire(kvbuf.at[ti, k], kvbuf.at[ti, k], "tp", other))
    for copy in kv_side:
        copy.wait_recv()
    length = 4 * rows
    keys = kvbuf[0].reshape(length, HD)
    values = kvbuf[1].reshape(length, HD)
    kv_out[...] = kvbuf[...]
    seen = keep[...] > 0.5
    for h in range(heads):
        sc = nt_dot(q_rot[:, h * HD : (h + 1) * HD], keys) * scale
        sc = jnp.where(seen, sc, NEGATIVE)
        e = jnp.exp(sc - jnp.max(sc, axis=1, keepdims=True))
        p = e / jnp.sum(e, axis=1, keepdims=True)
        probs[h] = p
        attbuf[0, :, h * HD : (h + 1) * HD] = jnp.dot(
            p.astype(BF), values, preferred_element_type=F32
        ).astype(BF)
    a_in = [None] * 4
    for k in (1, 2, 3):
        a_in[k] = wire(attbuf.at[0], attbuf.at[k], "fsdp", fs[k])
    bulk(BULK[3])
    c_side = []
    for k in (1, 2, 3):
        c_in[k].wait_recv()
        c_side.append(wire(call.at[cs[k], ti], call.at[cs[k], ti], "tp", other))
    o_in = []
    for k in range(4):
        if k:
            a_in[k].wait_recv()
        att_plane[k] = attbuf[k]
        block = jnp.dot(attbuf[k], w_o[...], preferred_element_type=F32).astype(BF)
        obuf[k, 0] = block[0:hrows]
        obuf[k, 1] = block[hrows:rows]
        o_in.append(wire(obuf.at[k, other], orecv.at[k], "tp", other))
    b_in = [None] * 4
    for k in (1, 2, 3, 0):
        o_in[k].wait_recv()
        both = (obuf[k, ti].astype(F32) + orecv[k].astype(F32)).astype(BF)
        if k:
            bbuf[k] = both
            b_in[k] = wire(bbuf.at[k], brecv.at[k], "fsdp", fs[k])
        else:
            brecv[0] = both
    bulk(BULK[4])
    for k in (1, 2, 3):
        g_in[k].wait_recv()
    gains_all[...] = grel[...]
    squares = jnp.zeros((hrows, 1), F32)
    for k in range(4):
        if k:
            b_in[k].wait_recv()
        h_new = tok[mine, lanes(fs[k])].astype(F32) + brecv[k].astype(F32)
        state[:, lanes(fs[k])] = h_new
        squares += jnp.sum(h_new * h_new, axis=1, keepdims=True)
    r2 = lax.rsqrt(squares * (1.0 / depth) + 1e-06)
    for k in range(4):
        nown[:, lanes(fs[k])] = (state[:, lanes(fs[k])] * r2 * grel[k, 1:2, :]).astype(BF)
    n_in = [None] * 4
    for k in (1, 2, 3):
        n_in[k] = wire(nown, nall.at[ci, ti], "ctx", cs[k])
    n_side = [wire(nown, nall.at[ci, ti], "tp", other)]
    nall[ci, ti] = nown[...]
    bulk(BULK[5])
    for k in (1, 2, 3):
        n_in[k].wait_recv()
        n_side.append(wire(nall.at[cs[k], ti], nall.at[cs[k], ti], "tp", other))
        bulk(BULK[6])
    bulk(1000)
    gather.settle()
    keep_local(wfull.at[0], gate_full)
    keep_local(wfull.at[1], up_full)
    for k in range(4):
        n_side[k].wait_recv()
        x = nall[cs[k]].reshape(rows, depth)
        at = pl.ds(pl.multiple_of(cs[k] * rows, rows), rows)
        g = jnp.dot(x, wfull[0].reshape(depth, units), preferred_element_type=F32)
        u = jnp.dot(x, wfull[1].reshape(depth, units), preferred_element_type=F32)
        gate[at, :] = g
        upward[at, :] = u
        cdf = 0.5 * (1.0 + jnp.tanh(0.7978845608028654 * (g + 0.044715 * (g * g * g))))
        hidden[at, :] = (g * cdf * u).astype(BF)
    keep_local(nall, normed_all)
    for copy in c_side:
        copy.wait_recv()
    keep_local(call, cot_all)
    product = Product(wire, True, hidden, call, shard, parts, near, far, sums)
    product.start()
    product.middle()
    product.end()
    for copy in locals_[2:]:
        copy.wait()
    wire.finish()


BULK = (3, 4, 3, 3, 3, 6, 1)


def call_forward(heads, tok, cot, gains, cos, sin, keep, w_q, w_kv, w_o, w_gate, w_up):
    rows, depth = tok.shape
    slab, hrows, qcols, length = depth // 4, rows // 2, heads * HD, 4 * rows
    units = w_gate.shape[1] // 4
    reach = -(-(units + units % 128) // 128) * 128
    shape = jax.ShapeDtypeStruct
    vmem = pl.BlockSpec(memory_space=pltpu.VMEM)
    hbm = pl.BlockSpec(memory_space=pl.ANY)
    pcols = qcols + HD
    sizes = product_sizes(True, slab, units)
    pair = [pltpu.VMEM((2, *size), BF) for size in sizes]
    single = [pltpu.VMEM(size, BF) for size in sizes]
    return pl.pallas_call(
        functools.partial(forward_kernel, heads),
        out_shape=[
            shape((rows, qcols), BF),
            shape((2, 4, rows, HD), BF),
            shape((heads, rows, length), F32),
            shape((hrows, depth), F32),
            shape((4, 8, slab), F32),
            shape((4, 2, hrows, depth), BF),
            shape((4, 2, hrows, depth), BF),
            shape((4, slab, units), BF),
            shape((4, slab, units), BF),
            shape((4, rows, slab), BF),
            shape((4, rows, qcols), BF),
            shape((length, units), F32),
            shape((length, units), F32),
            shape((length, units), BF),
            shape((units, slab), BF),
        ],
        in_specs=[vmem] * 9 + [hbm] * 2,
        out_specs=[vmem] * 5 + [hbm] * 4 + [vmem] * 6,
        scratch_shapes=[
            pltpu.VMEM((4, rows, slab), BF),
            pltpu.VMEM((4, rows, 128), F32),
            pltpu.VMEM((4, rows, pcols), BF),
            pltpu.VMEM((4, rows, pcols), BF),
            pltpu.VMEM((2, 4, rows, HD), BF),
            pltpu.VMEM((4, rows, qcols), BF),
            pltpu.VMEM((4, 2, hrows, slab), BF),
            pltpu.VMEM((4, hrows, slab), BF),
            pltpu.VMEM((4, hrows, slab), BF),
            pltpu.VMEM((4, hrows, slab), BF),
            pltpu.VMEM((hrows, depth), BF),
            pltpu.VMEM((4, 8, slab), F32),
            pltpu.VMEM((2, slab, reach), BF),
            pltpu.VMEM((2, 4, slab, units), BF),
            pltpu.VMEM((4, 2, hrows, depth), BF),
            pltpu.VMEM((4, 2, hrows, depth), BF),
            list(pair),
            list(pair),
            list(single),
            list(single),
            pltpu.SemaphoreType.DMA((132,)),
            pltpu.SemaphoreType.DMA((132,)),
            pltpu.SemaphoreType.DMA((12,)),
        ],
        compiler_params=pltpu.CompilerParams(
            collective_id=1, has_side_effects=True, vmem_limit_bytes=67_043_328
        ),
        cost_estimate=pl.CostEstimate(
            flops=2 * length * slab * (2 * qcols + HD), bytes_accessed=400_000_000, transcendentals=0
        ),
        name="attention_forward",
    )(tok, cot, gains, cos, sin, keep, w_q, w_kv, w_o, w_gate, w_up)


class Product:
    def __init__(self, wire, flip, left, right, shard, mine, near, far, sums):
        self.wire, self.flip, self.left, self.right, self.shard = wire, flip, left, right, shard
        self.mine, self.near, self.far, self.sums = mine, near, far, sums
        self.fs = partners("fsdp", 4)
        self.slab = shard.shape[1] if flip else shard.shape[0]
        units = shard.shape[0] if flip else shard.shape[1]
        cut = 128 * ((units + 255) // 256)
        self.spans = ((0, cut), (cut, units - cut))
        self.first, self.second = (1, 2), (2, 1)
        self.one, self.two = {}, {}

    def piece(self, k, half):
        start, size = self.spans[half]
        block = pl.ds(pl.multiple_of(self.fs[k] * self.slab, self.slab), self.slab)
        if self.flip:
            right = self.right[..., block]
            right = right.reshape(-1, right.shape[-1])
            return tn_dot(self.left[:, start : start + size], right)
        return tn_dot(self.left[:, block], self.right[:, start : start + size])

    def start(self):
        for slot in (0, 1):
            for half in (0, 1):
                k = 3 if slot == 0 else self.first[half]
                self.mine[half][slot] = self.piece(k, half).astype(BF)
                self.one[half, slot] = self.wire(
                    self.mine[half].at[slot],
                    self.near[half].at[slot],
                    "fsdp",
                    self.fs[self.first[half]],
                )

    def middle(self):
        for half in (0, 1):
            own = self.piece(self.second[half], half)
            self.one[half, 0].wait_recv()
            self.sums[half][...] = (own + self.near[half][0].astype(F32)).astype(BF)
            self.two[half] = self.wire(
                self.sums[half], self.far[half], "fsdp", self.fs[self.second[half]]
            )

    def end(self):
        for half in (0, 1):
            start, size = self.spans[half]
            own = self.piece(0, half)
            self.one[half, 1].wait_recv()
            own += self.near[half][1].astype(F32)
            self.two[half].wait_recv()
            own += self.far[half][...].astype(F32)
            if self.flip:
                self.shard[start : start + size, :] = own.astype(BF)
            else:
                self.shard[:, start : start + size] = own.astype(BF)


def product_sizes(flip, slab, units):
    cut = 128 * ((units + 255) // 256)
    return [(size, slab) if flip else (slab, size) for size in (cut, units - cut)]


def turn(value, c, s):
    front = value[:, 0:128]
    return jnp.concatenate(
        [front * c + pltpu.roll(front, 64, 1) * s, value[:, 128:256]], axis=1
    )


class Line:
    def __init__(self, own, inbox, outbox, total, send, recv):
        self.own, self.inbox, self.outbox, self.total = own, inbox, outbox, total
        self.send, self.recv = send, recv
        self.ci = lax.axis_index("ctx")

    def copy(self, way, u):
        step = 1 if way == 0 else 3
        return pltpu.make_async_remote_copy(
            src_ref=self.outbox.at[way, u - 1 + way],
            dst_ref=self.inbox.at[way, u - 1 + way],
            send_sem=self.send.at[way, u - 1 + way],
            recv_sem=self.recv.at[way, u - 1 + way],
            device_id={"ctx": lax.rem(self.ci + step, 4)},
            device_id_type=MESH,
        )

    def sends(self, way, u):
        return self.ci < u if way == 0 else self.ci > u

    def fed(self, way):
        return self.ci > 0 if way == 0 else self.ci < 3

    def lead(self):
        for step in range(3):
            for way, u in ((0, 3 - step), (1, step)):

                @pl.when(jnp.logical_and(self.sends(way, u), jnp.logical_not(self.fed(way))))
                def _():
                    self.outbox[way, u - 1 + way] = self.own(u).astype(BF)
                    self.copy(way, u).start()

    def push(self, step):
        for way, u in ((0, 3 - step), (1, step)):

            @pl.when(jnp.logical_and(self.sends(way, u), self.fed(way)))
            def _():
                self.copy(way, u).wait_recv()
                slot = u - 1 + way
                self.outbox[way, slot] = (
                    self.own(u) + self.inbox[way, slot].astype(F32)
                ).astype(BF)
                self.copy(way, u).start()

    def collect(self):
        self.total[...] = self.own(self.ci)
        for way in (0, 1):

            @pl.when(self.fed(way))
            def _():
                self.copy(way, self.ci).wait_recv()
                self.total[...] += self.inbox[way, self.ci - 1 + way].astype(F32)

    def drain(self):
        for way in (0, 1):
            for u in range(1 - way, 4 - way):

                @pl.when(self.sends(way, u))
                def _():
                    self.copy(way, u).wait_send()


def line_scratch(*form):
    return [
        pltpu.VMEM((2, 3, *form), BF),
        pltpu.VMEM((2, 3, *form), BF),
        pltpu.VMEM(form, F32),
        pltpu.SemaphoreType.DMA((2, 3)),
        pltpu.SemaphoreType.DMA((2, 3)),
    ]


class Spread:
    def __init__(self, own, full, pieces, send, recv, local):
        self.own, self.full, self.pieces = own, full, pieces
        self.send, self.recv = send, recv
        self.height = own.shape[0] // pieces
        self.cs = partners("ctx", 4)
        self.ci = self.cs[0]
        self.inner = jnp.logical_and(self.ci > 0, self.ci < 3)
        self.local = pltpu.make_async_copy(own, full.at[self.ci], local)

    def strip(self, p):
        return pl.ds(p * self.height, self.height)

    def copy(self, kind, p, source, peer):
        place = self.full.at[source, self.strip(p), :]
        src = self.own.at[self.strip(p), :] if kind < 2 else place
        slot = (0, 1, 2, 1, 2)[kind]
        return pltpu.make_async_remote_copy(
            src_ref=src,
            dst_ref=place,
            send_sem=self.send.at[kind, p],
            recv_sem=self.recv.at[slot, p],
            device_id={"ctx": peer},
            device_id_type=MESH,
        )

    def out(self, kind, p):
        cs = self.cs
        source = (cs[0], cs[0], cs[1], cs[3], cs[2])[kind]
        peer = (cs[1], cs[3], cs[3], cs[1], cs[1])[kind]
        return self.copy(kind, p, source, peer)

    def arrived(self, slot, p):
        self.copy((0, 1, 2)[slot], p, self.ci, self.cs[1]).wait_recv()

    def begin(self):
        self.local.start()

    def give(self, p):
        self.out(0, p).start()

        @pl.when(self.inner)
        def _():
            self.out(1, p).start()

    def hand_on(self, p):
        @pl.when(self.inner)
        def _():
            self.arrived(0, p)
            self.out(2, p).start()
            self.arrived(1, p)
            self.out(3, p).start()

    def hand_far(self, p):
        @pl.when(self.inner)
        def _():
            self.arrived(2, p)
            self.out(4, p).start()

    def close(self):
        for p in range(self.pieces):

            @pl.when(jnp.logical_not(self.inner))
            def _():
                for slot in range(3):
                    self.arrived(slot, p)

            self.out(0, p).wait_send()

            @pl.when(self.inner)
            def _():
                for kind in range(1, 5):
                    self.out(kind, p).wait_send()

        self.local.wait()


def spread_scratch(pieces):
    return [
        pltpu.SemaphoreType.DMA((5, pieces)),
        pltpu.SemaphoreType.DMA((3, pieces)),
        pltpu.SemaphoreType.DMA,
    ]


def units_line(wire, part, side, line_refs, ti):
    other = 1 - ti
    side_in = [wire(part.at[u, other], side.at[u], "tp", other) for u in range(4)]
    for copy in side_in:
        copy.wait_recv()
    return Line(lambda u: part[u, ti].astype(F32) + side[u].astype(F32), *line_refs)


def backward_kernel(
    heads,
    dn,
    cot,
    state,
    gains_all,
    probs,
    q_rot,
    kv,
    cos,
    sin,
    w_o,
    normed,
    att,
    normed_all,
    d_gate,
    d_up,
    after,
    d_state,
    gain_part,
    dq_plane,
    dkv_plane,
    weight_grads,
    gate_all,
    up_all,
    side,
    dbuf,
    dslab,
    dpart,
    dfar,
    dkv2,
    kvt,
    zk,
    zfar,
    dqbuf,
    dkvbuf,
    dk_acc,
    dv_acc,
    own_out,
    own_query,
    row_refs,
    out_refs,
    query_refs,
    parts,
    sums,
    gate_recv,
    up_recv,
    shard_gate,
    shard_up,
    gate_sems,
    up_sems,
    send,
    recv,
    local,
):
    del after
    fs, cs = partners("fsdp", 4), partners("ctx", 4)
    ti = lax.axis_index("tp")
    other = 1 - ti
    hrows, depth = state.shape
    rows = 2 * hrows
    slab = depth // 4
    length = 4 * rows
    scale = HD ** (-0.5)
    greet(
        [("fsdp", fs[k]) for k in (1, 2, 3)]
        + [("ctx", cs[k]) for k in (1, 2, 3)]
        + [("tp", other)]
    )
    wire = Wire(send, recv)
    mine = pl.ds(pl.multiple_of(ti * hrows, hrows), hrows)

    def lanes(index):
        return pl.ds(pl.multiple_of(index * slab, slab), slab)

    gate = Product(wire, False, normed_all, d_gate, shard_gate, parts, *gate_recv, sums)
    up = Product(wire, False, normed_all, d_up, shard_up, parts, *up_recv, sums)
    gate_line = Spread(shard_gate, gate_all, PIECES, *gate_sems)
    up_line = Spread(shard_up, up_all, PIECES, *up_sems)
    gate.start()
    line = units_line(wire, dn, side, row_refs, ti)
    line.lead()
    squares = jnp.zeros((hrows, 1), F32)
    for k in range(4):
        u = state[:, lanes(fs[k])]
        squares += jnp.sum(u * u, axis=1, keepdims=True)
    r = lax.rsqrt(squares * (1.0 / depth) + 1e-06)
    gate.middle()
    line.push(0)
    line.push(1)
    gate.end()
    gate_line.begin()
    for p in range(PIECES):
        gate_line.give(p)
    line.push(2)
    line.collect()
    inner = jnp.zeros((hrows, 1), F32)
    for k in range(4):
        at = lanes(fs[k])
        inner += jnp.sum(
            state[:, at] * gains_all[k, 1:2, :] * line.total[:, at], axis=1, keepdims=True
        )
    pull = r * r * r * (inner * (1.0 / depth))
    d_in = {}
    d_side = {}
    gain_part[...] = jnp.zeros_like(gain_part)
    for k in (1, 2, 3, 0):
        at = lanes(fs[k])
        u, d = state[:, at], line.total[:, at]
        ds = cot[mine, at].astype(F32) + (r * (gains_all[k, 1:2, :] * d) - u * pull)
        d_state[:, at] = ds
        if k:
            dbuf[k] = ds.astype(BF)
            d_in[k] = wire(dbuf.at[k], dslab.at[k, ti], "fsdp", fs[k])
        else:
            dslab[0, ti] = ds.astype(BF)
            d_side[0] = wire(dslab.at[0, ti], dslab.at[0, ti], "tp", other)
        gain_part[k, 1:2, :] = jnp.sum(u * r * d, axis=0, keepdims=True)
    for k in (1, 2, 3):
        d_in[k].wait_recv()
        d_side[k] = wire(dslab.at[k, ti], dslab.at[k, ti], "tp", other)
    a_in = {}
    for k in (1, 2, 3, 0):
        d_side[k].wait_recv()
        block = dslab[k].reshape(rows, slab)
        dpart[k] = nt_dot(block, w_o[...]).astype(BF)
        if k:
            a_in[k] = wire(dpart.at[k], dfar.at[k], "fsdp", fs[k])
    wire.settle(list(gate.one.values()) + list(gate.two.values()))
    up.start()
    keys = kv[0].reshape(length, HD)
    values = kv[1].reshape(length, HD)
    c, s = cos[...], sin[...]
    quarter = heads * HD // 4
    branch = dslab[...].reshape(length, slab)
    for u in range(4):
        columns = att[:, :, u * quarter : (u + 1) * quarter].reshape(length, quarter)
        own_out[u] = tn_dot(columns, branch).astype(BF)
    out_line = Line(lambda u: own_out[u].astype(F32), *out_refs)
    for k in (1, 2, 3):
        a_in[k].wait_recv()
    for h in range(heads):
        at = slice(h * HD, (h + 1) * HD)
        d = dpart[0, :, at].astype(F32)
        for k in (1, 2, 3):
            d += dfar[k, :, at].astype(F32)
        d = d.astype(BF)
        p = probs[h]
        dp = nt_dot(d, values)
        delta = jnp.sum(p * dp, axis=1, keepdims=True)
        dsc = (p * (dp - delta)).astype(BF)
        dq = jnp.dot(dsc, keys, preferred_element_type=F32) * scale
        dqbuf[0, :, at] = turn(dq, c, -s).astype(BF)
        dk = tn_dot(dsc, q_rot[:, at])
        dv = tn_dot(p.astype(BF), d)
        if h == 0:
            dk_acc[...] = dk
            dv_acc[...] = dv
        else:
            dk_acc[...] += dk
            dv_acc[...] += dv
    dkv2[0] = (dk_acc[...] * scale).astype(BF).reshape(4, rows, HD)
    dkv2[1] = dv_acc[...].astype(BF).reshape(4, rows, HD)
    k_side = wire(dkv2.at[other], kvt, "tp", other)
    q_in = {}
    for k in (1, 2, 3):
        q_in[k] = wire(dqbuf.at[0], dqbuf.at[k], "fsdp", fs[k])
    k_side.wait_recv()
    z_in = {}
    for k in (1, 2, 3):
        zk[k] = (dkv2[ti, k].astype(F32) + kvt[k].astype(F32)).astype(BF)
        z_in[k] = wire(zk.at[k], zfar.at[k], "ctx", cs[k])
    for p in range(PIECES // 2):
        gate_line.hand_on(p)
    out_line.lead()
    own = dkv2[ti, 0].astype(F32) + kvt[0].astype(F32)
    for k in (1, 2, 3):
        z_in[k].wait_recv()
        own += zfar[k].astype(F32)
    zero = (1 - ti).astype(F32)
    dkvbuf[0] = turn(own, c * zero + (1.0 - zero), -s * zero).astype(BF)
    v_in = {}
    for k in (1, 2, 3):
        v_in[k] = wire(dkvbuf.at[0], dkvbuf.at[k], "fsdp", fs[k])
    up.middle()
    for p in range(PIECES // 2, PIECES):
        gate_line.hand_on(p)
    out_line.push(0)
    for k in (1, 2, 3):
        q_in[k].wait_recv()
    slabs = normed[...].reshape(length, slab)
    for u in (3, 0, 2, 1):
        columns = dqbuf[:, :, u * quarter : (u + 1) * quarter].reshape(length, quarter)
        own_query[u, 0:quarter] = tn_dot(columns, slabs).astype(BF)
    for k in (1, 2, 3):
        v_in[k].wait_recv()
    keep_q = pltpu.make_async_copy(dqbuf, dq_plane, local.at[0])
    keep_v = pltpu.make_async_copy(dkvbuf, dkv_plane, local.at[1])
    keep_q.start()
    keep_v.start()
    for u in (3, 0, 2, 1):
        columns = dkvbuf[:, :, u * (HD // 4) : (u + 1) * (HD // 4)].reshape(length, HD // 4)
        own_query[u, quarter:] = tn_dot(columns, slabs).astype(BF)
    query_line = Line(lambda u: own_query[u].astype(F32), *query_refs)
    query_line.lead()
    for p in range(PIECES // 2):
        gate_line.hand_far(p)
    up.end()
    up_line.begin()
    for p in range(PIECES // 2):
        up_line.give(p)
    out_line.push(1)
    query_line.push(0)
    for p in range(PIECES // 2, PIECES):
        gate_line.hand_far(p)
    for p in range(PIECES // 2, PIECES):
        up_line.give(p)
    out_line.push(2)
    query_line.push(1)
    query_line.push(2)
    for p in range(PIECES):
        up_line.hand_on(p)
    out_line.collect()
    weight_grads[0:quarter, :] = out_line.total[...].astype(BF)
    query_line.collect()
    weight_grads[quarter:, :] = query_line.total[...].astype(BF)
    for p in range(PIECES):
        up_line.hand_far(p)
    gate_line.close()
    up_line.close()
    for each in (line, out_line, query_line):
        each.drain()
    keep_q.wait()
    keep_v.wait()
    wire.finish()


PIECES = 4


def call_backward(
    heads, dn, cot, state, gains_all, probs, q_rot, kv, cos, sin, w_o, normed, att, normed_all, d_gate, d_up, after
):
    hrows, depth = state.shape
    rows, slab, qcols = 2 * hrows, depth // 4, heads * HD
    length = 4 * rows
    units = d_gate.shape[1]
    sizes = product_sizes(False, slab, units)
    pair = [pltpu.VMEM((2, *size), BF) for size in sizes]
    single = [pltpu.VMEM(size, BF) for size in sizes]
    shape = jax.ShapeDtypeStruct
    vmem = pl.BlockSpec(memory_space=pltpu.VMEM)
    hbm = pl.BlockSpec(memory_space=pl.ANY)
    return pl.pallas_call(
        functools.partial(backward_kernel, heads),
        out_shape=[
            shape((hrows, depth), F32),
            shape((4, 8, slab), F32),
            shape((4, rows, qcols), BF),
            shape((4, rows, HD), BF),
            shape((qcols // 2 + HD // 4, slab), BF),
            shape((4, slab, units), BF),
            shape((4, slab, units), BF),
        ],
        in_specs=[vmem] * 15 + [hbm],
        out_specs=[vmem] * 2 + [hbm] * 2 + [vmem] + [hbm] * 2,
        scratch_shapes=[
            pltpu.VMEM((4, hrows, depth), BF),
            pltpu.VMEM((4, hrows, slab), BF),
            pltpu.VMEM((4, 2, hrows, slab), BF),
            pltpu.VMEM((4, rows, qcols), BF),
            pltpu.VMEM((4, rows, qcols), BF),
            pltpu.VMEM((2, 4, rows, HD), BF),
            pltpu.VMEM((4, rows, HD), BF),
            pltpu.VMEM((4, rows, HD), BF),
            pltpu.VMEM((4, rows, HD), BF),
            pltpu.VMEM((4, rows, qcols), BF),
            pltpu.VMEM((4, rows, HD), BF),
            pltpu.VMEM((length, HD), F32),
            pltpu.VMEM((length, HD), F32),
            pltpu.VMEM((4, qcols // 4, slab), BF),
            pltpu.VMEM((4, (qcols + HD) // 4, slab), BF),
            line_scratch(hrows, depth),
            line_scratch(qcols // 4, slab),
            line_scratch((qcols + HD) // 4, slab),
            list(pair),
            list(single),
            [list(pair), list(single)],
            [list(pair), list(single)],
            pltpu.VMEM((slab, units), BF),
            pltpu.VMEM((slab, units), BF),
            spread_scratch(PIECES),
            spread_scratch(PIECES),
            pltpu.SemaphoreType.DMA((48,)),
            pltpu.SemaphoreType.DMA((48,)),
            pltpu.SemaphoreType.DMA((2,)),
        ],
        compiler_params=pltpu.CompilerParams(
            collective_id=5, has_side_effects=True, vmem_limit_bytes=67_043_328
        ),
        cost_estimate=pl.CostEstimate(
            flops=2 * length * slab * qcols, bytes_accessed=300_000_000, transcendentals=0
        ),
        name="attention_backward",
    )(dn, cot, state, gains_all, probs, q_rot, kv, cos, sin, w_o, normed, att, normed_all, d_gate, d_up, after)


STRIP = 80


def conversions(sources, targets, inbuf, outbuf, in_sems, out_sems):
    jobs = []
    for which in (0, 1):
        for p in range(sources[which].shape[1] // STRIP):
            jobs.append((which, p))
    for p in range(sources[2].shape[0] // (4 * STRIP)):
        jobs.append((2, p))

    def load(n):
        which, p = jobs[n]
        slot = n % 2
        if which < 2:
            source = sources[which].at[:, pl.ds(p * STRIP, STRIP), :]
            return pltpu.make_async_copy(source, inbuf[0].at[slot], in_sems.at[slot])
        source = sources[2].at[pl.ds(p * 4 * STRIP, 4 * STRIP), :]
        return pltpu.make_async_copy(source, inbuf[1].at[slot], in_sems.at[slot])

    def store(n):
        which, p = jobs[n]
        slot = n % 2
        if which < 2:
            target = targets[which].at[pl.ds(p * STRIP, STRIP), :]
            return pltpu.make_async_copy(outbuf[0].at[slot], target, out_sems.at[slot])
        target = targets[2].at[pl.ds(p * 4 * STRIP, 4 * STRIP), :]
        return pltpu.make_async_copy(outbuf[1].at[slot], target, out_sems.at[slot])

    load(0).start()
    for n, (which, p) in enumerate(jobs):
        slot = n % 2
        if n + 1 < len(jobs):
            load(n + 1).start()
        load(n).wait()
        if n >= 2:
            store(n - 2).wait()
        if which < 2:
            units = sources[which].shape[2]
            for j in range(4):
                outbuf[0][slot, :, j * units : (j + 1) * units] = inbuf[0][slot, j].astype(F32)
        else:
            outbuf[1][slot] = inbuf[1][slot].astype(F32)
        store(n).start()
        if n + 1 == len(jobs):
            store(n - 1).wait()
            store(n).wait()
        yield


def convert_kernel(gate_all, up_all, down_all, grad_gate, grad_up, grad_down, inbuf, outbuf, in_sems, out_sems):
    steps = conversions(
        (gate_all, up_all, down_all), (grad_gate, grad_up, grad_down), inbuf, outbuf, in_sems, out_sems
    )
    for _ in steps:
        pass


def call_convert(gate_all, up_all, down_all):
    slab, units = gate_all.shape[1:]
    shape = jax.ShapeDtypeStruct
    hbm = pl.BlockSpec(memory_space=pl.ANY)
    return pl.pallas_call(
        convert_kernel,
        out_shape=[
            shape((slab, 4 * units), F32),
            shape((slab, 4 * units), F32),
            shape((4 * units, slab), F32),
        ],
        in_specs=[hbm] * 3,
        out_specs=[hbm] * 3,
        scratch_shapes=[
            [pltpu.VMEM((2, 4, STRIP, units), BF), pltpu.VMEM((2, 4 * STRIP, slab), BF)],
            [pltpu.VMEM((2, STRIP, 4 * units), F32), pltpu.VMEM((2, 4 * STRIP, slab), F32)],
            pltpu.SemaphoreType.DMA((2,)),
            pltpu.SemaphoreType.DMA((2,)),
        ],
        cost_estimate=pl.CostEstimate(
            flops=0, bytes_accessed=18 * slab * 4 * units, transcendentals=0
        ),
        name="convert",
    )(gate_all, up_all, down_all)


def finish_kernel(
    part,
    state,
    tok,
    gains_all,
    gain_part,
    d_state,
    dq,
    dkv,
    w_q,
    w_kv,
    after,
    out,
    grad_tok,
    gain_grads,
    side,
    row_refs,
    obuf,
    gbuf,
    pbuf,
    pside,
    dbuf,
    drow,
    gpart,
    gfar,
    gsum,
    gnear,
    send,
    recv,
):
    del after
    fs, cs = partners("fsdp", 4), partners("ctx", 4)
    ti = lax.axis_index("tp")
    other = 1 - ti
    hrows, depth = state.shape
    slab = depth // 4
    greet(
        [("fsdp", fs[k]) for k in (1, 2, 3)]
        + [("ctx", cs[k]) for k in (1, 2, 3)]
        + [("tp", other)]
    )
    wire = Wire(send, recv)
    mine = pl.ds(pl.multiple_of(ti * hrows, hrows), hrows)

    def lanes(index):
        return pl.ds(pl.multiple_of(index * slab, slab), slab)

    line = units_line(wire, part, side, row_refs, ti)
    line.lead()
    line.push(0)
    kv_half = w_kv[:, pl.ds(pl.multiple_of(ti * HD, HD), HD)]
    p_in = {}
    for k in (1, 2, 3, 0):
        block = (nt_dot(dq[k], w_q[...]) + nt_dot(dkv[k], kv_half)).astype(BF)
        pbuf[k, 0] = block[0:hrows]
        pbuf[k, 1] = block[hrows : 2 * hrows]
        p_in[k] = wire(pbuf.at[k, other], pside.at[k], "tp", other)
    d_in = {}
    for k in (1, 2, 3, 0):
        p_in[k].wait_recv()
        both = (pbuf[k, ti].astype(F32) + pside[k].astype(F32)).astype(BF)
        if k:
            dbuf[k] = both
            d_in[k] = wire(dbuf.at[k], drow.at[k], "fsdp", fs[k])
        else:
            drow[0] = both
    line.push(1)
    squares = jnp.zeros((hrows, 1), F32)
    for k in range(4):
        u = tok[mine, lanes(fs[k])].astype(F32)
        squares += jnp.sum(u * u, axis=1, keepdims=True)
    r = lax.rsqrt(squares * (1.0 / depth) + 1e-06)
    inner = jnp.zeros((hrows, 1), F32)
    for k in range(4):
        if k:
            d_in[k].wait_recv()
        u = tok[mine, lanes(fs[k])].astype(F32)
        inner += jnp.sum(u * gains_all[k, 0:1, :] * drow[k].astype(F32), axis=1, keepdims=True)
    pull = r * r * r * (inner * (1.0 / depth))
    gpart[...] = gain_part[...]
    for k in range(4):
        at = lanes(fs[k])
        u, d = tok[mine, at].astype(F32), drow[k].astype(F32)
        gbuf[ti, :, at] = d_state[:, at] + (r * (gains_all[k, 0:1, :] * d) - u * pull)
        gpart[k, 0:1, :] = jnp.sum(u * r * d, axis=0, keepdims=True)
    g_side = wire(gbuf.at[ti], gbuf.at[ti], "tp", other)
    g_in = {}
    for k in (1, 2, 3):
        g_in[k] = wire(gpart.at[k], gfar.at[k], "fsdp", fs[k])
    line.push(2)
    line.collect()
    obuf[ti] = (state[...] + line.total[...]).astype(BF)
    o_side = wire(obuf.at[ti], obuf.at[ti], "tp", other)
    total = gpart[0]
    for k in (1, 2, 3):
        g_in[k].wait_recv()
        total += gfar[k]
    for step, (axis, peer) in enumerate((("ctx", cs[1]), ("ctx", cs[2]), ("tp", other))):
        gsum[step] = total
        copy = wire(gsum.at[step], gnear.at[step], axis, peer)
        copy.wait_recv()
        total = total + gnear[step]
    gain_grads[...] = total
    g_side.wait_recv()
    grad_tok[...] = gbuf[...]
    o_side.wait_recv()
    out[...] = obuf[...]
    line.drain()
    wire.finish()


def call_finish(part, state, tok, gains_all, gain_part, d_state, dq, dkv, w_q, w_kv, after):
    hrows, depth = state.shape
    rows, slab = 2 * hrows, depth // 4
    shape = jax.ShapeDtypeStruct
    vmem = pl.BlockSpec(memory_space=pltpu.VMEM)
    hbm = pl.BlockSpec(memory_space=pl.ANY)
    return pl.pallas_call(
        finish_kernel,
        out_shape=[
            shape((2, hrows, depth), BF),
            shape((2, hrows, depth), F32),
            shape((8, slab), F32),
        ],
        in_specs=[vmem] * 10 + [hbm],
        out_specs=[vmem] * 3,
        scratch_shapes=[
            pltpu.VMEM((4, hrows, depth), BF),
            line_scratch(hrows, depth),
            pltpu.VMEM((2, hrows, depth), BF),
            pltpu.VMEM((2, hrows, depth), F32),
            pltpu.VMEM((4, 2, hrows, slab), BF),
            pltpu.VMEM((4, hrows, slab), BF),
            pltpu.VMEM((4, hrows, slab), BF),
            pltpu.VMEM((4, hrows, slab), BF),
            pltpu.VMEM((4, 8, slab), F32),
            pltpu.VMEM((4, 8, slab), F32),
            pltpu.VMEM((3, 8, slab), F32),
            pltpu.VMEM((3, 8, slab), F32),
            pltpu.SemaphoreType.DMA((32,)),
            pltpu.SemaphoreType.DMA((32,)),
        ],
        compiler_params=pltpu.CompilerParams(collective_id=6, has_side_effects=True),
        cost_estimate=pl.CostEstimate(
            flops=2 * 4 * rows * slab * w_q.shape[1], bytes_accessed=150_000_000, transcendentals=0
        ),
        name="finish",
    )(part, state, tok, gains_all, gain_part, d_state, dq, dkv, w_q, w_kv, after)


def fast_device(
    tokens,
    segment_ids,
    w_query,
    w_keyval,
    w_out,
    w_gate,
    w_up,
    w_down,
    gain_attn,
    gain_ffn,
    cotangent,
):
    ci, ti = lax.axis_index("ctx"), lax.axis_index("tp")
    tok, cot = tokens[0], cotangent[0]
    rows, depth = tok.shape
    hrows, slab = rows // 2, depth // 4
    length = segment_ids.shape[1]
    heads = w_query.shape[1] // HD
    units = w_gate.shape[1] // 4

    def cut(value, start, size, axis):
        return lax.dynamic_slice_in_dim(value, start, size, axis)

    segment_row = segment_ids[0]
    local_segment = cut(segment_row, ci * rows, rows, 0)
    local_index = ci * rows + jnp.arange(rows, dtype=jnp.int32)
    earlier = jnp.sum((segment_row[None, :] < local_segment[:, None]).astype(jnp.int32), axis=1)
    position = (local_index - earlier).astype(F32)
    freqs = 10000.0 ** (-(jnp.arange(HD // 4, dtype=F32) * 2.0 / (HD // 2)))
    angle = position[:, None] * freqs[None, :]
    cosine, sine = jnp.cos(angle), jnp.sin(angle)
    cos = jnp.concatenate([cosine, cosine], axis=1)
    sin = jnp.concatenate([-sine, sine], axis=1)
    key_index = jnp.concatenate(
        [(ci ^ k) * rows + jnp.arange(rows, dtype=jnp.int32) for k in range(4)]
    )
    key_segment = jnp.concatenate([cut(segment_row, (ci ^ k) * rows, rows, 0) for k in range(4)])
    keep = (
        (local_segment[:, None] == key_segment[None, :])
        & (key_index[None, :] <= local_index[:, None])
    ).astype(F32)
    gains = jnp.concatenate(
        [gain_attn[None], gain_ffn[None], jnp.zeros((6, slab), gain_attn.dtype)]
    ).astype(F32)

    (
        q_rot,
        kv,
        probs,
        state,
        gains_all,
        normed_all,
        cot_all,
        gate_full,
        up_full,
        normed_slab,
        att_plane,
        gate,
        upward,
        hidden,
        shard_down,
    ) = call_forward(
        heads,
        tok,
        cot,
        gains,
        cos,
        sin,
        keep,
        w_query,
        w_keyval,
        w_out,
        w_gate,
        w_up,
    )
    down_full = call_gather(w_down, shard_down)
    normed_all = normed_all.reshape(length, depth)
    cot_all = cot_all.reshape(length, depth)
    gate_full = gate_full.reshape(depth, units)
    up_full = up_full.reshape(depth, units)
    down_full = down_full.reshape(depth, units)

    grad_down = lax.all_gather(shard_down, "ctx", axis=0, tiled=True)
    d_hidden = matmul(cot_all, down_full)
    _, geglu_pull = jax.vjp(geglu, gate, upward)
    d_gate, d_up = geglu_pull(d_hidden)
    d_gate = d_gate.astype(BF)
    d_up = d_up.astype(BF)
    dn = (times_transposed(d_gate, gate_full) + times_transposed(d_up, up_full)).astype(BF)
    dn = dn.reshape(4, 2, hrows, depth)
    part = times_transposed(hidden, down_full).astype(BF).reshape(4, 2, hrows, depth)
    d_state, gain_part, dq, dkv, weight_grads, gate_all, up_all = call_backward(
        heads,
        dn,
        cot,
        state,
        gains_all,
        probs,
        q_rot,
        kv,
        cos,
        sin,
        w_out,
        normed_slab,
        att_plane,
        normed_all,
        d_gate,
        d_up,
        shard_down,
    )
    weight_grads = lax.all_gather(weight_grads, "ctx", axis=0, tiled=False)
    grad_gate, grad_up, grad_down = call_convert(gate_all, up_all, grad_down)
    out, grad_tok, gain_grads = call_finish(
        part, state, tok, gains_all, gain_part, d_state, dq, dkv, w_query, w_keyval, grad_gate
    )
    quarter = heads * HD // 4
    grad_out = weight_grads[:, 0:quarter].reshape(4 * quarter, slab).astype(F32)
    grad_query = weight_grads[:, quarter : 2 * quarter].reshape(4 * quarter, slab).T.astype(F32)
    kv_mine = weight_grads[:, 2 * quarter :].reshape(HD, slab)
    kv_other = swap(kv_mine, "tp", 2, 1)
    grad_kv = jnp.where(
        ti == 0,
        jnp.concatenate([kv_mine, kv_other], axis=0),
        jnp.concatenate([kv_other, kv_mine], axis=0),
    ).T.astype(F32)

    return (
        out.reshape(1, rows, depth),
        grad_tok.reshape(1, rows, depth),
        grad_query,
        grad_kv,
        grad_out,
        grad_gate,
        grad_up,
        grad_down,
        gain_grads[0],
        gain_grads[1],
    )


def solution(mesh):
    sizes = (mesh.shape["fsdp"], mesh.shape["ctx"], mesh.shape["tp"])
    in_specs = (
        P("fsdp", "ctx", None),
        P("fsdp", None),
        P("fsdp", "tp"),
        P("fsdp", None),
        P("tp", "fsdp"),
        P("fsdp", "tp"),
        P("fsdp", "tp"),
        P("tp", "fsdp"),
        P("fsdp"),
        P("fsdp"),
        P("fsdp", "ctx", None),
    )
    out_specs = (
        P("fsdp", "ctx", None),
        P("fsdp", "ctx", None),
        P("fsdp", "tp"),
        P("fsdp", None),
        P("tp", "fsdp"),
        P("fsdp", "tp"),
        P("fsdp", "tp"),
        P("tp", "fsdp"),
        P("fsdp"),
        P("fsdp"),
    )

    def body(*args):
        rows, depth = args[0].shape[1:]
        fits = sizes == (4, 4, 2) and depth % 512 == 0 and rows % 32 == 0
        if fits:
            return fast_device(*args)
        return per_device(sizes, *args)

    return jax.shard_map(
        body, mesh=mesh, in_specs=in_specs, out_specs=out_specs, check_vma=False
    )
```

```python
import functools

import jax
import jax.numpy as jnp
from jax import lax
from jax.experimental import pallas as pl
from jax.experimental.pallas import tpu as pltpu
from jax.sharding import PartitionSpec as P

HD = 256
NEGATIVE = -1e30
BF = jnp.bfloat16
F32 = jnp.float32
MESH = pl.DeviceIdType.MESH


def rms_scale(value, gain):
    return value * lax.rsqrt(jnp.mean(value * value, axis=-1, keepdims=True) + 1e-06) * gain


def rotate(value, cosine, sine):
    quarter = value.shape[-1] // 4
    first = value[..., :quarter]
    second = value[..., quarter : 2 * quarter]
    rest = value[..., 2 * quarter :]
    return jnp.concatenate(
        [first * cosine - second * sine, second * cosine + first * sine, rest], axis=-1
    )


def unrotate(value, cosine, sine):
    return rotate(value, cosine, -sine)


def matmul(left, right):
    return jnp.dot(left, right, preferred_element_type=F32)


def times_transposed(left, right):
    return lax.dot_general(left, right, (((1,), (1,)), ((), ())), preferred_element_type=F32)


def transposed_times(left, right):
    return lax.dot_general(left, right, (((0,), (0,)), ((), ())), preferred_element_type=F32)


def geglu(gate_in, up_in):
    return jax.nn.gelu(gate_in, approximate=True) * up_in


def swap(value, axis, size, k):
    return lax.ppermute(value, axis, [(i, i ^ k) for i in range(size)])


def per_device(
    sizes,
    tokens,
    segment_ids,
    w_query,
    w_keyval,
    w_out,
    w_gate,
    w_up,
    w_down,
    gain_attn,
    gain_ffn,
    cotangent,
):
    nf, nc, nt = sizes
    fi, ci, ti = lax.axis_index("fsdp"), lax.axis_index("ctx"), lax.axis_index("tp")
    rows = tokens.shape[1]
    depth = tokens.shape[2]
    slab = depth // nf
    half = depth // nt
    heads = w_query.shape[1] // HD
    qcols = heads * HD
    units = w_gate.shape[1] // nc
    scale = HD ** (-0.5)

    def cut(value, start, size, axis):
        return lax.dynamic_slice_in_dim(value, start, size, axis)

    def all_to_all_blocks(blocks, axis, size):
        return [blocks[0]] + [swap(blocks[k], axis, size, k) for k in range(1, size)]

    def gather_blocks(value, axis, size):
        return [value] + [swap(value, axis, size, k) for k in range(1, size)]

    def absolute(blocks, index, axis):
        stacked = jnp.stack(blocks)
        size = len(blocks)
        return jnp.concatenate(
            [lax.dynamic_index_in_dim(stacked, j ^ index, 0, keepdims=False) for j in range(size)],
            axis=axis,
        )

    def rows_to_slabs(value):
        blocks = [cut(value, (fi ^ k) * slab, slab, 1) for k in range(nf)]
        return jnp.concatenate(all_to_all_blocks(blocks, "fsdp", nf), axis=0)

    def slabs_to_rows(value):
        blocks = list(value.reshape(nf, rows, slab))
        return absolute(all_to_all_blocks(blocks, "fsdp", nf), fi, 1)

    def reduce_rows(value, width):
        blocks = list(value.reshape(nf, rows, width))
        got = all_to_all_blocks(blocks, "fsdp", nf)
        return sum(block.astype(F32) for block in got)

    def gather_rows(value):
        return jnp.concatenate(gather_blocks(value, "fsdp", nf), axis=0)

    def both_halves(mine, axis):
        other = swap(mine, "tp", nt, 1)
        return jnp.where(
            ti == 0,
            jnp.concatenate([mine, other], axis=axis),
            jnp.concatenate([other, mine], axis=axis),
        )

    def tp_sum(value):
        low = value.astype(BF)
        return low.astype(F32) + swap(low, "tp", nt, 1).astype(F32)

    def gather_ctx(value):
        mine = cut(value, ti * half, half, 1)
        return both_halves(jnp.concatenate(gather_blocks(mine, "ctx", nc), axis=0), 1)

    def reduce_ctx(value):
        low = value.astype(BF)
        keep = cut(low, ti * half, half, 1)
        send = cut(low, (1 - ti) * half, half, 1)
        both = (keep.astype(F32) + swap(send, "tp", nt, 1).astype(F32)).astype(BF)
        got = all_to_all_blocks(list(both.reshape(nc, rows, half)), "ctx", nc)
        return sum(block.astype(F32) for block in got)

    gate_full = lax.all_gather(cut(w_gate, ci * units, units, 1), "fsdp", axis=0, tiled=True)
    up_full = lax.all_gather(cut(w_up, ci * units, units, 1), "fsdp", axis=0, tiled=True)
    down_full = lax.all_gather(
        cut(w_down, ci * units, units, 0).T, "fsdp", axis=0, tiled=True
    )

    gains = jnp.stack([gain_attn, gain_ffn])
    gains = absolute(gather_blocks(gains, "fsdp", nf), fi, 1).astype(F32)
    gain_one, gain_two = gains[0], gains[1]
    inputs = tokens[0].astype(F32)
    incoming = cotangent[0]

    segment_row = segment_ids[0]
    offset = ci * rows
    local_segment = lax.dynamic_slice_in_dim(segment_row, offset, rows, 0)
    local_index = offset + jnp.arange(rows, dtype=jnp.int32)
    earlier = jnp.sum((segment_row[None, :] < local_segment[:, None]).astype(jnp.int32), axis=1)
    position = (local_index - earlier).astype(F32)
    freqs = 10000.0 ** (-(jnp.arange(HD // 4, dtype=F32) * 2.0 / (HD // 2)))
    angle = position[:, None] * freqs[None, :]
    cosine = jnp.cos(angle)
    sine = jnp.sin(angle)

    normed_attn = rms_scale(inputs, gain_one).astype(BF)
    normed_slab = rows_to_slabs(normed_attn)
    kv_half = cut(w_keyval, ti * HD, HD, 1)
    partial = jnp.concatenate(
        [matmul(normed_slab, w_query).astype(BF), matmul(normed_slab, kv_half).astype(BF)], axis=1
    )
    projected = reduce_rows(partial, qcols + HD)
    query = projected[:, :qcols].reshape(rows, heads, HD)
    keyval = projected[:, qcols:]
    query_rows = (
        rotate(query, cosine[:, None, :], sine[:, None, :]).reshape(rows * heads, HD).astype(BF)
    )
    keyval = jnp.where(ti == 0, rotate(keyval, cosine, sine), keyval).astype(BF)
    kv_all = jnp.concatenate(gather_blocks(keyval, "ctx", nc), axis=0)
    kv_other = swap(kv_all, "tp", nt, 1)
    key_all = jnp.where(ti == 0, kv_all, kv_other)
    value_all = jnp.where(ti == 0, kv_other, kv_all)

    key_index = jnp.concatenate(
        [(ci ^ k) * rows + jnp.arange(rows, dtype=jnp.int32) for k in range(nc)]
    )
    key_segment = jnp.concatenate(
        [lax.dynamic_slice_in_dim(segment_row, (ci ^ k) * rows, rows, 0) for k in range(nc)]
    )
    row_index = jnp.repeat(local_index, heads)
    row_segment = jnp.repeat(local_segment, heads)
    mask = (row_segment[:, None] == key_segment[None, :]) & (
        key_index[None, :] <= row_index[:, None]
    )
    scores = jnp.where(mask, times_transposed(query_rows, key_all) * scale, NEGATIVE)
    peak = jnp.max(scores, axis=1, keepdims=True)
    terms = jnp.exp(scores - peak)
    probs = terms / jnp.sum(terms, axis=1, keepdims=True)
    probs_low = probs.astype(BF)
    attended = matmul(probs_low, value_all).reshape(rows, qcols).astype(BF)

    attended_plane = gather_rows(attended)
    branch = tp_sum(matmul(attended_plane, w_out)).astype(BF)
    hidden_state = inputs + slabs_to_rows(branch).astype(F32)
    normed_ffn = rms_scale(hidden_state, gain_two).astype(BF)

    normed_all = gather_ctx(normed_ffn)
    incoming_all = gather_ctx(incoming)
    gate = matmul(normed_all, gate_full)
    upward = matmul(normed_all, up_full)
    d_hidden = matmul(incoming_all, down_full)
    hidden, geglu_pull = jax.vjp(geglu, gate, upward)
    hidden = hidden.astype(BF)
    d_gate, d_up = geglu_pull(d_hidden)
    d_gate = d_gate.astype(BF)
    d_up = d_up.astype(BF)

    def finish(grad, axis):
        low = grad.astype(BF)
        blocks = [cut(low, (fi ^ k) * slab, slab, axis) for k in range(nf)]
        got = all_to_all_blocks(blocks, "fsdp", nf)
        return sum(block.astype(F32) for block in got).astype(BF)

    shard_down = finish(transposed_times(hidden, incoming_all), 1)
    grad_down = lax.all_gather(shard_down, "ctx", axis=0, tiled=True).astype(F32)
    shard_gate = finish(transposed_times(normed_all, d_gate), 0)
    grad_gate = lax.all_gather(shard_gate, "ctx", axis=0, tiled=False)
    shard_up = finish(transposed_times(normed_all, d_up), 0)
    grad_up = lax.all_gather(shard_up, "ctx", axis=0, tiled=False)

    def spread(value):
        return jnp.concatenate([value[j] for j in range(nc)], axis=1).astype(F32)

    grad_gate = spread(grad_gate)
    grad_up = spread(grad_up)

    d_normed_ffn = reduce_ctx(
        times_transposed(d_gate, gate_full) + times_transposed(d_up, up_full)
    ).astype(BF)
    d_normed_ffn = both_halves(d_normed_ffn, 1).astype(F32)
    feed = reduce_ctx(times_transposed(hidden, down_full))
    output = both_halves((cut(hidden_state, ti * half, half, 1) + feed).astype(BF), 1)

    unused, norm_pull = jax.vjp(rms_scale, hidden_state, gain_two)
    d_state_norm, grad_gain_two = norm_pull(d_normed_ffn)
    d_state = incoming.astype(F32) + d_state_norm
    d_branch_slab = rows_to_slabs(d_state.astype(BF))
    grad_out = transposed_times(attended_plane, d_branch_slab)
    d_attended = reduce_rows(times_transposed(d_branch_slab, w_out).astype(BF), qcols)
    d_attended = d_attended.astype(BF).reshape(rows * heads, HD)
    d_probs = times_transposed(d_attended, value_all)
    delta = jnp.sum(probs * d_probs, axis=1, keepdims=True)
    d_scores = (probs * (d_probs - delta)).astype(BF)
    d_rows = matmul(d_scores, key_all) * scale
    d_key = transposed_times(d_scores, query_rows) * scale
    d_value = transposed_times(probs_low, d_attended)
    d_key, d_value = d_key.astype(BF), d_value.astype(BF)
    keep = jnp.where(ti == 0, d_key, d_value)
    send = jnp.where(ti == 0, d_value, d_key)
    d_kv = (keep.astype(F32) + swap(send, "tp", nt, 1).astype(F32)).astype(BF)
    d_kv = sum(
        block.astype(F32)
        for block in all_to_all_blocks(list(d_kv.reshape(nc, rows, HD)), "ctx", nc)
    )
    d_kv = jnp.where(ti == 0, unrotate(d_kv, cosine, sine), d_kv).astype(BF)
    d_query = unrotate(d_rows.reshape(rows, heads, HD), cosine[:, None, :], sine[:, None, :])
    d_query = d_query.reshape(rows, qcols).astype(BF)
    d_plane = gather_rows(jnp.concatenate([d_query, d_kv], axis=1))
    d_query_plane = d_plane[:, :qcols]
    d_kv_plane = d_plane[:, qcols:]
    d_normed = tp_sum(
        times_transposed(d_query_plane, w_query) + times_transposed(d_kv_plane, kv_half)
    ).astype(BF)
    d_normed_attn = slabs_to_rows(d_normed).astype(F32)
    grad_query = transposed_times(normed_slab, d_query_plane)
    grad_kv = transposed_times(normed_slab, d_kv_plane)
    unused, norm_pull_one = jax.vjp(rms_scale, inputs, gain_one)
    d_input_norm, grad_gain_one = norm_pull_one(d_normed_attn)
    grad_inputs = d_state + d_input_norm

    grad_out = lax.psum(grad_out.astype(BF), "ctx").astype(F32)
    grad_query = lax.psum(grad_query.astype(BF), "ctx").astype(F32)
    grad_kv = lax.psum(grad_kv.astype(BF), "ctx")
    grad_kv = both_halves(grad_kv, 1).astype(F32)
    gain_grads = jnp.stack([grad_gain_one, grad_gain_two])
    gain_blocks = [cut(gain_grads, (fi ^ k) * slab, slab, 1) for k in range(nf)]
    gain_grads = sum(all_to_all_blocks(gain_blocks, "fsdp", nf))
    step = 1
    while step < nc:
        gain_grads = gain_grads + swap(gain_grads, "ctx", nc, step)
        step *= 2
    return (
        output[None],
        grad_inputs[None],
        grad_query,
        grad_kv,
        grad_out,
        grad_gate,
        grad_up,
        grad_down,
        gain_grads[0],
        gain_grads[1],
    )


def partners(axis, size):
    me = lax.axis_index(axis)
    flip = me + 1 - 2 * lax.rem(me, 2)
    return [me, flip, lax.rem(me + 2, size), size - 1 - me]


class Wire:
    def __init__(self, send, recv):
        self.send, self.recv, self.count, self.live = send, recv, 0, []

    def __call__(self, src, dst, axis, peer):
        slot = self.count
        self.count += 1
        copy = pltpu.make_async_remote_copy(
            src_ref=src,
            dst_ref=dst,
            send_sem=self.send.at[slot],
            recv_sem=self.recv.at[slot],
            device_id={axis: peer},
            device_id_type=MESH,
        )
        copy.start()
        self.live.append(copy)
        return copy

    def settle(self, copies):
        for copy in copies:
            copy.wait_send()
            self.live = [each for each in self.live if each is not copy]

    def finish(self):
        for copy in self.live:
            copy.wait_send()


def greet(peers):
    barrier = pltpu.get_barrier_semaphore()
    for axis, peer in peers:
        pl.semaphore_signal(barrier, inc=1, device_id={axis: peer}, device_id_type=MESH)
    pl.semaphore_wait(barrier, len(peers))


def wide(value, columns):
    return jnp.concatenate([value] * (columns // value.shape[1]), axis=1)


def nt_dot(left, right):
    return lax.dot_general(left, right, (((1,), (1,)), ((), ())), preferred_element_type=F32)


def tn_dot(left, right):
    return lax.dot_general(left, right, (((0,), (0,)), ((), ())), preferred_element_type=F32)


class Gather:
    def __init__(self, wire, fs, pieces, height, place, own=None):
        self.wire, self.fs, self.pieces, self.height = wire, fs, pieces, height
        self.place, self.own = place, own
        self.arrivals = {}

    def strip(self, p):
        return pl.ds(p * self.height, self.height)

    def send(self, m, p, k):
        target = self.place(m, self.fs[0], self.strip(p))
        source = self.own.at[self.strip(p), :] if self.own is not None else target
        self.arrivals[m, p, k] = self.wire(source, target, "fsdp", self.fs[k])

    def pass_on(self, m, p, k, to):
        self.arrivals.pop((m, p, k)).wait_recv()
        target = self.place(m, self.fs[k], self.strip(p))
        self.arrivals[m, p, 3] = self.wire(target, target, "fsdp", self.fs[to])

    def steps(self, which, prepare):
        half = self.pieces // 2
        for m in which:
            prepare(m)
            for i in range(half):
                self.send(m, i, 1)
                self.send(m, half + i, 2)
                yield
            for i in range(half):
                self.pass_on(m, half + i, 2, 1)
                self.pass_on(m, i, 1, 2)
                yield
            for i in range(half):
                self.send(m, half + i, 1)
                self.send(m, i, 2)
                yield

    def settle(self):
        for copy in self.arrivals.values():
            copy.wait_recv()


def middle_kernel(
    w_down,
    shard_down,
    cot_in,
    normed_in,
    gate_in,
    up_in,
    hidden_in,
    gate_w_in,
    up_w_in,
    d_up,
    dn,
    part,
    shard_gate,
    down_all,
    down_rows,
    dfull,
    cot,
    normed,
    gate,
    upward,
    hidden,
    gate_w,
    up_w,
    dh,
    d_gate,
    parts,
    near,
    far,
    sums,
    sems,
    send,
    recv,
    local,
):
    fs, cs = partners("fsdp", 4), partners("ctx", 4)
    ci = lax.axis_index("ctx")
    units, slab = down_rows.shape
    length, _ = cot.shape
    loads = [
        pltpu.make_async_copy(source, target, local.at[n])
        for n, (source, target) in enumerate(
            (
                (w_down.at[pl.ds(pl.multiple_of(ci * units, 64), units), :], down_rows),
                (cot_in, cot),
                (gate_in, gate),
                (up_in, upward),
                (normed_in, normed),
                (gate_w_in, gate_w),
                (up_w_in, up_w),
                (hidden_in, hidden),
            )
        )
    ]
    loads[0].start()
    greet([("fsdp", fs[1]), ("fsdp", fs[2]), ("ctx", cs[1]), ("ctx", cs[3])])
    for load in loads[1:]:
        load.start()
    wire = Wire(send, recv)
    spread = Spread(shard_down, down_all, PIECES, *sems)
    spread.begin()
    for p in range(PIECES):
        spread.give(p)
    gather = Gather(wire, fs, 8, slab // 8, lambda m, index, at: dfull.at[index, at, :])

    def prepare(m):
        loads[0].wait()
        dfull[fs[0]] = down_rows[...].T

    def lanes(index):
        return pl.ds(pl.multiple_of(index * slab, slab), slab)

    for n, _ in enumerate(gather.steps((0,), prepare)):
        if n == 3:
            loads[1].wait()
            dh[...] = jnp.dot(cot[:, lanes(fs[0])], dfull[fs[0]], preferred_element_type=F32)
        if n >= 8:
            spread.hand_on(n - 8)
    for load in loads[2:]:
        load.wait()
    gather.settle()
    for k in (1, 2, 3):
        dh[...] += jnp.dot(cot[:, lanes(fs[k])], dfull[fs[k]], preferred_element_type=F32)
    step = 128
    for n in range(length // step):
        at = slice(n * step, (n + 1) * step)
        v, d = gate[at, :], dh[at, :]
        square = v * v
        t = jnp.tanh(0.7978845608028654 * (v + 0.044715 * (square * v)))
        cdf = 0.5 * (1.0 + t)
        slope = cdf + (0.5 * v) * (1.0 - t * t) * (
            0.7978845608028654 * (1.0 + 0.134145 * square)
        )
        d_gate[at, :] = (d * upward[at, :] * slope).astype(BF)
        d_up[at, :] = (d * (v * cdf)).astype(BF)
    product = Product(wire, False, normed, d_gate, shard_gate, parts, near, far, sums)
    product.start()
    for p in range(PIECES // 2):
        spread.hand_far(p)
    for j in range(4):
        block = nt_dot(d_gate[...], gate_w[j]) + nt_dot(d_up[...], up_w[j])
        dn[:, j * slab : (j + 1) * slab] = block.astype(BF)
    product.middle()
    for p in range(PIECES // 2, PIECES):
        spread.hand_far(p)
    for j in range(4):
        part[:, j * slab : (j + 1) * slab] = nt_dot(hidden[...], dfull[j]).astype(BF)
    product.end()
    spread.close()
    wire.finish()


def call_middle(w_down, shard_down, cot, normed, gate, upward, hidden, gate_w, up_w):
    units, slab = shard_down.shape
    length, depth = cot.shape
    sizes = product_sizes(False, slab, units)
    pair = [pltpu.VMEM((2, *size), BF) for size in sizes]
    single = [pltpu.VMEM(size, BF) for size in sizes]
    shape = jax.ShapeDtypeStruct
    vmem = pl.BlockSpec(memory_space=pltpu.VMEM)
    hbm = pl.BlockSpec(memory_space=pl.ANY)
    return pl.pallas_call(
        middle_kernel,
        out_shape=[
            shape((length, units), BF),
            shape((length, depth), BF),
            shape((length, depth), BF),
            shape((slab, units), BF),
            shape((4, units, slab), BF),
        ],
        in_specs=[hbm] * 9,
        out_specs=[vmem] * 4 + [hbm],
        scratch_shapes=[
            pltpu.VMEM((units, slab), BF),
            pltpu.VMEM((4, slab, units), BF),
            pltpu.VMEM((length, depth), BF),
            pltpu.VMEM((length, depth), BF),
            pltpu.VMEM((length, units), F32),
            pltpu.VMEM((length, units), F32),
            pltpu.VMEM((length, units), BF),
            pltpu.VMEM((4, slab, units), BF),
            pltpu.VMEM((4, slab, units), BF),
            pltpu.VMEM((length, units), F32),
            pltpu.VMEM((length, units), BF),
            list(pair),
            list(pair),
            list(single),
            list(single),
            spread_scratch(PIECES),
            pltpu.SemaphoreType.DMA((32,)),
            pltpu.SemaphoreType.DMA((32,)),
            pltpu.SemaphoreType.DMA((8,)),
        ],
        compiler_params=pltpu.CompilerParams(
            collective_id=2, has_side_effects=True, vmem_limit_bytes=67_043_328
        ),
        cost_estimate=pl.CostEstimate(
            flops=12 * length * depth * units, bytes_accessed=300_000_000, transcendentals=0
        ),
        name="feed_forward_backward",
    )(w_down, shard_down, cot, normed, gate, upward, hidden, gate_w, up_w)


def forward_kernel(
    heads,
    tok,
    cot,
    gains,
    cos,
    sin,
    keep,
    w_q,
    w_kv,
    w_o,
    w_gate,
    w_up,
    q_rot,
    kv_out,
    probs,
    state,
    gains_all,
    normed_all,
    cot_all,
    gate_full,
    up_full,
    normed_slab,
    att_plane,
    gate,
    upward,
    hidden,
    shard,
    xbuf,
    rbuf,
    part,
    precv,
    kvbuf,
    attbuf,
    obuf,
    orecv,
    bbuf,
    brecv,
    nown,
    grel,
    window,
    wfull,
    nall,
    call,
    parts,
    near,
    far,
    sums,
    send,
    recv,
    local,
):
    fs, cs = partners("fsdp", 4), partners("ctx", 4)
    ci, ti = lax.axis_index("ctx"), lax.axis_index("tp")
    other = 1 - ti
    rows, depth = tok.shape
    slab = depth // 4
    hrows = rows // 2
    qcols = heads * HD
    units = gate_full.shape[2]
    scale = HD ** (-0.5)
    wire = Wire(send, recv)
    locals_ = []

    def keep_local(src, dst):
        copy = pltpu.make_async_copy(src, dst, local.at[len(locals_)])
        copy.start()
        locals_.append(copy)
        return copy

    def lanes(index):
        return pl.ds(pl.multiple_of(index * slab, slab), slab)

    mine = pl.ds(pl.multiple_of(ti * hrows, hrows), hrows)
    first = pl.ds(pl.multiple_of(((ci * units) // 128) * 128, 128), window.shape[2])
    win = [
        keep_local(w_gate.at[:, first], window.at[0]),
        keep_local(w_up.at[:, first], window.at[1]),
    ]
    greet(
        [("fsdp", fs[k]) for k in (1, 2, 3)]
        + [("ctx", cs[k]) for k in (1, 2, 3)]
        + [("tp", other)]
    )

    x_in = [None] * 4
    for k in (1, 2, 3):
        x_in[k] = wire(tok.at[:, lanes(fs[k])], xbuf.at[k], "fsdp", fs[k])
    g_in = [None] * 4
    for k in (1, 2, 3):
        g_in[k] = wire(gains, grel.at[k], "fsdp", fs[k])
    grel[0] = gains[...]
    xbuf[0] = tok[:, lanes(fs[0])]
    x = tok[...].astype(F32)
    r = lax.rsqrt(jnp.sum(x * x, axis=1, keepdims=True) * (1.0 / depth) + 1e-06)
    rbuf[0] = jnp.broadcast_to(r, (rows, 128))
    r_in = [None] * 4
    for k in (1, 2, 3):
        r_in[k] = wire(rbuf.at[0], rbuf.at[k], "fsdp", fs[k])
    c_in = [None] * 4
    for k in (1, 2, 3):
        c_in[k] = wire(cot.at[mine, :], call.at[ci, ti], "ctx", cs[k])
    for half in (0, 1):
        call[ci, half] = cot[half * hrows : (half + 1) * hrows, :]

    odd = units % 128
    pieces = 8
    height = slab // pieces

    def prepare(m):
        win[m].wait()
        if odd:

            @pl.when(lax.rem(ci, 2) == 0)
            def _():
                wfull[m, fs[0]] = window[m, :, 0:units]

            @pl.when(lax.rem(ci, 2) == 1)
            def _():
                wfull[m, fs[0]] = window[m, :, odd : odd + units]
        else:
            wfull[m, fs[0]] = window[m, :, 0:units]

    gather = Gather(wire, fs, pieces, height, lambda m, index, at: wfull.at[m, index, at, :])
    schedule = gather.steps((0, 1), prepare)

    def bulk(count):
        for _ in range(count):
            next(schedule, None)

    bulk(BULK[0])
    gain_one = gains[0:1, :]
    kv_half = w_kv[:, pl.ds(pl.multiple_of(ti * HD, HD), HD)]
    p_in = [None] * 4
    for k in range(4):
        if k:
            x_in[k].wait_recv()
            r_in[k].wait_recv()
        normed = (xbuf[k].astype(F32) * wide(rbuf[k], slab) * gain_one).astype(BF)
        normed_slab[k] = normed
        part[k, :, 0:qcols] = jnp.dot(normed, w_q[...], preferred_element_type=F32).astype(BF)
        part[k, :, qcols:] = jnp.dot(normed, kv_half, preferred_element_type=F32).astype(BF)
        if k:
            p_in[k] = wire(part.at[k], precv.at[k], "fsdp", fs[k])
    bulk(BULK[1])
    for k in (1, 2, 3):
        p_in[k].wait_recv()

    def total(start, size):
        out = part[0, :, start : start + size].astype(F32)
        for k in (1, 2, 3):
            out += precv[k, :, start : start + size].astype(F32)
        return out

    c, s = cos[...], sin[...]
    zero = (1 - ti).astype(F32)
    kvbuf[ti, 0] = turn(total(qcols, HD), c * zero + (1.0 - zero), s * zero).astype(BF)
    kv_in = [None] * 4
    for k in (1, 2, 3):
        kv_in[k] = wire(kvbuf.at[ti, 0], kvbuf.at[ti, k], "ctx", cs[k])
    kv_side = [wire(kvbuf.at[ti, 0], kvbuf.at[ti, 0], "tp", other)]
    for h in range(heads):
        q_rot[:, h * HD : (h + 1) * HD] = turn(total(h * HD, HD), c, s).astype(BF)
    bulk(BULK[2])
    for k in (1, 2, 3):
        kv_in[k].wait_recv()
        kv_side.append(wire(kvbuf.at[ti, k], kvbuf.at[ti, k], "tp", other))
    for copy in kv_side:
        copy.wait_recv()
    length = 4 * rows
    keys = kvbuf[0].reshape(length, HD)
    values = kvbuf[1].reshape(length, HD)
    kv_out[...] = kvbuf[...]
    seen = keep[...] > 0.5
    for h in range(heads):
        sc = nt_dot(q_rot[:, h * HD : (h + 1) * HD], keys) * scale
        sc = jnp.where(seen, sc, NEGATIVE)
        e = jnp.exp(sc - jnp.max(sc, axis=1, keepdims=True))
        p = e / jnp.sum(e, axis=1, keepdims=True)
        probs[h] = p
        attbuf[0, :, h * HD : (h + 1) * HD] = jnp.dot(
            p.astype(BF), values, preferred_element_type=F32
        ).astype(BF)
    a_in = [None] * 4
    for k in (1, 2, 3):
        a_in[k] = wire(attbuf.at[0], attbuf.at[k], "fsdp", fs[k])
    bulk(BULK[3])
    c_side = []
    for k in (1, 2, 3):
        c_in[k].wait_recv()
        c_side.append(wire(call.at[cs[k], ti], call.at[cs[k], ti], "tp", other))
    o_in = []
    for k in range(4):
        if k:
            a_in[k].wait_recv()
        att_plane[k] = attbuf[k]
        block = jnp.dot(attbuf[k], w_o[...], preferred_element_type=F32).astype(BF)
        obuf[k, 0] = block[0:hrows]
        obuf[k, 1] = block[hrows:rows]
        o_in.append(wire(obuf.at[k, other], orecv.at[k], "tp", other))
    b_in = [None] * 4
    for k in (1, 2, 3, 0):
        o_in[k].wait_recv()
        both = (obuf[k, ti].astype(F32) + orecv[k].astype(F32)).astype(BF)
        if k:
            bbuf[k] = both
            b_in[k] = wire(bbuf.at[k], brecv.at[k], "fsdp", fs[k])
        else:
            brecv[0] = both
    bulk(BULK[4])
    for k in (1, 2, 3):
        g_in[k].wait_recv()
    gains_all[...] = grel[...]
    squares = jnp.zeros((hrows, 1), F32)
    for k in range(4):
        if k:
            b_in[k].wait_recv()
        h_new = tok[mine, lanes(fs[k])].astype(F32) + brecv[k].astype(F32)
        state[:, lanes(fs[k])] = h_new
        squares += jnp.sum(h_new * h_new, axis=1, keepdims=True)
    r2 = lax.rsqrt(squares * (1.0 / depth) + 1e-06)
    for k in range(4):
        nown[:, lanes(fs[k])] = (state[:, lanes(fs[k])] * r2 * grel[k, 1:2, :]).astype(BF)
    n_in = [None] * 4
    for k in (1, 2, 3):
        n_in[k] = wire(nown, nall.at[ci, ti], "ctx", cs[k])
    n_side = [wire(nown, nall.at[ci, ti], "tp", other)]
    nall[ci, ti] = nown[...]
    bulk(BULK[5])
    for k in (1, 2, 3):
        n_in[k].wait_recv()
        n_side.append(wire(nall.at[cs[k], ti], nall.at[cs[k], ti], "tp", other))
        bulk(BULK[6])
    bulk(1000)
    gather.settle()
    keep_local(wfull.at[0], gate_full)
    keep_local(wfull.at[1], up_full)
    for k in range(4):
        n_side[k].wait_recv()
        x = nall[cs[k]].reshape(rows, depth)
        at = pl.ds(pl.multiple_of(cs[k] * rows, rows), rows)
        g = jnp.dot(x, wfull[0].reshape(depth, units), preferred_element_type=F32)
        u = jnp.dot(x, wfull[1].reshape(depth, units), preferred_element_type=F32)
        gate[at, :] = g
        upward[at, :] = u
        cdf = 0.5 * (1.0 + jnp.tanh(0.7978845608028654 * (g + 0.044715 * (g * g * g))))
        hidden[at, :] = (g * cdf * u).astype(BF)
    keep_local(nall, normed_all)
    for copy in c_side:
        copy.wait_recv()
    keep_local(call, cot_all)
    product = Product(wire, True, hidden, call, shard, parts, near, far, sums)
    product.start()
    product.middle()
    product.end()
    for copy in locals_[2:]:
        copy.wait()
    wire.finish()


BULK = (3, 4, 3, 3, 3, 6, 1)


def call_forward(heads, tok, cot, gains, cos, sin, keep, w_q, w_kv, w_o, w_gate, w_up):
    rows, depth = tok.shape
    slab, hrows, qcols, length = depth // 4, rows // 2, heads * HD, 4 * rows
    units = w_gate.shape[1] // 4
    reach = -(-(units + units % 128) // 128) * 128
    shape = jax.ShapeDtypeStruct
    vmem = pl.BlockSpec(memory_space=pltpu.VMEM)
    hbm = pl.BlockSpec(memory_space=pl.ANY)
    pcols = qcols + HD
    sizes = product_sizes(True, slab, units)
    pair = [pltpu.VMEM((2, *size), BF) for size in sizes]
    single = [pltpu.VMEM(size, BF) for size in sizes]
    return pl.pallas_call(
        functools.partial(forward_kernel, heads),
        out_shape=[
            shape((rows, qcols), BF),
            shape((2, 4, rows, HD), BF),
            shape((heads, rows, length), F32),
            shape((hrows, depth), F32),
            shape((4, 8, slab), F32),
            shape((4, 2, hrows, depth), BF),
            shape((4, 2, hrows, depth), BF),
            shape((4, slab, units), BF),
            shape((4, slab, units), BF),
            shape((4, rows, slab), BF),
            shape((4, rows, qcols), BF),
            shape((length, units), F32),
            shape((length, units), F32),
            shape((length, units), BF),
            shape((units, slab), BF),
        ],
        in_specs=[vmem] * 9 + [hbm] * 2,
        out_specs=[vmem] * 5 + [hbm] * 4 + [vmem] * 6,
        scratch_shapes=[
            pltpu.VMEM((4, rows, slab), BF),
            pltpu.VMEM((4, rows, 128), F32),
            pltpu.VMEM((4, rows, pcols), BF),
            pltpu.VMEM((4, rows, pcols), BF),
            pltpu.VMEM((2, 4, rows, HD), BF),
            pltpu.VMEM((4, rows, qcols), BF),
            pltpu.VMEM((4, 2, hrows, slab), BF),
            pltpu.VMEM((4, hrows, slab), BF),
            pltpu.VMEM((4, hrows, slab), BF),
            pltpu.VMEM((4, hrows, slab), BF),
            pltpu.VMEM((hrows, depth), BF),
            pltpu.VMEM((4, 8, slab), F32),
            pltpu.VMEM((2, slab, reach), BF),
            pltpu.VMEM((2, 4, slab, units), BF),
            pltpu.VMEM((4, 2, hrows, depth), BF),
            pltpu.VMEM((4, 2, hrows, depth), BF),
            list(pair),
            list(pair),
            list(single),
            list(single),
            pltpu.SemaphoreType.DMA((132,)),
            pltpu.SemaphoreType.DMA((132,)),
            pltpu.SemaphoreType.DMA((12,)),
        ],
        compiler_params=pltpu.CompilerParams(
            collective_id=1, has_side_effects=True, vmem_limit_bytes=67_043_328
        ),
        cost_estimate=pl.CostEstimate(
            flops=2 * length * slab * (2 * qcols + HD), bytes_accessed=400_000_000, transcendentals=0
        ),
        name="attention_forward",
    )(tok, cot, gains, cos, sin, keep, w_q, w_kv, w_o, w_gate, w_up)


class Product:
    def __init__(self, wire, flip, left, right, shard, mine, near, far, sums):
        self.wire, self.flip, self.left, self.right, self.shard = wire, flip, left, right, shard
        self.mine, self.near, self.far, self.sums = mine, near, far, sums
        self.fs = partners("fsdp", 4)
        self.slab = shard.shape[1] if flip else shard.shape[0]
        units = shard.shape[0] if flip else shard.shape[1]
        cut = 128 * ((units + 255) // 256)
        self.spans = ((0, cut), (cut, units - cut))
        self.first, self.second = (1, 2), (2, 1)
        self.one, self.two = {}, {}

    def piece(self, k, half):
        start, size = self.spans[half]
        block = pl.ds(pl.multiple_of(self.fs[k] * self.slab, self.slab), self.slab)
        if self.flip:
            right = self.right[..., block]
            right = right.reshape(-1, right.shape[-1])
            return tn_dot(self.left[:, start : start + size], right)
        return tn_dot(self.left[:, block], self.right[:, start : start + size])

    def start(self):
        for slot in (0, 1):
            for half in (0, 1):
                k = 3 if slot == 0 else self.first[half]
                self.mine[half][slot] = self.piece(k, half).astype(BF)
                self.one[half, slot] = self.wire(
                    self.mine[half].at[slot],
                    self.near[half].at[slot],
                    "fsdp",
                    self.fs[self.first[half]],
                )

    def middle(self):
        for half in (0, 1):
            own = self.piece(self.second[half], half)
            self.one[half, 0].wait_recv()
            self.sums[half][...] = (own + self.near[half][0].astype(F32)).astype(BF)
            self.two[half] = self.wire(
                self.sums[half], self.far[half], "fsdp", self.fs[self.second[half]]
            )

    def end(self):
        for half in (0, 1):
            start, size = self.spans[half]
            own = self.piece(0, half)
            self.one[half, 1].wait_recv()
            own += self.near[half][1].astype(F32)
            self.two[half].wait_recv()
            own += self.far[half][...].astype(F32)
            if self.flip:
                self.shard[start : start + size, :] = own.astype(BF)
            else:
                self.shard[:, start : start + size] = own.astype(BF)


def product_sizes(flip, slab, units):
    cut = 128 * ((units + 255) // 256)
    return [(size, slab) if flip else (slab, size) for size in (cut, units - cut)]


def turn(value, c, s):
    front = value[:, 0:128]
    return jnp.concatenate(
        [front * c + pltpu.roll(front, 64, 1) * s, value[:, 128:256]], axis=1
    )


class Line:
    def __init__(self, own, inbox, outbox, total, send, recv):
        self.own, self.inbox, self.outbox, self.total = own, inbox, outbox, total
        self.send, self.recv = send, recv
        self.ci = lax.axis_index("ctx")

    def copy(self, way, u):
        step = 1 if way == 0 else 3
        return pltpu.make_async_remote_copy(
            src_ref=self.outbox.at[way, u - 1 + way],
            dst_ref=self.inbox.at[way, u - 1 + way],
            send_sem=self.send.at[way, u - 1 + way],
            recv_sem=self.recv.at[way, u - 1 + way],
            device_id={"ctx": lax.rem(self.ci + step, 4)},
            device_id_type=MESH,
        )

    def sends(self, way, u):
        return self.ci < u if way == 0 else self.ci > u

    def fed(self, way):
        return self.ci > 0 if way == 0 else self.ci < 3

    def lead(self):
        for step in range(3):
            for way, u in ((0, 3 - step), (1, step)):

                @pl.when(jnp.logical_and(self.sends(way, u), jnp.logical_not(self.fed(way))))
                def _():
                    self.outbox[way, u - 1 + way] = self.own(u).astype(BF)
                    self.copy(way, u).start()

    def hop(self, way, u):
        self.copy(way, u).wait_recv()
        slot = u - 1 + way
        self.outbox[way, slot] = (self.own(u) + self.inbox[way, slot].astype(F32)).astype(BF)
        self.copy(way, u).start()

    def push_near(self):
        @pl.when(self.ci == 1)
        def _():
            self.hop(0, 3)
            self.hop(0, 2)

        @pl.when(self.ci == 2)
        def _():
            self.hop(1, 0)
            self.hop(1, 1)

    def push_far(self):
        @pl.when(self.ci == 1)
        def _():
            self.hop(1, 0)

        @pl.when(self.ci == 2)
        def _():
            self.hop(0, 3)

    def collect(self):
        self.total[...] = self.own(self.ci)
        for way in (0, 1):

            @pl.when(self.fed(way))
            def _():
                self.copy(way, self.ci).wait_recv()
                self.total[...] += self.inbox[way, self.ci - 1 + way].astype(F32)

    def drain(self):
        for way in (0, 1):
            for u in range(1 - way, 4 - way):

                @pl.when(self.sends(way, u))
                def _():
                    self.copy(way, u).wait_send()


def line_scratch(*form):
    return [
        pltpu.VMEM((2, 3, *form), BF),
        pltpu.VMEM((2, 3, *form), BF),
        pltpu.VMEM(form, F32),
        pltpu.SemaphoreType.DMA((2, 3)),
        pltpu.SemaphoreType.DMA((2, 3)),
    ]


class Spread:
    def __init__(self, own, full, pieces, send, recv, local, height=None):
        self.own, self.full, self.pieces = own, full, pieces
        self.send, self.recv = send, recv
        self.height = height or own.shape[0] // pieces
        self.cs = partners("ctx", 4)
        self.ci = self.cs[0]
        self.inner = jnp.logical_and(self.ci > 0, self.ci < 3)
        self.local = local

    def strip(self, p):
        return pl.ds(p * self.height, self.height)

    def copy(self, kind, p, source, peer):
        place = self.full.at[source, self.strip(p), :]
        src = self.own.at[self.strip(p), :] if kind < 2 else place
        slot = (0, 1, 2, 1, 2)[kind]
        return pltpu.make_async_remote_copy(
            src_ref=src,
            dst_ref=place,
            send_sem=self.send.at[kind, p],
            recv_sem=self.recv.at[slot, p],
            device_id={"ctx": peer},
            device_id_type=MESH,
        )

    def out(self, kind, p):
        cs = self.cs
        source = (cs[0], cs[0], cs[1], cs[3], cs[2])[kind]
        peer = (cs[1], cs[3], cs[3], cs[1], cs[1])[kind]
        return self.copy(kind, p, source, peer)

    def arrived(self, slot, p):
        self.copy((0, 1, 2)[slot], p, self.ci, self.cs[1]).wait_recv()

    def keep(self):
        return pltpu.make_async_copy(self.own, self.full.at[self.ci], self.local)

    def begin(self):
        self.keep().start()

    def give(self, p):
        self.out(0, p).start()

        @pl.when(self.inner)
        def _():
            self.out(1, p).start()

    def hand_on(self, p):
        @pl.when(self.inner)
        def _():
            self.arrived(0, p)
            self.out(2, p).start()
            self.arrived(1, p)
            self.out(3, p).start()

    def hand_far(self, p):
        @pl.when(self.inner)
        def _():
            self.arrived(2, p)
            self.out(4, p).start()

    def close(self, near=True, far=True):
        for p in range(self.pieces):

            @pl.when(jnp.logical_not(self.inner))
            def _():
                for slot in range(0 if near else 2, 3 if far else 2):
                    self.arrived(slot, p)

            if near:
                self.out(0, p).wait_send()

            @pl.when(self.inner)
            def _():
                if near and not far:
                    self.arrived(2, p)
                for kind in range(1 if near else 4, 5 if far else 4):
                    self.out(kind, p).wait_send()

        if near:
            self.keep().wait()

    def hand_again(self, p):
        @pl.when(self.inner)
        def _():
            self.out(4, p).start()


def spread_scratch(pieces):
    return [
        pltpu.SemaphoreType.DMA((5, pieces)),
        pltpu.SemaphoreType.DMA((3, pieces)),
        pltpu.SemaphoreType.DMA,
    ]


def units_line(wire, part, side, line_refs, ti):
    other = 1 - ti
    side_in = [wire(part.at[u, other], side.at[u], "tp", other) for u in range(4)]
    for copy in side_in:
        copy.wait_recv()
    return Line(lambda u: part[u, ti].astype(F32) + side[u].astype(F32), *line_refs)


def backward_kernel(
    heads,
    dn,
    cot,
    state,
    gains_all,
    probs,
    q_rot,
    kv,
    cos,
    sin,
    w_o,
    normed,
    att,
    normed_all,
    shard_gate,
    d_up,
    part,
    tok,
    w_q,
    w_kv,
    out,
    grad_tok,
    gain_grads,
    gate_all,
    up_all,
    weights_all,
    side,
    dbuf,
    dslab,
    dpart,
    dfar,
    dkv2,
    kvt,
    zk,
    zfar,
    dqbuf,
    dkvbuf,
    dk_acc,
    dv_acc,
    own_out,
    own_query,
    row_refs,
    out_refs,
    query_refs,
    parts,
    sums,
    product_recv,
    shard_up,
    gate_sems,
    up_sems,
    gpart,
    weight_grads,
    weight_sems,
    last_sems,
    obuf,
    gbuf,
    pbuf,
    pside,
    nbuf,
    nrow,
    gfar,
    gsum,
    gnear,
    gall,
    send,
    recv,
    local,
):
    fs, cs = partners("fsdp", 4), partners("ctx", 4)
    ci, ti = lax.axis_index("ctx"), lax.axis_index("tp")
    other = 1 - ti
    hrows, depth = state.shape
    rows = 2 * hrows
    slab = depth // 4
    length = 4 * rows
    scale = HD ** (-0.5)
    greet(
        [("fsdp", fs[k]) for k in (1, 2, 3)]
        + [("ctx", cs[k]) for k in (1, 2, 3)]
        + [("tp", other)]
    )
    wire = Wire(send, recv)
    mine = pl.ds(pl.multiple_of(ti * hrows, hrows), hrows)

    def lanes(index):
        return pl.ds(pl.multiple_of(index * slab, slab), slab)

    up = Product(wire, False, normed_all, d_up, shard_up, parts, *product_recv, sums)
    gate_line = Spread(shard_gate, gate_all, PIECES, *gate_sems)
    up_line = Spread(shard_up, up_all, PIECES, *up_sems)
    line = units_line(wire, dn, side, row_refs, ti)
    line.lead()
    gate_line.begin()
    for p in range(PIECES // 2):
        gate_line.give(p)
    up.start()
    squares = jnp.zeros((hrows, 1), F32)
    for k in range(4):
        u = state[:, lanes(fs[k])]
        squares += jnp.sum(u * u, axis=1, keepdims=True)
    r = lax.rsqrt(squares * (1.0 / depth) + 1e-06)
    line.push_near()
    line.push_far()
    for p in range(PIECES // 2, PIECES):
        gate_line.give(p)
    up.middle()
    line.collect()
    inner = jnp.zeros((hrows, 1), F32)
    for k in range(4):
        at = lanes(fs[k])
        inner += jnp.sum(
            state[:, at] * gains_all[k, 1:2, :] * line.total[:, at], axis=1, keepdims=True
        )
    pull = r * r * r * (inner * (1.0 / depth))
    d_in = {}
    d_side = {}
    gpart[...] = jnp.zeros_like(gpart)
    for k in (1, 2, 3, 0):
        at = lanes(fs[k])
        u, d = state[:, at], line.total[:, at]
        ds = cot[mine, at].astype(F32) + (r * (gains_all[k, 1:2, :] * d) - u * pull)
        gbuf[ti, :, at] = ds
        if k:
            dbuf[k] = ds.astype(BF)
            d_in[k] = wire(dbuf.at[k], dslab.at[k, ti], "fsdp", fs[k])
        else:
            dslab[0, ti] = ds.astype(BF)
            d_side[0] = wire(dslab.at[0, ti], dslab.at[0, ti], "tp", other)
        gpart[k, 1:2, :] = jnp.sum(u * r * d, axis=0, keepdims=True)
    for k in (1, 2, 3):
        d_in[k].wait_recv()
        d_side[k] = wire(dslab.at[k, ti], dslab.at[k, ti], "tp", other)
    for p in range(PIECES // 2):
        gate_line.hand_on(p)
    a_in = {}
    for k in (1, 2, 3, 0):
        d_side[k].wait_recv()
        block = dslab[k].reshape(rows, slab)
        dpart[k] = nt_dot(block, w_o[...]).astype(BF)
        if k:
            a_in[k] = wire(dpart.at[k], dfar.at[k], "fsdp", fs[k])
    for p in range(PIECES // 2, PIECES):
        gate_line.hand_on(p)
    up.end()
    keys = kv[0].reshape(length, HD)
    values = kv[1].reshape(length, HD)
    c, s = cos[...], sin[...]
    quarter = heads * HD // 4
    branch = dslab[...].reshape(length, slab)
    for u in range(4):
        columns = att[:, :, u * quarter : (u + 1) * quarter].reshape(length, quarter)
        own_out[u] = tn_dot(columns, branch).astype(BF)
    out_line = Line(lambda u: own_out[u].astype(F32), *out_refs)
    for k in (1, 2, 3):
        a_in[k].wait_recv()
    for h in range(heads):
        at = slice(h * HD, (h + 1) * HD)
        d = dpart[0, :, at].astype(F32)
        for k in (1, 2, 3):
            d += dfar[k, :, at].astype(F32)
        d = d.astype(BF)
        p = probs[h]
        dp = nt_dot(d, values)
        delta = jnp.sum(p * dp, axis=1, keepdims=True)
        dsc = (p * (dp - delta)).astype(BF)
        dq = jnp.dot(dsc, keys, preferred_element_type=F32) * scale
        dqbuf[0, :, at] = turn(dq, c, -s).astype(BF)
        dk = tn_dot(dsc, q_rot[:, at])
        dv = tn_dot(p.astype(BF), d)
        if h == 0:
            dk_acc[...] = dk
            dv_acc[...] = dv
        else:
            dk_acc[...] += dk
            dv_acc[...] += dv
    for p in range(PIECES // 2):
        gate_line.hand_far(p)
    dkv2[0] = (dk_acc[...] * scale).astype(BF).reshape(4, rows, HD)
    dkv2[1] = dv_acc[...].astype(BF).reshape(4, rows, HD)
    k_side = wire(dkv2.at[other], kvt, "tp", other)
    q_in = {}
    for k in (1, 2, 3):
        q_in[k] = wire(dqbuf.at[0], dqbuf.at[k], "fsdp", fs[k])
    k_side.wait_recv()
    z_in = {}
    for k in (1, 2, 3):
        zk[k] = (dkv2[ti, k].astype(F32) + kvt[k].astype(F32)).astype(BF)
        z_in[k] = wire(zk.at[k], zfar.at[k], "ctx", cs[k])
    out_line.lead()
    for p in range(PIECES // 2, PIECES):
        gate_line.hand_far(p)
    own = dkv2[ti, 0].astype(F32) + kvt[0].astype(F32)
    for k in (1, 2, 3):
        z_in[k].wait_recv()
        own += zfar[k].astype(F32)
    zero = (1 - ti).astype(F32)
    dkvbuf[0] = turn(own, c * zero + (1.0 - zero), -s * zero).astype(BF)
    v_in = {}
    for k in (1, 2, 3):
        v_in[k] = wire(dkvbuf.at[0], dkvbuf.at[k], "fsdp", fs[k])
    up_line.begin()
    for p in range(PIECES):
        up_line.give(p)
    out_line.push_near()
    for k in (1, 2, 3):
        q_in[k].wait_recv()
    slabs = normed[...].reshape(length, slab)
    for u in (3, 0, 2, 1):
        columns = dqbuf[:, :, u * quarter : (u + 1) * quarter].reshape(length, quarter)
        own_query[u, 0:quarter] = tn_dot(columns, slabs).astype(BF)
    for k in (1, 2, 3):
        v_in[k].wait_recv()
    for u in (3, 0, 2, 1):
        columns = dkvbuf[:, :, u * (HD // 4) : (u + 1) * (HD // 4)].reshape(length, HD // 4)
        own_query[u, quarter:] = tn_dot(columns, slabs).astype(BF)
    query_line = Line(lambda u: own_query[u].astype(F32), *query_refs)
    kv_half = w_kv[:, pl.ds(pl.multiple_of(ti * HD, HD), HD)]
    p_in = {}
    for k in (1, 2, 3, 0):
        block = (nt_dot(dqbuf[k], w_q[...]) + nt_dot(dkvbuf[k], kv_half)).astype(BF)
        pbuf[k, 0] = block[0:hrows]
        pbuf[k, 1] = block[hrows:rows]
        p_in[k] = wire(pbuf.at[k, other], pside.at[k], "tp", other)
    out_line.push_far()
    query_line.lead()
    n_in = {}
    for k in (1, 2, 3, 0):
        p_in[k].wait_recv()
        both = (pbuf[k, ti].astype(F32) + pside[k].astype(F32)).astype(BF)
        if k:
            nbuf[k] = both
            n_in[k] = wire(nbuf.at[k], nrow.at[k], "fsdp", fs[k])
        else:
            nrow[0] = both
    squares = jnp.zeros((hrows, 1), F32)
    for k in range(4):
        u = tok[mine, lanes(fs[k])].astype(F32)
        squares += jnp.sum(u * u, axis=1, keepdims=True)
    r = lax.rsqrt(squares * (1.0 / depth) + 1e-06)
    for p in range(PIECES):
        up_line.hand_on(p)
    line.drain()
    last = units_line(wire, part, side, [*row_refs[:3], *last_sems], ti)
    last.lead()
    for p in range(PIECES // 2):
        up_line.hand_far(p)
    inner = jnp.zeros((hrows, 1), F32)
    for k in range(4):
        if k:
            n_in[k].wait_recv()
        u = tok[mine, lanes(fs[k])].astype(F32)
        inner += jnp.sum(u * gains_all[k, 0:1, :] * nrow[k].astype(F32), axis=1, keepdims=True)
    pull = r * r * r * (inner * (1.0 / depth))
    for k in range(4):
        at = lanes(fs[k])
        u, d = tok[mine, at].astype(F32), nrow[k].astype(F32)
        gbuf[ti, :, at] += (r * (gains_all[k, 0:1, :] * d) - u * pull)
        gpart[k, 0:1, :] = jnp.sum(u * r * d, axis=0, keepdims=True)
    t_side = wire(gbuf.at[ti], gbuf.at[ti], "tp", other)
    g_in = {}
    for k in (1, 2, 3):
        g_in[k] = wire(gpart.at[k], gfar.at[k], "fsdp", fs[k])
    for p in range(PIECES // 2, PIECES):
        up_line.hand_far(p)
    query_line.push_near()
    gain_sum = gpart[0]
    for k in (1, 2, 3):
        g_in[k].wait_recv()
        gain_sum += gfar[k]
    gsum[...] = gain_sum
    near_gain = wire(gsum, gnear, "tp", other)
    near_gain.wait_recv()
    gall[ci] = gain_sum + gnear[...]
    all_gain = [wire(gall.at[ci], gall.at[ci], "ctx", cs[k]) for k in (1, 2, 3)]
    query_line.push_far()
    last.push_near()
    out_line.collect()
    weight_grads[0:quarter, :] = out_line.total[...].astype(BF)
    query_line.collect()
    weight_grads[quarter:, :] = query_line.total[...].astype(BF)
    weight_line = Spread(weight_grads, weights_all, PIECES, *weight_sems)
    weight_line.begin()
    for p in range(PIECES):
        weight_line.give(p)
    last.push_far()
    for p in range(PIECES):
        weight_line.hand_on(p)
    for p in range(PIECES // 2):
        weight_line.hand_far(p)
    last.collect()
    obuf[ti] = (state[...] + last.total[...]).astype(BF)
    o_side = wire(obuf.at[ti], obuf.at[ti], "tp", other)
    for p in range(PIECES // 2, PIECES):
        weight_line.hand_far(p)
    t_side.wait_recv()
    keep_t = pltpu.make_async_copy(gbuf, grad_tok, local.at[0])
    keep_t.start()
    o_side.wait_recv()
    keep_o = pltpu.make_async_copy(obuf, out, local.at[1])
    keep_o.start()
    for copy in all_gain:
        copy.wait_recv()
    gain_grads[...] = gall[0] + gall[1] + gall[2] + gall[3]
    gate_line.close()
    up_line.close()
    weight_line.close()
    for each in (last, out_line, query_line):
        each.drain()
    keep_t.wait()
    keep_o.wait()
    wire.finish()


PIECES = 4


def call_backward(
    heads, dn, cot, state, gains_all, probs, q_rot, kv, cos, sin, w_o, normed, att, normed_all, shard_gate, d_up, part, tok, w_q, w_kv
):
    hrows, depth = state.shape
    rows, slab, qcols = 2 * hrows, depth // 4, heads * HD
    length = 4 * rows
    units = d_up.shape[1]
    sizes = product_sizes(False, slab, units)
    pair = [pltpu.VMEM((2, *size), BF) for size in sizes]
    single = [pltpu.VMEM(size, BF) for size in sizes]
    shape = jax.ShapeDtypeStruct
    vmem = pl.BlockSpec(memory_space=pltpu.VMEM)
    hbm = pl.BlockSpec(memory_space=pl.ANY)
    return pl.pallas_call(
        functools.partial(backward_kernel, heads),
        out_shape=[
            shape((2, hrows, depth), BF),
            shape((2, hrows, depth), F32),
            shape((8, slab), F32),
            shape((4, slab, units), BF),
            shape((4, slab, units), BF),
            shape((4, qcols // 2 + HD // 4, slab), BF),
        ],
        in_specs=[vmem] * 13 + [hbm] + [vmem] * 5,
        out_specs=[hbm] * 2 + [vmem] + [hbm] * 3,
        scratch_shapes=[
            pltpu.VMEM((4, hrows, depth), BF),
            pltpu.VMEM((4, hrows, slab), BF),
            pltpu.VMEM((4, 2, hrows, slab), BF),
            pltpu.VMEM((4, rows, qcols), BF),
            pltpu.VMEM((4, rows, qcols), BF),
            pltpu.VMEM((2, 4, rows, HD), BF),
            pltpu.VMEM((4, rows, HD), BF),
            pltpu.VMEM((4, rows, HD), BF),
            pltpu.VMEM((4, rows, HD), BF),
            pltpu.VMEM((4, rows, qcols), BF),
            pltpu.VMEM((4, rows, HD), BF),
            pltpu.VMEM((length, HD), F32),
            pltpu.VMEM((length, HD), F32),
            pltpu.VMEM((4, qcols // 4, slab), BF),
            pltpu.VMEM((4, (qcols + HD) // 4, slab), BF),
            line_scratch(hrows, depth),
            line_scratch(qcols // 4, slab),
            line_scratch((qcols + HD) // 4, slab),
            list(pair),
            list(single),
            [list(pair), list(single)],
            pltpu.VMEM((slab, units), BF),
            spread_scratch(PIECES),
            spread_scratch(PIECES),
            pltpu.VMEM((4, 8, slab), F32),
            pltpu.VMEM((qcols // 2 + HD // 4, slab), BF),
            spread_scratch(PIECES),
            [pltpu.SemaphoreType.DMA((2, 3)), pltpu.SemaphoreType.DMA((2, 3))],
            pltpu.VMEM((2, hrows, depth), BF),
            pltpu.VMEM((2, hrows, depth), F32),
            pltpu.VMEM((4, 2, hrows, slab), BF),
            pltpu.VMEM((4, hrows, slab), BF),
            pltpu.VMEM((4, hrows, slab), BF),
            pltpu.VMEM((4, hrows, slab), BF),
            pltpu.VMEM((4, 8, slab), F32),
            pltpu.VMEM((8, slab), F32),
            pltpu.VMEM((8, slab), F32),
            pltpu.VMEM((4, 8, slab), F32),
            pltpu.SemaphoreType.DMA((64,)),
            pltpu.SemaphoreType.DMA((64,)),
            pltpu.SemaphoreType.DMA((2,)),
        ],
        compiler_params=pltpu.CompilerParams(
            collective_id=5, has_side_effects=True, vmem_limit_bytes=67_043_328
        ),
        cost_estimate=pl.CostEstimate(
            flops=2 * length * slab * qcols, bytes_accessed=300_000_000, transcendentals=0
        ),
        name="attention_backward",
    )(dn, cot, state, gains_all, probs, q_rot, kv, cos, sin, w_o, normed, att, normed_all, shard_gate, d_up, part, tok, w_q, w_kv)


STRIP = 80


def conversions(sources, targets, inbuf, outbuf, in_sems, out_sems):
    jobs = []
    for which in (0, 1):
        for p in range(sources[which].shape[1] // STRIP):
            jobs.append((which, p))
    for p in range(sources[2].shape[0] // (4 * STRIP)):
        jobs.append((2, p))

    def load(n):
        which, p = jobs[n]
        slot = n % 2
        if which < 2:
            source = sources[which].at[:, pl.ds(p * STRIP, STRIP), :]
            return pltpu.make_async_copy(source, inbuf[0].at[slot], in_sems.at[slot])
        source = sources[2].at[pl.ds(p * 4 * STRIP, 4 * STRIP), :]
        return pltpu.make_async_copy(source, inbuf[1].at[slot], in_sems.at[slot])

    def store(n):
        which, p = jobs[n]
        slot = n % 2
        if which < 2:
            target = targets[which].at[pl.ds(p * STRIP, STRIP), :]
            return pltpu.make_async_copy(outbuf[0].at[slot], target, out_sems.at[slot])
        target = targets[2].at[pl.ds(p * 4 * STRIP, 4 * STRIP), :]
        return pltpu.make_async_copy(outbuf[1].at[slot], target, out_sems.at[slot])

    load(0).start()
    for n, (which, p) in enumerate(jobs):
        slot = n % 2
        if n + 1 < len(jobs):
            load(n + 1).start()
        load(n).wait()
        if n >= 2:
            store(n - 2).wait()
        if which < 2:
            units = sources[which].shape[2]
            for j in range(4):
                outbuf[0][slot, :, j * units : (j + 1) * units] = inbuf[0][slot, j].astype(F32)
        else:
            outbuf[1][slot] = inbuf[1][slot].astype(F32)
        store(n).start()
        if n + 1 == len(jobs):
            store(n - 1).wait()
            store(n).wait()
        yield


def convert_kernel(gate_all, up_all, down_all, grad_gate, grad_up, grad_down, inbuf, outbuf, in_sems, out_sems):
    steps = conversions(
        (gate_all, up_all, down_all), (grad_gate, grad_up, grad_down), inbuf, outbuf, in_sems, out_sems
    )
    for _ in steps:
        pass


def call_convert(gate_all, up_all, down_all):
    slab, units = gate_all.shape[1:]
    shape = jax.ShapeDtypeStruct
    hbm = pl.BlockSpec(memory_space=pl.ANY)
    return pl.pallas_call(
        convert_kernel,
        out_shape=[
            shape((slab, 4 * units), F32),
            shape((slab, 4 * units), F32),
            shape((4 * units, slab), F32),
        ],
        in_specs=[hbm] * 3,
        out_specs=[hbm] * 3,
        scratch_shapes=[
            [pltpu.VMEM((2, 4, STRIP, units), BF), pltpu.VMEM((2, 4 * STRIP, slab), BF)],
            [pltpu.VMEM((2, STRIP, 4 * units), F32), pltpu.VMEM((2, 4 * STRIP, slab), F32)],
            pltpu.SemaphoreType.DMA((2,)),
            pltpu.SemaphoreType.DMA((2,)),
        ],
        cost_estimate=pl.CostEstimate(
            flops=0, bytes_accessed=18 * slab * 4 * units, transcendentals=0
        ),
        name="convert",
    )(gate_all, up_all, down_all)


def fast_device(
    tokens,
    segment_ids,
    w_query,
    w_keyval,
    w_out,
    w_gate,
    w_up,
    w_down,
    gain_attn,
    gain_ffn,
    cotangent,
):
    ci, ti = lax.axis_index("ctx"), lax.axis_index("tp")
    tok, cot = tokens[0], cotangent[0]
    rows, depth = tok.shape
    hrows, slab = rows // 2, depth // 4
    length = segment_ids.shape[1]
    heads = w_query.shape[1] // HD
    units = w_gate.shape[1] // 4

    def cut(value, start, size, axis):
        return lax.dynamic_slice_in_dim(value, start, size, axis)

    segment_row = segment_ids[0]
    local_segment = cut(segment_row, ci * rows, rows, 0)
    local_index = ci * rows + jnp.arange(rows, dtype=jnp.int32)
    earlier = jnp.sum((segment_row[None, :] < local_segment[:, None]).astype(jnp.int32), axis=1)
    position = (local_index - earlier).astype(F32)
    freqs = 10000.0 ** (-(jnp.arange(HD // 4, dtype=F32) * 2.0 / (HD // 2)))
    angle = position[:, None] * freqs[None, :]
    cosine, sine = jnp.cos(angle), jnp.sin(angle)
    cos = jnp.concatenate([cosine, cosine], axis=1)
    sin = jnp.concatenate([-sine, sine], axis=1)
    key_index = jnp.concatenate(
        [(ci ^ k) * rows + jnp.arange(rows, dtype=jnp.int32) for k in range(4)]
    )
    key_segment = jnp.concatenate([cut(segment_row, (ci ^ k) * rows, rows, 0) for k in range(4)])
    keep = (
        (local_segment[:, None] == key_segment[None, :])
        & (key_index[None, :] <= local_index[:, None])
    ).astype(F32)
    gains = jnp.concatenate(
        [gain_attn[None], gain_ffn[None], jnp.zeros((6, slab), gain_attn.dtype)]
    ).astype(F32)

    (
        q_rot,
        kv,
        probs,
        state,
        gains_all,
        normed_all,
        cot_all,
        gate_full,
        up_full,
        normed_slab,
        att_plane,
        gate,
        upward,
        hidden,
        shard_down,
    ) = call_forward(
        heads,
        tok,
        cot,
        gains,
        cos,
        sin,
        keep,
        w_query,
        w_keyval,
        w_out,
        w_gate,
        w_up,
    )
    normed_all = normed_all.reshape(length, depth)
    cot_all = cot_all.reshape(length, depth)
    d_up, dn, part, shard_gate, down_all = call_middle(
        w_down, shard_down, cot_all, normed_all, gate, upward, hidden, gate_full, up_full
    )
    dn = dn.reshape(4, 2, hrows, depth)
    part = part.reshape(4, 2, hrows, depth)
    out, grad_tok, gain_grads, gate_all, up_all, weight_grads = call_backward(
        heads,
        dn,
        cot,
        state,
        gains_all,
        probs,
        q_rot,
        kv,
        cos,
        sin,
        w_out,
        normed_slab,
        att_plane,
        normed_all,
        shard_gate,
        d_up,
        part,
        tok,
        w_query,
        w_keyval,
    )
    grad_gate, grad_up, grad_down = call_convert(
        gate_all, up_all, down_all.reshape(4 * units, slab)
    )
    quarter = heads * HD // 4
    grad_out = weight_grads[:, 0:quarter].reshape(4 * quarter, slab).astype(F32)
    grad_query = weight_grads[:, quarter : 2 * quarter].reshape(4 * quarter, slab).T.astype(F32)
    kv_mine = weight_grads[:, 2 * quarter :].reshape(HD, slab)
    kv_other = swap(kv_mine, "tp", 2, 1)
    grad_kv = jnp.where(
        ti == 0,
        jnp.concatenate([kv_mine, kv_other], axis=0),
        jnp.concatenate([kv_other, kv_mine], axis=0),
    ).T.astype(F32)

    return (
        out.reshape(1, rows, depth),
        grad_tok.reshape(1, rows, depth),
        grad_query,
        grad_kv,
        grad_out,
        grad_gate,
        grad_up,
        grad_down,
        gain_grads[0],
        gain_grads[1],
    )


def solution(mesh):
    sizes = (mesh.shape["fsdp"], mesh.shape["ctx"], mesh.shape["tp"])
    in_specs = (
        P("fsdp", "ctx", None),
        P("fsdp", None),
        P("fsdp", "tp"),
        P("fsdp", None),
        P("tp", "fsdp"),
        P("fsdp", "tp"),
        P("fsdp", "tp"),
        P("tp", "fsdp"),
        P("fsdp"),
        P("fsdp"),
        P("fsdp", "ctx", None),
    )
    out_specs = (
        P("fsdp", "ctx", None),
        P("fsdp", "ctx", None),
        P("fsdp", "tp"),
        P("fsdp", None),
        P("tp", "fsdp"),
        P("fsdp", "tp"),
        P("fsdp", "tp"),
        P("tp", "fsdp"),
        P("fsdp"),
        P("fsdp"),
    )

    def body(*args):
        rows, depth = args[0].shape[1:]
        fits = sizes == (4, 4, 2) and depth % 512 == 0 and rows % 32 == 0
        if fits:
            return fast_device(*args)
        return per_device(sizes, *args)

    return jax.shard_map(
        body, mesh=mesh, in_specs=in_specs, out_specs=out_specs, check_vma=False
    )
```

```python
import functools

import jax
import jax.numpy as jnp
from jax import lax
from jax.experimental import pallas as pl
from jax.experimental.pallas import tpu as pltpu
from jax.sharding import PartitionSpec as P

HD = 256
NEGATIVE = -1e30
BF = jnp.bfloat16
F32 = jnp.float32
MESH = pl.DeviceIdType.MESH


def rms_scale(value, gain):
    return value * lax.rsqrt(jnp.mean(value * value, axis=-1, keepdims=True) + 1e-06) * gain


def rotate(value, cosine, sine):
    quarter = value.shape[-1] // 4
    first = value[..., :quarter]
    second = value[..., quarter : 2 * quarter]
    rest = value[..., 2 * quarter :]
    return jnp.concatenate(
        [first * cosine - second * sine, second * cosine + first * sine, rest], axis=-1
    )


def unrotate(value, cosine, sine):
    return rotate(value, cosine, -sine)


def matmul(left, right):
    return jnp.dot(left, right, preferred_element_type=F32)


def times_transposed(left, right):
    return lax.dot_general(left, right, (((1,), (1,)), ((), ())), preferred_element_type=F32)


def transposed_times(left, right):
    return lax.dot_general(left, right, (((0,), (0,)), ((), ())), preferred_element_type=F32)


def geglu(gate_in, up_in):
    return jax.nn.gelu(gate_in, approximate=True) * up_in


def swap(value, axis, size, k):
    return lax.ppermute(value, axis, [(i, i ^ k) for i in range(size)])


def per_device(
    sizes,
    tokens,
    segment_ids,
    w_query,
    w_keyval,
    w_out,
    w_gate,
    w_up,
    w_down,
    gain_attn,
    gain_ffn,
    cotangent,
):
    nf, nc, nt = sizes
    fi, ci, ti = lax.axis_index("fsdp"), lax.axis_index("ctx"), lax.axis_index("tp")
    rows = tokens.shape[1]
    depth = tokens.shape[2]
    slab = depth // nf
    half = depth // nt
    heads = w_query.shape[1] // HD
    qcols = heads * HD
    units = w_gate.shape[1] // nc
    scale = HD ** (-0.5)

    def cut(value, start, size, axis):
        return lax.dynamic_slice_in_dim(value, start, size, axis)

    def all_to_all_blocks(blocks, axis, size):
        return [blocks[0]] + [swap(blocks[k], axis, size, k) for k in range(1, size)]

    def gather_blocks(value, axis, size):
        return [value] + [swap(value, axis, size, k) for k in range(1, size)]

    def absolute(blocks, index, axis):
        stacked = jnp.stack(blocks)
        size = len(blocks)
        return jnp.concatenate(
            [lax.dynamic_index_in_dim(stacked, j ^ index, 0, keepdims=False) for j in range(size)],
            axis=axis,
        )

    def rows_to_slabs(value):
        blocks = [cut(value, (fi ^ k) * slab, slab, 1) for k in range(nf)]
        return jnp.concatenate(all_to_all_blocks(blocks, "fsdp", nf), axis=0)

    def slabs_to_rows(value):
        blocks = list(value.reshape(nf, rows, slab))
        return absolute(all_to_all_blocks(blocks, "fsdp", nf), fi, 1)

    def reduce_rows(value, width):
        blocks = list(value.reshape(nf, rows, width))
        got = all_to_all_blocks(blocks, "fsdp", nf)
        return sum(block.astype(F32) for block in got)

    def gather_rows(value):
        return jnp.concatenate(gather_blocks(value, "fsdp", nf), axis=0)

    def both_halves(mine, axis):
        other = swap(mine, "tp", nt, 1)
        return jnp.where(
            ti == 0,
            jnp.concatenate([mine, other], axis=axis),
            jnp.concatenate([other, mine], axis=axis),
        )

    def tp_sum(value):
        low = value.astype(BF)
        return low.astype(F32) + swap(low, "tp", nt, 1).astype(F32)

    def gather_ctx(value):
        mine = cut(value, ti * half, half, 1)
        return both_halves(jnp.concatenate(gather_blocks(mine, "ctx", nc), axis=0), 1)

    def reduce_ctx(value):
        low = value.astype(BF)
        keep = cut(low, ti * half, half, 1)
        send = cut(low, (1 - ti) * half, half, 1)
        both = (keep.astype(F32) + swap(send, "tp", nt, 1).astype(F32)).astype(BF)
        got = all_to_all_blocks(list(both.reshape(nc, rows, half)), "ctx", nc)
        return sum(block.astype(F32) for block in got)

    gate_full = lax.all_gather(cut(w_gate, ci * units, units, 1), "fsdp", axis=0, tiled=True)
    up_full = lax.all_gather(cut(w_up, ci * units, units, 1), "fsdp", axis=0, tiled=True)
    down_full = lax.all_gather(
        cut(w_down, ci * units, units, 0).T, "fsdp", axis=0, tiled=True
    )

    gains = jnp.stack([gain_attn, gain_ffn])
    gains = absolute(gather_blocks(gains, "fsdp", nf), fi, 1).astype(F32)
    gain_one, gain_two = gains[0], gains[1]
    inputs = tokens[0].astype(F32)
    incoming = cotangent[0]

    segment_row = segment_ids[0]
    offset = ci * rows
    local_segment = lax.dynamic_slice_in_dim(segment_row, offset, rows, 0)
    local_index = offset + jnp.arange(rows, dtype=jnp.int32)
    earlier = jnp.sum((segment_row[None, :] < local_segment[:, None]).astype(jnp.int32), axis=1)
    position = (local_index - earlier).astype(F32)
    freqs = 10000.0 ** (-(jnp.arange(HD // 4, dtype=F32) * 2.0 / (HD // 2)))
    angle = position[:, None] * freqs[None, :]
    cosine = jnp.cos(angle)
    sine = jnp.sin(angle)

    normed_attn = rms_scale(inputs, gain_one).astype(BF)
    normed_slab = rows_to_slabs(normed_attn)
    kv_half = cut(w_keyval, ti * HD, HD, 1)
    partial = jnp.concatenate(
        [matmul(normed_slab, w_query).astype(BF), matmul(normed_slab, kv_half).astype(BF)], axis=1
    )
    projected = reduce_rows(partial, qcols + HD)
    query = projected[:, :qcols].reshape(rows, heads, HD)
    keyval = projected[:, qcols:]
    query_rows = (
        rotate(query, cosine[:, None, :], sine[:, None, :]).reshape(rows * heads, HD).astype(BF)
    )
    keyval = jnp.where(ti == 0, rotate(keyval, cosine, sine), keyval).astype(BF)
    kv_all = jnp.concatenate(gather_blocks(keyval, "ctx", nc), axis=0)
    kv_other = swap(kv_all, "tp", nt, 1)
    key_all = jnp.where(ti == 0, kv_all, kv_other)
    value_all = jnp.where(ti == 0, kv_other, kv_all)

    key_index = jnp.concatenate(
        [(ci ^ k) * rows + jnp.arange(rows, dtype=jnp.int32) for k in range(nc)]
    )
    key_segment = jnp.concatenate(
        [lax.dynamic_slice_in_dim(segment_row, (ci ^ k) * rows, rows, 0) for k in range(nc)]
    )
    row_index = jnp.repeat(local_index, heads)
    row_segment = jnp.repeat(local_segment, heads)
    mask = (row_segment[:, None] == key_segment[None, :]) & (
        key_index[None, :] <= row_index[:, None]
    )
    scores = jnp.where(mask, times_transposed(query_rows, key_all) * scale, NEGATIVE)
    peak = jnp.max(scores, axis=1, keepdims=True)
    terms = jnp.exp(scores - peak)
    probs = terms / jnp.sum(terms, axis=1, keepdims=True)
    probs_low = probs.astype(BF)
    attended = matmul(probs_low, value_all).reshape(rows, qcols).astype(BF)

    attended_plane = gather_rows(attended)
    branch = tp_sum(matmul(attended_plane, w_out)).astype(BF)
    hidden_state = inputs + slabs_to_rows(branch).astype(F32)
    normed_ffn = rms_scale(hidden_state, gain_two).astype(BF)

    normed_all = gather_ctx(normed_ffn)
    incoming_all = gather_ctx(incoming)
    gate = matmul(normed_all, gate_full)
    upward = matmul(normed_all, up_full)
    d_hidden = matmul(incoming_all, down_full)
    hidden, geglu_pull = jax.vjp(geglu, gate, upward)
    hidden = hidden.astype(BF)
    d_gate, d_up = geglu_pull(d_hidden)
    d_gate = d_gate.astype(BF)
    d_up = d_up.astype(BF)

    def finish(grad, axis):
        low = grad.astype(BF)
        blocks = [cut(low, (fi ^ k) * slab, slab, axis) for k in range(nf)]
        got = all_to_all_blocks(blocks, "fsdp", nf)
        return sum(block.astype(F32) for block in got).astype(BF)

    shard_down = finish(transposed_times(hidden, incoming_all), 1)
    grad_down = lax.all_gather(shard_down, "ctx", axis=0, tiled=True).astype(F32)
    shard_gate = finish(transposed_times(normed_all, d_gate), 0)
    grad_gate = lax.all_gather(shard_gate, "ctx", axis=0, tiled=False)
    shard_up = finish(transposed_times(normed_all, d_up), 0)
    grad_up = lax.all_gather(shard_up, "ctx", axis=0, tiled=False)

    def spread(value):
        return jnp.concatenate([value[j] for j in range(nc)], axis=1).astype(F32)

    grad_gate = spread(grad_gate)
    grad_up = spread(grad_up)

    d_normed_ffn = reduce_ctx(
        times_transposed(d_gate, gate_full) + times_transposed(d_up, up_full)
    ).astype(BF)
    d_normed_ffn = both_halves(d_normed_ffn, 1).astype(F32)
    feed = reduce_ctx(times_transposed(hidden, down_full))
    output = both_halves((cut(hidden_state, ti * half, half, 1) + feed).astype(BF), 1)

    unused, norm_pull = jax.vjp(rms_scale, hidden_state, gain_two)
    d_state_norm, grad_gain_two = norm_pull(d_normed_ffn)
    d_state = incoming.astype(F32) + d_state_norm
    d_branch_slab = rows_to_slabs(d_state.astype(BF))
    grad_out = transposed_times(attended_plane, d_branch_slab)
    d_attended = reduce_rows(times_transposed(d_branch_slab, w_out).astype(BF), qcols)
    d_attended = d_attended.astype(BF).reshape(rows * heads, HD)
    d_probs = times_transposed(d_attended, value_all)
    delta = jnp.sum(probs * d_probs, axis=1, keepdims=True)
    d_scores = (probs * (d_probs - delta)).astype(BF)
    d_rows = matmul(d_scores, key_all) * scale
    d_key = transposed_times(d_scores, query_rows) * scale
    d_value = transposed_times(probs_low, d_attended)
    d_key, d_value = d_key.astype(BF), d_value.astype(BF)
    keep = jnp.where(ti == 0, d_key, d_value)
    send = jnp.where(ti == 0, d_value, d_key)
    d_kv = (keep.astype(F32) + swap(send, "tp", nt, 1).astype(F32)).astype(BF)
    d_kv = sum(
        block.astype(F32)
        for block in all_to_all_blocks(list(d_kv.reshape(nc, rows, HD)), "ctx", nc)
    )
    d_kv = jnp.where(ti == 0, unrotate(d_kv, cosine, sine), d_kv).astype(BF)
    d_query = unrotate(d_rows.reshape(rows, heads, HD), cosine[:, None, :], sine[:, None, :])
    d_query = d_query.reshape(rows, qcols).astype(BF)
    d_plane = gather_rows(jnp.concatenate([d_query, d_kv], axis=1))
    d_query_plane = d_plane[:, :qcols]
    d_kv_plane = d_plane[:, qcols:]
    d_normed = tp_sum(
        times_transposed(d_query_plane, w_query) + times_transposed(d_kv_plane, kv_half)
    ).astype(BF)
    d_normed_attn = slabs_to_rows(d_normed).astype(F32)
    grad_query = transposed_times(normed_slab, d_query_plane)
    grad_kv = transposed_times(normed_slab, d_kv_plane)
    unused, norm_pull_one = jax.vjp(rms_scale, inputs, gain_one)
    d_input_norm, grad_gain_one = norm_pull_one(d_normed_attn)
    grad_inputs = d_state + d_input_norm

    grad_out = lax.psum(grad_out.astype(BF), "ctx").astype(F32)
    grad_query = lax.psum(grad_query.astype(BF), "ctx").astype(F32)
    grad_kv = lax.psum(grad_kv.astype(BF), "ctx")
    grad_kv = both_halves(grad_kv, 1).astype(F32)
    gain_grads = jnp.stack([grad_gain_one, grad_gain_two])
    gain_blocks = [cut(gain_grads, (fi ^ k) * slab, slab, 1) for k in range(nf)]
    gain_grads = sum(all_to_all_blocks(gain_blocks, "fsdp", nf))
    step = 1
    while step < nc:
        gain_grads = gain_grads + swap(gain_grads, "ctx", nc, step)
        step *= 2
    return (
        output[None],
        grad_inputs[None],
        grad_query,
        grad_kv,
        grad_out,
        grad_gate,
        grad_up,
        grad_down,
        gain_grads[0],
        gain_grads[1],
    )


def partners(axis, size):
    me = lax.axis_index(axis)
    flip = me + 1 - 2 * lax.rem(me, 2)
    return [me, flip, lax.rem(me + 2, size), size - 1 - me]


class Wire:
    def __init__(self, send, recv):
        self.send, self.recv, self.count, self.live = send, recv, 0, []

    def __call__(self, src, dst, axis, peer):
        slot = self.count
        self.count += 1
        copy = pltpu.make_async_remote_copy(
            src_ref=src,
            dst_ref=dst,
            send_sem=self.send.at[slot],
            recv_sem=self.recv.at[slot],
            device_id={axis: peer},
            device_id_type=MESH,
        )
        copy.start()
        self.live.append(copy)
        return copy

    def settle(self, copies):
        for copy in copies:
            copy.wait_send()
            self.live = [each for each in self.live if each is not copy]

    def finish(self):
        for copy in self.live:
            copy.wait_send()


def greet(peers):
    barrier = pltpu.get_barrier_semaphore()
    for axis, peer in peers:
        pl.semaphore_signal(barrier, inc=1, device_id={axis: peer}, device_id_type=MESH)
    pl.semaphore_wait(barrier, len(peers))


def wide(value, columns):
    return jnp.concatenate([value] * (columns // value.shape[1]), axis=1)


def nt_dot(left, right):
    return lax.dot_general(left, right, (((1,), (1,)), ((), ())), preferred_element_type=F32)


def tn_dot(left, right):
    return lax.dot_general(left, right, (((0,), (0,)), ((), ())), preferred_element_type=F32)


class Gather:
    def __init__(self, wire, fs, pieces, height, place, own=None):
        self.wire, self.fs, self.pieces, self.height = wire, fs, pieces, height
        self.place, self.own = place, own
        self.arrivals = {}

    def strip(self, p):
        return pl.ds(p * self.height, self.height)

    def send(self, m, p, k):
        target = self.place(m, self.fs[0], self.strip(p))
        source = self.own.at[self.strip(p), :] if self.own is not None else target
        self.arrivals[m, p, k] = self.wire(source, target, "fsdp", self.fs[k])

    def pass_on(self, m, p, k, to):
        self.arrivals.pop((m, p, k)).wait_recv()
        target = self.place(m, self.fs[k], self.strip(p))
        self.arrivals[m, p, 3] = self.wire(target, target, "fsdp", self.fs[to])

    def steps(self, which, prepare):
        half = self.pieces // 2
        for m in which:
            prepare(m)
            for i in range(half):
                self.send(m, i, 1)
                self.send(m, half + i, 2)
                yield
            for i in range(half):
                self.pass_on(m, half + i, 2, 1)
                self.pass_on(m, i, 1, 2)
                yield
            for i in range(half):
                self.send(m, half + i, 1)
                self.send(m, i, 2)
                yield

    def settle(self):
        for copy in self.arrivals.values():
            copy.wait_recv()


def middle_kernel(
    w_down,
    shard_down,
    cot_in,
    normed_in,
    gate_in,
    up_in,
    hidden_in,
    gate_w_in,
    up_w_in,
    d_up,
    dn,
    part,
    shard_gate,
    down_all,
    dfull,
    cot,
    normed,
    gate,
    upward,
    hidden,
    gate_w,
    up_w,
    dh,
    d_gate,
    parts,
    near,
    far,
    sums,
    sems,
    send,
    recv,
    local,
):
    fs, cs = partners("fsdp", 4), partners("ctx", 4)
    ci = lax.axis_index("ctx")
    units, slab = dfull.shape[1:]
    length, _ = cot.shape
    loads = [
        pltpu.make_async_copy(source, target, local.at[n])
        for n, (source, target) in enumerate(
            (
                (w_down.at[pl.ds(pl.multiple_of(ci * units, 64), units), :], dfull.at[fs[0]]),
                (cot_in, cot),
                (gate_in, gate),
                (up_in, upward),
                (normed_in, normed),
                (gate_w_in, gate_w),
                (up_w_in, up_w),
                (hidden_in, hidden),
            )
        )
    ]
    loads[0].start()
    greet([("fsdp", fs[1]), ("fsdp", fs[2]), ("ctx", cs[1]), ("ctx", cs[3])])
    for load in loads[1:]:
        load.start()
    wire = Wire(send, recv)
    spread = Spread(shard_down, down_all, PIECES, *sems)
    spread.begin()
    for p in range(PIECES):
        spread.give(p)
    gather = Gather(wire, fs, 10, units // 10, lambda m, index, at: dfull.at[index, at, :])

    def prepare(m):
        loads[0].wait()

    def lanes(index):
        return pl.ds(pl.multiple_of(index * slab, slab), slab)

    for n, _ in enumerate(gather.steps((0,), prepare)):
        if n == 3:
            loads[1].wait()
            dh[...] = nt_dot(cot[:, lanes(fs[0])], dfull[fs[0]])
        if n >= 15 - PIECES:
            spread.hand_on(n - 15 + PIECES)
    for load in loads[2:]:
        load.wait()
    gather.settle()
    for k in (1, 2, 3):
        dh[...] += nt_dot(cot[:, lanes(fs[k])], dfull[fs[k]])
    step = 128
    for n in range(length // step):
        at = slice(n * step, (n + 1) * step)
        v, d = gate[at, :], dh[at, :]
        square = v * v
        t = jnp.tanh(0.7978845608028654 * (v + 0.044715 * (square * v)))
        cdf = 0.5 * (1.0 + t)
        slope = cdf + (0.5 * v) * (1.0 - t * t) * (
            0.7978845608028654 * (1.0 + 0.134145 * square)
        )
        d_gate[at, :] = (d * upward[at, :] * slope).astype(BF)
        d_up[at, :] = (d * (v * cdf)).astype(BF)
    product = Product(wire, True, d_gate, normed, shard_gate, parts, near, far, sums)
    product.start()
    for p in range(PIECES // 2):
        spread.hand_far(p)
    for j in range(4):
        block = jnp.dot(d_gate[...], gate_w[j], preferred_element_type=F32)
        block += jnp.dot(d_up[...], up_w[j], preferred_element_type=F32)
        dn[:, j * slab : (j + 1) * slab] = block.astype(BF)
    product.middle()
    for p in range(PIECES // 2, PIECES):
        spread.hand_far(p)
    for j in range(4):
        part[:, j * slab : (j + 1) * slab] = jnp.dot(
            hidden[...], dfull[j], preferred_element_type=F32
        ).astype(BF)
    product.end()
    spread.close()
    wire.finish()


def call_middle(w_down, shard_down, cot, normed, gate, upward, hidden, gate_w, up_w):
    units, slab = shard_down.shape
    length, depth = cot.shape
    sizes = product_sizes(True, slab, units)
    pair = [pltpu.VMEM((2, *size), BF) for size in sizes]
    single = [pltpu.VMEM(size, BF) for size in sizes]
    shape = jax.ShapeDtypeStruct
    vmem = pl.BlockSpec(memory_space=pltpu.VMEM)
    hbm = pl.BlockSpec(memory_space=pl.ANY)
    return pl.pallas_call(
        middle_kernel,
        out_shape=[
            shape((length, units), BF),
            shape((length, depth), BF),
            shape((length, depth), BF),
            shape((units, slab), BF),
            shape((4, units, slab), BF),
        ],
        in_specs=[hbm] * 9,
        out_specs=[vmem] * 4 + [hbm],
        scratch_shapes=[
            pltpu.VMEM((4, units, slab), BF),
            pltpu.VMEM((length, depth), BF),
            pltpu.VMEM((length, depth), BF),
            pltpu.VMEM((length, units), F32),
            pltpu.VMEM((length, units), F32),
            pltpu.VMEM((length, units), BF),
            pltpu.VMEM((4, units, slab), BF),
            pltpu.VMEM((4, units, slab), BF),
            pltpu.VMEM((length, units), F32),
            pltpu.VMEM((length, units), BF),
            list(pair),
            list(pair),
            list(single),
            list(single),
            spread_scratch(PIECES),
            pltpu.SemaphoreType.DMA((40,)),
            pltpu.SemaphoreType.DMA((40,)),
            pltpu.SemaphoreType.DMA((8,)),
        ],
        compiler_params=pltpu.CompilerParams(
            collective_id=2, has_side_effects=True, vmem_limit_bytes=67_043_328
        ),
        cost_estimate=pl.CostEstimate(
            flops=12 * length * depth * units, bytes_accessed=300_000_000, transcendentals=0
        ),
        name="feed_forward_backward",
    )(w_down, shard_down, cot, normed, gate, upward, hidden, gate_w, up_w)


def forward_kernel(
    heads,
    tok,
    cot,
    gains,
    cos,
    sin,
    keep,
    w_q,
    w_kv,
    w_o,
    w_gate,
    w_up,
    q_rot,
    kv_out,
    probs,
    state,
    gains_all,
    normed_all,
    cot_all,
    gate_full,
    up_full,
    normed_slab,
    att_plane,
    gate,
    upward,
    hidden,
    shard,
    xbuf,
    rbuf,
    part,
    precv,
    kvbuf,
    attbuf,
    obuf,
    orecv,
    bbuf,
    brecv,
    nown,
    grel,
    window,
    wfull,
    nall,
    call,
    parts,
    near,
    far,
    sums,
    send,
    recv,
    local,
):
    fs, cs = partners("fsdp", 4), partners("ctx", 4)
    ci, ti = lax.axis_index("ctx"), lax.axis_index("tp")
    other = 1 - ti
    rows, depth = tok.shape
    slab = depth // 4
    hrows = rows // 2
    qcols = heads * HD
    units = gate_full.shape[1]
    scale = HD ** (-0.5)
    wire = Wire(send, recv)
    locals_ = []

    def keep_local(src, dst):
        copy = pltpu.make_async_copy(src, dst, local.at[len(locals_)])
        copy.start()
        locals_.append(copy)
        return copy

    def lanes(index):
        return pl.ds(pl.multiple_of(index * slab, slab), slab)

    mine = pl.ds(pl.multiple_of(ti * hrows, hrows), hrows)
    first = pl.ds(pl.multiple_of(((ci * units) // 128) * 128, 128), window.shape[2])
    win = [
        keep_local(w_gate.at[:, first], window.at[0]),
        keep_local(w_up.at[:, first], window.at[1]),
    ]
    greet(
        [("fsdp", fs[k]) for k in (1, 2, 3)]
        + [("ctx", cs[k]) for k in (1, 2, 3)]
        + [("tp", other)]
    )

    x_in = [None] * 4
    for k in (1, 2, 3):
        x_in[k] = wire(tok.at[mine, lanes(fs[k])], xbuf.at[k, mine, :], "fsdp", fs[k])
    g_in = [None] * 4
    for k in (1, 2, 3):
        g_in[k] = wire(gains, grel.at[k], "fsdp", fs[k])
    grel[0] = gains[...]
    xbuf[0] = tok[:, lanes(fs[0])]
    x = tok[...].astype(F32)
    r = lax.rsqrt(jnp.sum(x * x, axis=1, keepdims=True) * (1.0 / depth) + 1e-06)
    rbuf[0] = jnp.broadcast_to(r, (rows, 128))
    r_in = [None] * 4
    for k in (1, 2, 3):
        r_in[k] = wire(rbuf.at[0, mine, :], rbuf.at[k, mine, :], "fsdp", fs[k])
    c_in = [None] * 4
    for k in (1, 2, 3):
        c_in[k] = wire(cot.at[mine, :], call.at[ci, ti], "ctx", cs[k])
    for half in (0, 1):
        call[ci, half] = cot[half * hrows : (half + 1) * hrows, :]

    odd = units % 128
    pieces = 10
    height = units // pieces

    def prepare(m):
        win[m].wait()
        if odd:

            @pl.when(lax.rem(ci, 2) == 0)
            def _():
                wfull[m, fs[0]] = window[m, :, 0:units].T

            @pl.when(lax.rem(ci, 2) == 1)
            def _():
                wfull[m, fs[0]] = window[m, :, odd : odd + units].T
        else:
            wfull[m, fs[0]] = window[m, :, 0:units].T

    gather = Gather(wire, fs, pieces, height, lambda m, index, at: wfull.at[m, index, at, :])
    schedule = gather.steps((0, 1), prepare)

    def bulk(count):
        for _ in range(count):
            next(schedule, None)

    bulk(BULK[0])
    gain_one = gains[0:1, :]
    kv_half = w_kv[:, pl.ds(pl.multiple_of(ti * HD, HD), HD)]
    p_in = [None] * 4
    pass_x = {}
    for k in range(4):
        if k == 1:
            for j in (1, 2, 3):
                x_in[j].wait_recv()
                r_in[j].wait_recv()
                for buffer in (xbuf, rbuf):
                    half = buffer.at[j, mine, :]
                    pass_x[j, buffer is rbuf] = wire(half, half, "tp", other)
        if k:
            pass_x[k, False].wait_recv()
            pass_x[k, True].wait_recv()
        normed = (xbuf[k].astype(F32) * wide(rbuf[k], slab) * gain_one).astype(BF)
        normed_slab[k] = normed
        part[k, :, 0:qcols] = jnp.dot(normed, w_q[...], preferred_element_type=F32).astype(BF)
        part[k, :, qcols:] = jnp.dot(normed, kv_half, preferred_element_type=F32).astype(BF)
        if k:
            p_in[k] = wire(part.at[k], precv.at[k], "fsdp", fs[k])
    bulk(BULK[1])
    for k in (1, 2, 3):
        p_in[k].wait_recv()

    def total(start, size):
        out = part[0, :, start : start + size].astype(F32)
        for k in (1, 2, 3):
            out += precv[k, :, start : start + size].astype(F32)
        return out

    c, s = cos[...], sin[...]
    zero = (1 - ti).astype(F32)
    kvbuf[ti, 0] = turn(total(qcols, HD), c * zero + (1.0 - zero), s * zero).astype(BF)
    kv_in = [None] * 4
    for k in (1, 2, 3):
        kv_in[k] = wire(kvbuf.at[ti, 0], kvbuf.at[ti, k], "ctx", cs[k])
    kv_side = [wire(kvbuf.at[ti, 0], kvbuf.at[ti, 0], "tp", other)]
    for h in range(heads):
        q_rot[:, h * HD : (h + 1) * HD] = turn(total(h * HD, HD), c, s).astype(BF)
    bulk(BULK[2])
    for k in (1, 2, 3):
        kv_in[k].wait_recv()
        kv_side.append(wire(kvbuf.at[ti, k], kvbuf.at[ti, k], "tp", other))
    for copy in kv_side:
        copy.wait_recv()
    length = 4 * rows
    keys = kvbuf[0].reshape(length, HD)
    values = kvbuf[1].reshape(length, HD)
    kv_out[...] = kvbuf[...]
    seen = keep[...] > 0.5
    for h in range(heads):
        sc = nt_dot(q_rot[:, h * HD : (h + 1) * HD], keys) * scale
        sc = jnp.where(seen, sc, NEGATIVE)
        e = jnp.exp(sc - jnp.max(sc, axis=1, keepdims=True))
        p = e / jnp.sum(e, axis=1, keepdims=True)
        probs[h] = p
        attbuf[0, :, h * HD : (h + 1) * HD] = jnp.dot(
            p.astype(BF), values, preferred_element_type=F32
        ).astype(BF)
    a_in = {}
    for k in (1, 2):
        a_in[k] = wire(attbuf.at[0], attbuf.at[k], "fsdp", fs[k])
    bulk(BULK[3])
    c_side = []
    for k in (1, 2, 3):
        c_in[k].wait_recv()
        c_side.append(wire(call.at[cs[k], ti], call.at[cs[k], ti], "tp", other))
    o_in = []
    for k in range(4):
        if k == 1:
            for j, to, start in ((1, 2, 0), (2, 1, hrows)):
                a_in[j].wait_recv()
                a_in[3, j] = wire(
                    attbuf.at[j, pl.ds(start, hrows), :],
                    attbuf.at[3, pl.ds(start, hrows), :],
                    "fsdp",
                    fs[to],
                )
        if k == 3:
            a_in[3, 1].wait_recv()
            a_in[3, 2].wait_recv()
        att_plane[k] = attbuf[k]
        block = jnp.dot(attbuf[k], w_o[...], preferred_element_type=F32).astype(BF)
        obuf[k, 0] = block[0:hrows]
        obuf[k, 1] = block[hrows:rows]
        o_in.append(wire(obuf.at[k, other], orecv.at[k], "tp", other))
    b_in = [None] * 4
    for k in (1, 2, 3, 0):
        o_in[k].wait_recv()
        both = (obuf[k, ti].astype(F32) + orecv[k].astype(F32)).astype(BF)
        if k:
            bbuf[k] = both
            b_in[k] = wire(bbuf.at[k], brecv.at[k], "fsdp", fs[k])
        else:
            brecv[0] = both
    bulk(BULK[4])
    for k in (1, 2, 3):
        g_in[k].wait_recv()
    gains_all[...] = grel[...]
    squares = jnp.zeros((hrows, 1), F32)
    for k in range(4):
        if k:
            b_in[k].wait_recv()
        h_new = tok[mine, lanes(fs[k])].astype(F32) + brecv[k].astype(F32)
        state[:, lanes(fs[k])] = h_new
        squares += jnp.sum(h_new * h_new, axis=1, keepdims=True)
    r2 = lax.rsqrt(squares * (1.0 / depth) + 1e-06)
    for k in range(4):
        nown[:, lanes(fs[k])] = (state[:, lanes(fs[k])] * r2 * grel[k, 1:2, :]).astype(BF)
    n_in = [None] * 4
    for k in (1, 2, 3):
        n_in[k] = wire(nown, nall.at[ci, ti], "ctx", cs[k])
    n_side = [wire(nown, nall.at[ci, ti], "tp", other)]
    nall[ci, ti] = nown[...]
    bulk(BULK[5])
    for k in (1, 2, 3):
        n_in[k].wait_recv()
        n_side.append(wire(nall.at[cs[k], ti], nall.at[cs[k], ti], "tp", other))
        bulk(BULK[6])
    bulk(1000)
    for copy in n_side:
        copy.wait_recv()

    def project(f):
        x = nall[:, :, :, lanes(f)].reshape(length, slab)
        return nt_dot(x, wfull[0, f]), nt_dot(x, wfull[1, f])

    gate[...], upward[...] = project(fs[0])
    gather.settle()
    keep_local(wfull.at[0], gate_full)
    keep_local(wfull.at[1], up_full)
    for k in (1, 2, 3):
        g, u = project(fs[k])
        gate[...] += g
        upward[...] += u
    for k in range(4):
        at = slice(k * rows, (k + 1) * rows)
        g = gate[at, :]
        cdf = 0.5 * (1.0 + jnp.tanh(0.7978845608028654 * (g + 0.044715 * (g * g * g))))
        hidden[at, :] = (g * cdf * upward[at, :]).astype(BF)
    keep_local(nall, normed_all)
    for copy in c_side:
        copy.wait_recv()
    keep_local(call, cot_all)
    product = Product(wire, True, hidden, call, shard, parts, near, far, sums)
    product.start()
    product.middle()
    product.end()
    for copy in locals_[2:]:
        copy.wait()
    wire.finish()


BULK = (4, 5, 4, 4, 4, 7, 1)


def call_forward(heads, tok, cot, gains, cos, sin, keep, w_q, w_kv, w_o, w_gate, w_up):
    rows, depth = tok.shape
    slab, hrows, qcols, length = depth // 4, rows // 2, heads * HD, 4 * rows
    units = w_gate.shape[1] // 4
    reach = -(-(units + units % 128) // 128) * 128
    shape = jax.ShapeDtypeStruct
    vmem = pl.BlockSpec(memory_space=pltpu.VMEM)
    hbm = pl.BlockSpec(memory_space=pl.ANY)
    pcols = qcols + HD
    sizes = product_sizes(True, slab, units)
    pair = [pltpu.VMEM((2, *size), BF) for size in sizes]
    single = [pltpu.VMEM(size, BF) for size in sizes]
    return pl.pallas_call(
        functools.partial(forward_kernel, heads),
        out_shape=[
            shape((rows, qcols), BF),
            shape((2, 4, rows, HD), BF),
            shape((heads, rows, length), F32),
            shape((hrows, depth), F32),
            shape((4, 8, slab), F32),
            shape((4, 2, hrows, depth), BF),
            shape((4, 2, hrows, depth), BF),
            shape((4, units, slab), BF),
            shape((4, units, slab), BF),
            shape((4, rows, slab), BF),
            shape((4, rows, qcols), BF),
            shape((length, units), F32),
            shape((length, units), F32),
            shape((length, units), BF),
            shape((units, slab), BF),
        ],
        in_specs=[vmem] * 9 + [hbm] * 2,
        out_specs=[vmem] * 5 + [hbm] * 4 + [vmem] * 6,
        scratch_shapes=[
            pltpu.VMEM((4, rows, slab), BF),
            pltpu.VMEM((4, rows, 128), F32),
            pltpu.VMEM((4, rows, pcols), BF),
            pltpu.VMEM((4, rows, pcols), BF),
            pltpu.VMEM((2, 4, rows, HD), BF),
            pltpu.VMEM((4, rows, qcols), BF),
            pltpu.VMEM((4, 2, hrows, slab), BF),
            pltpu.VMEM((4, hrows, slab), BF),
            pltpu.VMEM((4, hrows, slab), BF),
            pltpu.VMEM((4, hrows, slab), BF),
            pltpu.VMEM((hrows, depth), BF),
            pltpu.VMEM((4, 8, slab), F32),
            pltpu.VMEM((2, slab, reach), BF),
            pltpu.VMEM((2, 4, units, slab), BF),
            pltpu.VMEM((4, 2, hrows, depth), BF),
            pltpu.VMEM((4, 2, hrows, depth), BF),
            list(pair),
            list(pair),
            list(single),
            list(single),
            pltpu.SemaphoreType.DMA((132,)),
            pltpu.SemaphoreType.DMA((132,)),
            pltpu.SemaphoreType.DMA((12,)),
        ],
        compiler_params=pltpu.CompilerParams(
            collective_id=1, has_side_effects=True, vmem_limit_bytes=67_043_328
        ),
        cost_estimate=pl.CostEstimate(
            flops=2 * length * slab * (2 * qcols + HD), bytes_accessed=400_000_000, transcendentals=0
        ),
        name="attention_forward",
    )(tok, cot, gains, cos, sin, keep, w_q, w_kv, w_o, w_gate, w_up)


class Product:
    def __init__(self, wire, flip, left, right, shard, mine, near, far, sums):
        self.wire, self.flip, self.left, self.right, self.shard = wire, flip, left, right, shard
        self.mine, self.near, self.far, self.sums = mine, near, far, sums
        self.fs = partners("fsdp", 4)
        self.slab = shard.shape[1] if flip else shard.shape[0]
        units = shard.shape[0] if flip else shard.shape[1]
        cut = 128 * ((units + 255) // 256)
        self.spans = ((0, cut), (cut, units - cut))
        self.first, self.second = (1, 2), (2, 1)
        self.one, self.two = {}, {}

    def piece(self, k, half):
        start, size = self.spans[half]
        block = pl.ds(pl.multiple_of(self.fs[k] * self.slab, self.slab), self.slab)
        if self.flip:
            right = self.right[..., block]
            right = right.reshape(-1, right.shape[-1])
            return tn_dot(self.left[:, start : start + size], right)
        return tn_dot(self.left[:, block], self.right[:, start : start + size])

    def start(self):
        for slot in (0, 1):
            for half in (0, 1):
                k = 3 if slot == 0 else self.first[half]
                self.mine[half][slot] = self.piece(k, half).astype(BF)
                self.one[half, slot] = self.wire(
                    self.mine[half].at[slot],
                    self.near[half].at[slot],
                    "fsdp",
                    self.fs[self.first[half]],
                )

    def middle(self):
        for half in (0, 1):
            own = self.piece(self.second[half], half)
            self.one[half, 0].wait_recv()
            self.sums[half][...] = (own + self.near[half][0].astype(F32)).astype(BF)
            self.two[half] = self.wire(
                self.sums[half], self.far[half], "fsdp", self.fs[self.second[half]]
            )

    def end(self):
        for half in (0, 1):
            start, size = self.spans[half]
            own = self.piece(0, half)
            self.one[half, 1].wait_recv()
            own += self.near[half][1].astype(F32)
            self.two[half].wait_recv()
            own += self.far[half][...].astype(F32)
            if self.flip:
                self.shard[start : start + size, :] = own.astype(BF)
            else:
                self.shard[:, start : start + size] = own.astype(BF)


def product_sizes(flip, slab, units):
    cut = 128 * ((units + 255) // 256)
    return [(size, slab) if flip else (slab, size) for size in (cut, units - cut)]


def turn(value, c, s):
    front = value[:, 0:128]
    return jnp.concatenate(
        [front * c + pltpu.roll(front, 64, 1) * s, value[:, 128:256]], axis=1
    )


class Line:
    def __init__(self, own, inbox, outbox, total, send, recv):
        self.own, self.inbox, self.outbox, self.total = own, inbox, outbox, total
        self.send, self.recv = send, recv
        self.ci = lax.axis_index("ctx")

    def copy(self, way, u):
        step = 1 if way == 0 else 3
        return pltpu.make_async_remote_copy(
            src_ref=self.outbox.at[way, u - 1 + way],
            dst_ref=self.inbox.at[way, u - 1 + way],
            send_sem=self.send.at[way, u - 1 + way],
            recv_sem=self.recv.at[way, u - 1 + way],
            device_id={"ctx": lax.rem(self.ci + step, 4)},
            device_id_type=MESH,
        )

    def sends(self, way, u):
        return self.ci < u if way == 0 else self.ci > u

    def fed(self, way):
        return self.ci > 0 if way == 0 else self.ci < 3

    def lead(self):
        for step in range(3):
            for way, u in ((0, 3 - step), (1, step)):

                @pl.when(jnp.logical_and(self.sends(way, u), jnp.logical_not(self.fed(way))))
                def _():
                    self.outbox[way, u - 1 + way] = self.own(u).astype(BF)
                    self.copy(way, u).start()

    def hop(self, way, u):
        self.copy(way, u).wait_recv()
        slot = u - 1 + way
        self.outbox[way, slot] = (self.own(u) + self.inbox[way, slot].astype(F32)).astype(BF)
        self.copy(way, u).start()

    def push_near(self, steps=(0, 1)):
        for step in steps:

            @pl.when(self.ci == 1)
            def _():
                self.hop(0, 3 - step)

            @pl.when(self.ci == 2)
            def _():
                self.hop(1, step)

    def push_far(self):
        @pl.when(self.ci == 1)
        def _():
            self.hop(1, 0)

        @pl.when(self.ci == 2)
        def _():
            self.hop(0, 3)

    def collect(self):
        self.total[...] = self.own(self.ci)
        for way in (0, 1):

            @pl.when(self.fed(way))
            def _():
                self.copy(way, self.ci).wait_recv()
                self.total[...] += self.inbox[way, self.ci - 1 + way].astype(F32)

    def drain(self):
        for way in (0, 1):
            for u in range(1 - way, 4 - way):

                @pl.when(self.sends(way, u))
                def _():
                    self.copy(way, u).wait_send()


def line_scratch(*form):
    return [
        pltpu.VMEM((2, 3, *form), BF),
        pltpu.VMEM((2, 3, *form), BF),
        pltpu.VMEM(form, F32),
        pltpu.SemaphoreType.DMA((2, 3)),
        pltpu.SemaphoreType.DMA((2, 3)),
    ]


class Spread:
    def __init__(self, own, full, pieces, send, recv, local, height=None):
        self.own, self.full, self.pieces = own, full, pieces
        self.send, self.recv = send, recv
        self.height = height or own.shape[0] // pieces
        self.cs = partners("ctx", 4)
        self.ci = self.cs[0]
        self.inner = jnp.logical_and(self.ci > 0, self.ci < 3)
        self.local = local

    def strip(self, p):
        return pl.ds(p * self.height, self.height)

    def copy(self, kind, p, source, peer):
        place = self.full.at[source, self.strip(p), :]
        src = self.own.at[self.strip(p), :] if kind < 2 else place
        slot = (0, 1, 2, 1, 2)[kind]
        return pltpu.make_async_remote_copy(
            src_ref=src,
            dst_ref=place,
            send_sem=self.send.at[kind, p],
            recv_sem=self.recv.at[slot, p],
            device_id={"ctx": peer},
            device_id_type=MESH,
        )

    def out(self, kind, p):
        cs = self.cs
        source = (cs[0], cs[0], cs[1], cs[3], cs[2])[kind]
        peer = (cs[1], cs[3], cs[3], cs[1], cs[1])[kind]
        return self.copy(kind, p, source, peer)

    def arrived(self, slot, p):
        self.copy((0, 1, 2)[slot], p, self.ci, self.cs[1]).wait_recv()

    def keep(self):
        return pltpu.make_async_copy(self.own, self.full.at[self.ci], self.local)

    def begin(self):
        self.keep().start()

    def give(self, p):
        self.out(0, p).start()

        @pl.when(self.inner)
        def _():
            self.out(1, p).start()

    def hand_on(self, p):
        @pl.when(self.inner)
        def _():
            self.arrived(0, p)
            self.out(2, p).start()
            self.arrived(1, p)
            self.out(3, p).start()

    def hand_far(self, p):
        @pl.when(self.inner)
        def _():
            self.arrived(2, p)
            self.out(4, p).start()

    def close(self, near=True, far=True):
        for p in range(self.pieces):

            @pl.when(jnp.logical_not(self.inner))
            def _():
                for slot in range(0 if near else 2, 3 if far else 2):
                    self.arrived(slot, p)

            if near:
                self.out(0, p).wait_send()

            @pl.when(self.inner)
            def _():
                if near and not far:
                    self.arrived(2, p)
                for kind in range(1 if near else 4, 5 if far else 4):
                    self.out(kind, p).wait_send()

        if near:
            self.keep().wait()

    def hand_again(self, p):
        @pl.when(self.inner)
        def _():
            self.out(4, p).start()


def spread_scratch(pieces):
    return [
        pltpu.SemaphoreType.DMA((5, pieces)),
        pltpu.SemaphoreType.DMA((3, pieces)),
        pltpu.SemaphoreType.DMA,
    ]


def units_line(wire, part, side, line_refs, ti):
    other = 1 - ti
    side_in = [wire(part.at[u, other], side.at[u], "tp", other) for u in range(4)]
    for copy in side_in:
        copy.wait_recv()
    return Line(lambda u: part[u, ti].astype(F32) + side[u].astype(F32), *line_refs)


def backward_kernel(
    heads,
    dn,
    cot_in,
    state,
    gains_all,
    probs_in,
    q_rot_in,
    kv_in,
    cos,
    sin,
    w_o_in,
    normed_in,
    att_in,
    normed_all,
    shard_gate,
    d_up,
    part_in,
    tok_in,
    w_q_in,
    w_kv_in,
    out,
    grad_tok,
    gain_grads,
    gate_all,
    up_all,
    weights_all,
    kv_side,
    side,
    dbuf,
    dslab,
    dpart,
    dfar,
    dkv2,
    kvt,
    zk,
    zfar,
    dqbuf,
    dkvbuf,
    dk_acc,
    dv_acc,
    own_out,
    own_query,
    row_refs,
    out_refs,
    query_refs,
    parts,
    sums,
    product_recv,
    shard_up,
    gate_sems,
    up_sems,
    gpart,
    weight_grads,
    weight_sems,
    last_sems,
    obuf,
    gbuf,
    pbuf,
    pside,
    nbuf,
    nrow,
    gfar,
    gsum,
    gnear,
    gall,
    late,
    late_sems,
    send,
    recv,
    local,
):
    fs, cs = partners("fsdp", 4), partners("ctx", 4)
    ci, ti = lax.axis_index("ctx"), lax.axis_index("tp")
    other = 1 - ti
    hrows, depth = state.shape
    rows = 2 * hrows
    slab = depth // 4
    length = 4 * rows
    scale = HD ** (-0.5)
    sources = (cot_in, probs_in, q_rot_in, kv_in, w_o_in, normed_in, att_in, part_in, tok_in, w_q_in, w_kv_in)
    cot, probs, q_rot, kv, w_o, normed, att, part, tok, w_q, w_kv = late
    loads = [
        pltpu.make_async_copy(source, target, late_sems.at[n])
        for n, (source, target) in enumerate(zip(sources, late))
    ]
    greet(
        [("fsdp", fs[k]) for k in (1, 2, 3)]
        + [("ctx", cs[k]) for k in (1, 2, 3)]
        + [("tp", other)]
    )
    wire = Wire(send, recv)
    mine = pl.ds(pl.multiple_of(ti * hrows, hrows), hrows)

    def lanes(index):
        return pl.ds(pl.multiple_of(index * slab, slab), slab)

    up = Product(wire, True, d_up, normed_all, shard_up, parts, *product_recv, sums)
    gate_line = Spread(shard_gate, gate_all, PIECES, *gate_sems)
    up_line = Spread(shard_up, up_all, PIECES, *up_sems)
    line = units_line(wire, dn, side, row_refs, ti)
    line.lead()
    gate_line.begin()
    for p in range(PIECES // 2):
        gate_line.give(p)
    for load in loads:
        load.start()
    up.start()
    squares = jnp.zeros((hrows, 1), F32)
    for k in range(4):
        u = state[:, lanes(fs[k])]
        squares += jnp.sum(u * u, axis=1, keepdims=True)
    r = lax.rsqrt(squares * (1.0 / depth) + 1e-06)
    line.push_near()
    line.push_far()
    for p in range(PIECES // 2, PIECES):
        gate_line.give(p)
    line.collect()
    for load in loads:
        load.wait()
    inner = jnp.zeros((hrows, 1), F32)
    for k in range(4):
        at = lanes(fs[k])
        inner += jnp.sum(
            state[:, at] * gains_all[k, 1:2, :] * line.total[:, at], axis=1, keepdims=True
        )
    pull = r * r * r * (inner * (1.0 / depth))
    d_in = {}
    d_side = {}
    gpart[...] = jnp.zeros_like(gpart)
    for k in (1, 2, 3, 0):
        at = lanes(fs[k])
        u, d = state[:, at], line.total[:, at]
        ds = cot[mine, at].astype(F32) + (r * (gains_all[k, 1:2, :] * d) - u * pull)
        gbuf[ti, :, at] = ds
        if k:
            dbuf[k] = ds.astype(BF)
            d_in[k] = wire(dbuf.at[k], dslab.at[k, ti], "fsdp", fs[k])
        else:
            dslab[0, ti] = ds.astype(BF)
            d_side[0] = wire(dslab.at[0, ti], dslab.at[0, ti], "tp", other)
        gpart[k, 1:2, :] = jnp.sum(u * r * d, axis=0, keepdims=True)
    up.middle()
    for k in (1, 2, 3):
        d_in[k].wait_recv()
        d_side[k] = wire(dslab.at[k, ti], dslab.at[k, ti], "tp", other)
    for p in range(PIECES // 2):
        gate_line.hand_on(p)
    a_in = {}
    for k in (1, 2, 3, 0):
        d_side[k].wait_recv()
        block = dslab[k].reshape(rows, slab)
        dpart[k] = nt_dot(block, w_o[...]).astype(BF)
        if k:
            a_in[k] = wire(dpart.at[k], dfar.at[k], "fsdp", fs[k])
    for p in range(PIECES // 2, PIECES):
        gate_line.hand_on(p)
    up.end()
    keys = kv[0].reshape(length, HD)
    values = kv[1].reshape(length, HD)
    c, s = cos[...], sin[...]
    quarter = heads * HD // 4
    branch = dslab[...].reshape(length, slab)
    for u in range(4):
        columns = att[:, :, u * quarter : (u + 1) * quarter].reshape(length, quarter)
        own_out[u] = tn_dot(columns, branch).astype(BF)
    out_line = Line(lambda u: own_out[u].astype(F32), *out_refs)
    for k in (1, 2, 3):
        a_in[k].wait_recv()
    for h in range(heads):
        at = slice(h * HD, (h + 1) * HD)
        d = dpart[0, :, at].astype(F32)
        for k in (1, 2, 3):
            d += dfar[k, :, at].astype(F32)
        d = d.astype(BF)
        p = probs[h]
        dp = nt_dot(d, values)
        delta = jnp.sum(p * dp, axis=1, keepdims=True)
        dsc = (p * (dp - delta)).astype(BF)
        dq = jnp.dot(dsc, keys, preferred_element_type=F32) * scale
        dqbuf[0, :, at] = turn(dq, c, -s).astype(BF)
        dk = tn_dot(dsc, q_rot[:, at])
        dv = tn_dot(p.astype(BF), d)
        if h == 0:
            dk_acc[...] = dk
            dv_acc[...] = dv
        else:
            dk_acc[...] += dk
            dv_acc[...] += dv
    for p in range(PIECES // 2):
        gate_line.hand_far(p)
    dkv2[0] = (dk_acc[...] * scale).astype(BF).reshape(4, rows, HD)
    dkv2[1] = dv_acc[...].astype(BF).reshape(4, rows, HD)
    k_side = wire(dkv2.at[other], kvt, "tp", other)
    q_in = {}
    for k in (1, 2, 3):
        q_in[k] = wire(dqbuf.at[0], dqbuf.at[k], "fsdp", fs[k])
    k_side.wait_recv()
    z_in = {}
    for k in (1, 2, 3):
        zk[k] = (dkv2[ti, k].astype(F32) + kvt[k].astype(F32)).astype(BF)
        z_in[k] = wire(zk.at[k], zfar.at[k], "ctx", cs[k])
    out_line.lead()
    for p in range(PIECES // 2, PIECES):
        gate_line.hand_far(p)
    own = dkv2[ti, 0].astype(F32) + kvt[0].astype(F32)
    for k in (1, 2, 3):
        z_in[k].wait_recv()
        own += zfar[k].astype(F32)
    zero = (1 - ti).astype(F32)
    dkvbuf[0] = turn(own, c * zero + (1.0 - zero), -s * zero).astype(BF)
    v_in = {}
    for k in (1, 2, 3):
        v_in[k] = wire(dkvbuf.at[0], dkvbuf.at[k], "fsdp", fs[k])
    out_line.push_near()
    up_line.begin()
    for p in range(PIECES):
        up_line.give(p)
    for k in (1, 2, 3):
        q_in[k].wait_recv()
    slabs = normed[...].reshape(length, slab)
    for u in (3, 0, 2, 1):
        columns = dqbuf[:, :, u * quarter : (u + 1) * quarter].reshape(length, quarter)
        own_query[u, 0:quarter] = tn_dot(columns, slabs).astype(BF)
    for k in (1, 2, 3):
        v_in[k].wait_recv()
    for u in (3, 0, 2, 1):
        columns = dkvbuf[:, :, u * (HD // 4) : (u + 1) * (HD // 4)].reshape(length, HD // 4)
        own_query[u, quarter:] = tn_dot(columns, slabs).astype(BF)
    query_line = Line(lambda u: own_query[u].astype(F32), *query_refs)
    kv_half = w_kv[:, pl.ds(pl.multiple_of(ti * HD, HD), HD)]
    p_in = {}
    for k in (1, 2, 3, 0):
        block = (nt_dot(dqbuf[k], w_q[...]) + nt_dot(dkvbuf[k], kv_half)).astype(BF)
        pbuf[k, 0] = block[0:hrows]
        pbuf[k, 1] = block[hrows:rows]
        p_in[k] = wire(pbuf.at[k, other], pside.at[k], "tp", other)
    out_line.push_far()
    query_line.lead()
    n_in = {}
    for k in (1, 2, 3, 0):
        p_in[k].wait_recv()
        both = (pbuf[k, ti].astype(F32) + pside[k].astype(F32)).astype(BF)
        if k:
            nbuf[k] = both
            n_in[k] = wire(nbuf.at[k], nrow.at[k], "fsdp", fs[k])
        else:
            nrow[0] = both
    squares = jnp.zeros((hrows, 1), F32)
    for k in range(4):
        u = tok[mine, lanes(fs[k])].astype(F32)
        squares += jnp.sum(u * u, axis=1, keepdims=True)
    r = lax.rsqrt(squares * (1.0 / depth) + 1e-06)
    for p in range(PIECES):
        up_line.hand_on(p)
    query_line.push_near((0,))
    inner = jnp.zeros((hrows, 1), F32)
    for k in range(4):
        if k:
            n_in[k].wait_recv()
        u = tok[mine, lanes(fs[k])].astype(F32)
        inner += jnp.sum(u * gains_all[k, 0:1, :] * nrow[k].astype(F32), axis=1, keepdims=True)
    pull = r * r * r * (inner * (1.0 / depth))
    for k in range(4):
        at = lanes(fs[k])
        u, d = tok[mine, at].astype(F32), nrow[k].astype(F32)
        gbuf[ti, :, at] += (r * (gains_all[k, 0:1, :] * d) - u * pull)
        gpart[k, 0:1, :] = jnp.sum(u * r * d, axis=0, keepdims=True)
    t_side = wire(gbuf.at[ti], gbuf.at[ti], "tp", other)
    g_in = {}
    for k in (1, 2, 3):
        g_in[k] = wire(gpart.at[k], gfar.at[k], "fsdp", fs[k])
    for p in range(PIECES // 2):
        up_line.hand_far(p)
    query_line.push_far()
    query_line.push_near((1,))
    for p in range(PIECES // 2, PIECES):
        up_line.hand_far(p)
    gain_sum = gpart[0]
    for k in (1, 2, 3):
        g_in[k].wait_recv()
        gain_sum += gfar[k]
    gsum[...] = gain_sum
    near_gain = wire(gsum, gnear, "tp", other)
    near_gain.wait_recv()
    gall[ci] = gain_sum + gnear[...]
    all_gain = [wire(gall.at[ci], gall.at[ci], "ctx", cs[k]) for k in (1, 2, 3)]
    out_line.collect()
    weight_grads[0:quarter, :] = out_line.total[...].astype(BF)
    query_line.collect()
    weight_grads[quarter:, :] = query_line.total[...].astype(BF)
    weight_line = Spread(weight_grads, weights_all, PIECES, *weight_sems)
    weight_line.begin()
    for p in range(PIECES):
        weight_line.give(p)
    line.drain()
    last = units_line(wire, part, side, [*row_refs[:3], *last_sems], ti)
    last.lead()
    for p in range(PIECES):
        weight_line.hand_on(p)
    last.push_near()
    for p in range(PIECES // 2):
        weight_line.hand_far(p)
    last.push_far()
    for p in range(PIECES // 2, PIECES):
        weight_line.hand_far(p)
    last.collect()
    obuf[ti] = (state[...] + last.total[...]).astype(BF)
    o_side = wire(obuf.at[ti], obuf.at[ti], "tp", other)
    t_side.wait_recv()
    keep_t = pltpu.make_async_copy(gbuf, grad_tok, local.at[0])
    keep_t.start()
    o_side.wait_recv()
    keep_o = pltpu.make_async_copy(obuf, out, local.at[1])
    keep_o.start()
    for copy in all_gain:
        copy.wait_recv()
    gain_grads[...] = gall[0] + gall[1] + gall[2] + gall[3]
    gate_line.close()
    up_line.close()
    weight_line.close()
    tail = pl.ds(2 * quarter, HD // 4)
    kv_last = wire(weights_all.at[:, tail, :], kv_side, "tp", other)
    kv_last.wait_recv()
    for each in (last, out_line, query_line):
        each.drain()
    keep_t.wait()
    keep_o.wait()
    wire.finish()


PIECES = 4


def call_backward(
    heads, dn, cot, state, gains_all, probs, q_rot, kv, cos, sin, w_o, normed, att, normed_all, shard_gate, d_up, part, tok, w_q, w_kv
):
    hrows, depth = state.shape
    rows, slab, qcols = 2 * hrows, depth // 4, heads * HD
    length = 4 * rows
    units = d_up.shape[1]
    late = (cot, probs, q_rot, kv, w_o, normed, att, part, tok, w_q, w_kv)
    sizes = product_sizes(True, slab, units)
    pair = [pltpu.VMEM((2, *size), BF) for size in sizes]
    single = [pltpu.VMEM(size, BF) for size in sizes]
    shape = jax.ShapeDtypeStruct
    vmem = pl.BlockSpec(memory_space=pltpu.VMEM)
    hbm = pl.BlockSpec(memory_space=pl.ANY)
    return pl.pallas_call(
        functools.partial(backward_kernel, heads),
        out_shape=[
            shape((2, hrows, depth), BF),
            shape((2, hrows, depth), F32),
            shape((8, slab), F32),
            shape((4, units, slab), BF),
            shape((4, units, slab), BF),
            shape((4, qcols // 2 + HD // 4, slab), BF),
            shape((4, HD // 4, slab), BF),
        ],
        in_specs=[vmem, hbm, vmem, vmem, hbm, hbm, hbm, vmem, vmem]
        + [hbm] * 3
        + [vmem, hbm, vmem]
        + [hbm] * 4,
        out_specs=[hbm] * 2 + [vmem] + [hbm] * 4,
        scratch_shapes=[
            pltpu.VMEM((4, hrows, depth), BF),
            pltpu.VMEM((4, hrows, slab), BF),
            pltpu.VMEM((4, 2, hrows, slab), BF),
            pltpu.VMEM((4, rows, qcols), BF),
            pltpu.VMEM((4, rows, qcols), BF),
            pltpu.VMEM((2, 4, rows, HD), BF),
            pltpu.VMEM((4, rows, HD), BF),
            pltpu.VMEM((4, rows, HD), BF),
            pltpu.VMEM((4, rows, HD), BF),
            pltpu.VMEM((4, rows, qcols), BF),
            pltpu.VMEM((4, rows, HD), BF),
            pltpu.VMEM((length, HD), F32),
            pltpu.VMEM((length, HD), F32),
            pltpu.VMEM((4, qcols // 4, slab), BF),
            pltpu.VMEM((4, (qcols + HD) // 4, slab), BF),
            line_scratch(hrows, depth),
            line_scratch(qcols // 4, slab),
            line_scratch((qcols + HD) // 4, slab),
            list(pair),
            list(single),
            [list(pair), list(single)],
            pltpu.VMEM((units, slab), BF),
            spread_scratch(PIECES),
            spread_scratch(PIECES),
            pltpu.VMEM((4, 8, slab), F32),
            pltpu.VMEM((qcols // 2 + HD // 4, slab), BF),
            spread_scratch(PIECES),
            [pltpu.SemaphoreType.DMA((2, 3)), pltpu.SemaphoreType.DMA((2, 3))],
            pltpu.VMEM((2, hrows, depth), BF),
            pltpu.VMEM((2, hrows, depth), F32),
            pltpu.VMEM((4, 2, hrows, slab), BF),
            pltpu.VMEM((4, hrows, slab), BF),
            pltpu.VMEM((4, hrows, slab), BF),
            pltpu.VMEM((4, hrows, slab), BF),
            pltpu.VMEM((4, 8, slab), F32),
            pltpu.VMEM((8, slab), F32),
            pltpu.VMEM((8, slab), F32),
            pltpu.VMEM((4, 8, slab), F32),
            [pltpu.VMEM(each.shape, each.dtype) for each in late],
            pltpu.SemaphoreType.DMA((len(late),)),
            pltpu.SemaphoreType.DMA((64,)),
            pltpu.SemaphoreType.DMA((64,)),
            pltpu.SemaphoreType.DMA((2,)),
        ],
        compiler_params=pltpu.CompilerParams(
            collective_id=5, has_side_effects=True, vmem_limit_bytes=67_043_328
        ),
        cost_estimate=pl.CostEstimate(
            flops=2 * length * slab * qcols, bytes_accessed=300_000_000, transcendentals=0
        ),
        name="attention_backward",
    )(dn, cot, state, gains_all, probs, q_rot, kv, cos, sin, w_o, normed, att, normed_all, shard_gate, d_up, part, tok, w_q, w_kv)


STRIP = 128


def convert_kernel(
    gate_all,
    up_all,
    down_all,
    weights_all,
    kv_side,
    out_in,
    tok_in,
    grad_gate,
    grad_up,
    grad_down,
    grad_out,
    grad_query,
    grad_kv,
    out,
    grad_tok,
    wide_in,
    wide_out,
    tall_in,
    tall_out,
    turn_in,
    turn_out,
    kv_in,
    kv_out,
    same_out,
    same_tok,
    in_sems,
    out_sems,
):
    ti = lax.axis_index("tp")
    units, slab = gate_all.shape[1:]
    quarter = grad_query.shape[1] // 4
    loads, works, stores = [], [], []

    def job(sources, work, target_from, target):
        n = len(loads)
        slot = n % 3
        loads.append(
            [
                pltpu.make_async_copy(source, place(slot), in_sems.at[slot, m])
                for m, (source, place) in enumerate(sources)
            ]
        )
        works.append(lambda: work(slot))
        stores.append(pltpu.make_async_copy(target_from(slot), target, out_sems.at[slot]))

    def strips(source, target):
        for p in range(slab // STRIP):
            rows = pl.ds(p * STRIP, STRIP)

            def work(slot):
                block = wide_in[slot].reshape(4 * units, STRIP)
                for j in range(6):
                    at = slice(j * 4 * units // 6, (j + 1) * 4 * units // 6)
                    wide_out[slot, :, at] = block[at].T.astype(F32)

            job(
                [(source.at[:, :, rows], lambda slot: wide_in.at[slot])],
                work,
                lambda slot: wide_out.at[slot],
                target.at[rows, :],
            )

    def tall_work(slot):
        tall_out[slot] = tall_in[slot].astype(F32)

    def low_work(slot):
        tall_out[slot, 0:quarter] = tall_in[slot, 0:quarter].astype(F32)

    strips(gate_all, grad_gate)
    strips(up_all, grad_up)
    high = tall_in.shape[1]
    for p in range(4 * units // high):
        rows = pl.ds(p * high, high)
        job(
            [(down_all.at[rows, :], lambda slot: tall_in.at[slot])],
            tall_work,
            lambda slot: tall_out.at[slot],
            grad_down.at[rows, :],
        )
    for j in range(4):
        part = pl.ds(0, quarter)
        job(
            [(weights_all.at[j, part, :], lambda slot: tall_in.at[slot, part, :])],
            low_work,
            lambda slot: tall_out.at[slot, part, :],
            grad_out.at[pl.ds(j * quarter, quarter), :],
        )
    early = [
        pltpu.make_async_copy(
            weights_all.at[j, pl.ds(quarter, quarter), :],
            turn_in.at[pl.ds(j * quarter, quarter), :],
            in_sems.at[3, j],
        )
        for j in range(4)
    ] + [
        pltpu.make_async_copy(
            weights_all.at[:, pl.ds(2 * quarter, HD // 4), :], kv_in.at[0], in_sems.at[4, 0]
        ),
        pltpu.make_async_copy(kv_side, kv_in.at[1], in_sems.at[4, 1]),
    ]
    same = [
        pltpu.make_async_copy(out_in, same_out, in_sems.at[4, 2]),
        pltpu.make_async_copy(tok_in, same_tok, in_sems.at[4, 3]),
    ]
    for copy in loads[0] + loads[1] + early + same:
        copy.start()
    for n in range(len(loads)):
        if n + 2 < len(loads):
            for copy in loads[n + 2]:
                copy.start()
        for copy in loads[n]:
            copy.wait()
        if n >= 3:
            stores[n - 3].wait()
        works[n]()
        stores[n].start()
    late = []
    for n, (copy, source, target) in enumerate(
        ((same[0], same_out, out), (same[1], same_tok, grad_tok))
    ):
        copy.wait()
        late.append(pltpu.make_async_copy(source, target, out_sems.at[3 + n]))
        late[-1].start()
    for copy in early:
        copy.wait()
    for i in range(4 * quarter // 256):
        turn_out[:, i * 256 : (i + 1) * 256] = turn_in[i * 256 : (i + 1) * 256, :].T.astype(F32)
    late.append(pltpu.make_async_copy(turn_out, grad_query, out_sems.at[5]))
    late[-1].start()
    for n, place in ((0, ti), (1, 1 - ti)):
        at = pl.ds(pl.multiple_of(place * HD, HD), HD)
        kv_out[:, at] = kv_in[n].reshape(HD, slab).T.astype(F32)
    late.append(pltpu.make_async_copy(kv_out, grad_kv, out_sems.at[6]))
    late[-1].start()
    for copy in stores[-3:] + late:
        copy.wait()


def call_convert(gate_all, up_all, down_all, weights_all, kv_side, out, grad_tok):
    units, slab = gate_all.shape[1:]
    quarter = (weights_all.shape[1] - HD // 4) // 2
    shape = jax.ShapeDtypeStruct
    hbm = pl.BlockSpec(memory_space=pl.ANY)
    return pl.pallas_call(
        convert_kernel,
        out_shape=[
            shape((slab, 4 * units), F32),
            shape((slab, 4 * units), F32),
            shape((4 * units, slab), F32),
            shape((4 * quarter, slab), F32),
            shape((slab, 4 * quarter), F32),
            shape((slab, 2 * HD), F32),
            shape(out.shape, out.dtype),
            shape(grad_tok.shape, grad_tok.dtype),
        ],
        in_specs=[hbm] * 7,
        out_specs=[hbm] * 8,
        scratch_shapes=[
            pltpu.VMEM((3, 4, units, STRIP), BF),
            pltpu.VMEM((3, STRIP, 4 * units), F32),
            pltpu.VMEM((3, units, slab), BF),
            pltpu.VMEM((3, units, slab), F32),
            pltpu.VMEM((4 * quarter, slab), BF),
            pltpu.VMEM((slab, 4 * quarter), F32),
            pltpu.VMEM((2, 4, HD // 4, slab), BF),
            pltpu.VMEM((slab, 2 * HD), F32),
            pltpu.VMEM(out.shape, out.dtype),
            pltpu.VMEM(grad_tok.shape, grad_tok.dtype),
            pltpu.SemaphoreType.DMA((5, 4)),
            pltpu.SemaphoreType.DMA((7,)),
        ],
        compiler_params=pltpu.CompilerParams(vmem_limit_bytes=67_043_328),
        cost_estimate=pl.CostEstimate(
            flops=0, bytes_accessed=20 * slab * 4 * units, transcendentals=0
        ),
        name="convert",
    )(gate_all, up_all, down_all, weights_all, kv_side, out, grad_tok)


def fast_device(
    tokens,
    segment_ids,
    w_query,
    w_keyval,
    w_out,
    w_gate,
    w_up,
    w_down,
    gain_attn,
    gain_ffn,
    cotangent,
):
    ci = lax.axis_index("ctx")
    tok, cot = tokens[0], cotangent[0]
    rows, depth = tok.shape
    hrows, slab = rows // 2, depth // 4
    length = segment_ids.shape[1]
    heads = w_query.shape[1] // HD
    units = w_gate.shape[1] // 4

    def cut(value, start, size, axis):
        return lax.dynamic_slice_in_dim(value, start, size, axis)

    segment_row = segment_ids[0]
    local_segment = cut(segment_row, ci * rows, rows, 0)
    local_index = ci * rows + jnp.arange(rows, dtype=jnp.int32)
    earlier = jnp.sum((segment_row[None, :] < local_segment[:, None]).astype(jnp.int32), axis=1)
    position = (local_index - earlier).astype(F32)
    freqs = 10000.0 ** (-(jnp.arange(HD // 4, dtype=F32) * 2.0 / (HD // 2)))
    angle = position[:, None] * freqs[None, :]
    cosine, sine = jnp.cos(angle), jnp.sin(angle)
    cos = jnp.concatenate([cosine, cosine], axis=1)
    sin = jnp.concatenate([-sine, sine], axis=1)
    key_index = jnp.concatenate(
        [(ci ^ k) * rows + jnp.arange(rows, dtype=jnp.int32) for k in range(4)]
    )
    key_segment = jnp.concatenate([cut(segment_row, (ci ^ k) * rows, rows, 0) for k in range(4)])
    keep = (
        (local_segment[:, None] == key_segment[None, :])
        & (key_index[None, :] <= local_index[:, None])
    ).astype(F32)
    gains = jnp.concatenate(
        [gain_attn[None], gain_ffn[None], jnp.zeros((6, slab), gain_attn.dtype)]
    ).astype(F32)

    (
        q_rot,
        kv,
        probs,
        state,
        gains_all,
        normed_all,
        cot_all,
        gate_full,
        up_full,
        normed_slab,
        att_plane,
        gate,
        upward,
        hidden,
        shard_down,
    ) = call_forward(
        heads,
        tok,
        cot,
        gains,
        cos,
        sin,
        keep,
        w_query,
        w_keyval,
        w_out,
        w_gate,
        w_up,
    )
    normed_all = normed_all.reshape(length, depth)
    cot_all = cot_all.reshape(length, depth)
    d_up, dn, part, shard_gate, down_all = call_middle(
        w_down, shard_down, cot_all, normed_all, gate, upward, hidden, gate_full, up_full
    )
    dn = dn.reshape(4, 2, hrows, depth)
    part = part.reshape(4, 2, hrows, depth)
    out, grad_tok, gain_grads, gate_all, up_all, weight_grads, kv_side = call_backward(
        heads,
        dn,
        cot,
        state,
        gains_all,
        probs,
        q_rot,
        kv,
        cos,
        sin,
        w_out,
        normed_slab,
        att_plane,
        normed_all,
        shard_gate,
        d_up,
        part,
        tok,
        w_query,
        w_keyval,
    )
    (
        grad_gate,
        grad_up,
        grad_down,
        grad_out,
        grad_query,
        grad_kv,
        out,
        grad_tok,
    ) = call_convert(
        gate_all,
        up_all,
        down_all.reshape(4 * units, slab),
        weight_grads,
        kv_side,
        out,
        grad_tok,
    )

    return (
        out.reshape(1, rows, depth),
        grad_tok.reshape(1, rows, depth),
        grad_query,
        grad_kv,
        grad_out,
        grad_gate,
        grad_up,
        grad_down,
        gain_grads[0],
        gain_grads[1],
    )


def solution(mesh):
    sizes = (mesh.shape["fsdp"], mesh.shape["ctx"], mesh.shape["tp"])
    in_specs = (
        P("fsdp", "ctx", None),
        P("fsdp", None),
        P("fsdp", "tp"),
        P("fsdp", None),
        P("tp", "fsdp"),
        P("fsdp", "tp"),
        P("fsdp", "tp"),
        P("tp", "fsdp"),
        P("fsdp"),
        P("fsdp"),
        P("fsdp", "ctx", None),
    )
    out_specs = (
        P("fsdp", "ctx", None),
        P("fsdp", "ctx", None),
        P("fsdp", "tp"),
        P("fsdp", None),
        P("tp", "fsdp"),
        P("fsdp", "tp"),
        P("fsdp", "tp"),
        P("tp", "fsdp"),
        P("fsdp"),
        P("fsdp"),
    )

    def body(*args):
        rows, depth = args[0].shape[1:]
        fits = sizes == (4, 4, 2) and depth % 512 == 0 and rows % 32 == 0
        if fits:
            return fast_device(*args)
        return per_device(sizes, *args)

    return jax.shard_map(
        body, mesh=mesh, in_specs=in_specs, out_specs=out_specs, check_vma=False
    )
```

```python
import functools

import jax
import jax.numpy as jnp
from jax import lax
from jax.experimental import pallas as pl
from jax.experimental.pallas import tpu as pltpu
from jax.sharding import PartitionSpec as P

HD = 256
NEGATIVE = -1e30
BF = jnp.bfloat16
F32 = jnp.float32
MESH = pl.DeviceIdType.MESH


def rms_scale(value, gain):
    return value * lax.rsqrt(jnp.mean(value * value, axis=-1, keepdims=True) + 1e-06) * gain


def rotate(value, cosine, sine):
    quarter = value.shape[-1] // 4
    first = value[..., :quarter]
    second = value[..., quarter : 2 * quarter]
    rest = value[..., 2 * quarter :]
    return jnp.concatenate(
        [first * cosine - second * sine, second * cosine + first * sine, rest], axis=-1
    )


def unrotate(value, cosine, sine):
    return rotate(value, cosine, -sine)


def matmul(left, right):
    return jnp.dot(left, right, preferred_element_type=F32)


def times_transposed(left, right):
    return lax.dot_general(left, right, (((1,), (1,)), ((), ())), preferred_element_type=F32)


def transposed_times(left, right):
    return lax.dot_general(left, right, (((0,), (0,)), ((), ())), preferred_element_type=F32)


def geglu(gate_in, up_in):
    return jax.nn.gelu(gate_in, approximate=True) * up_in


def swap(value, axis, size, k):
    return lax.ppermute(value, axis, [(i, i ^ k) for i in range(size)])


def per_device(
    sizes,
    tokens,
    segment_ids,
    w_query,
    w_keyval,
    w_out,
    w_gate,
    w_up,
    w_down,
    gain_attn,
    gain_ffn,
    cotangent,
):
    nf, nc, nt = sizes
    fi, ci, ti = lax.axis_index("fsdp"), lax.axis_index("ctx"), lax.axis_index("tp")
    rows = tokens.shape[1]
    depth = tokens.shape[2]
    slab = depth // nf
    half = depth // nt
    heads = w_query.shape[1] // HD
    qcols = heads * HD
    units = w_gate.shape[1] // nc
    scale = HD ** (-0.5)

    def cut(value, start, size, axis):
        return lax.dynamic_slice_in_dim(value, start, size, axis)

    def all_to_all_blocks(blocks, axis, size):
        return [blocks[0]] + [swap(blocks[k], axis, size, k) for k in range(1, size)]

    def gather_blocks(value, axis, size):
        return [value] + [swap(value, axis, size, k) for k in range(1, size)]

    def absolute(blocks, index, axis):
        stacked = jnp.stack(blocks)
        size = len(blocks)
        return jnp.concatenate(
            [lax.dynamic_index_in_dim(stacked, j ^ index, 0, keepdims=False) for j in range(size)],
            axis=axis,
        )

    def rows_to_slabs(value):
        blocks = [cut(value, (fi ^ k) * slab, slab, 1) for k in range(nf)]
        return jnp.concatenate(all_to_all_blocks(blocks, "fsdp", nf), axis=0)

    def slabs_to_rows(value):
        blocks = list(value.reshape(nf, rows, slab))
        return absolute(all_to_all_blocks(blocks, "fsdp", nf), fi, 1)

    def reduce_rows(value, width):
        blocks = list(value.reshape(nf, rows, width))
        got = all_to_all_blocks(blocks, "fsdp", nf)
        return sum(block.astype(F32) for block in got)

    def gather_rows(value):
        return jnp.concatenate(gather_blocks(value, "fsdp", nf), axis=0)

    def both_halves(mine, axis):
        other = swap(mine, "tp", nt, 1)
        return jnp.where(
            ti == 0,
            jnp.concatenate([mine, other], axis=axis),
            jnp.concatenate([other, mine], axis=axis),
        )

    def tp_sum(value):
        low = value.astype(BF)
        return low.astype(F32) + swap(low, "tp", nt, 1).astype(F32)

    def gather_ctx(value):
        mine = cut(value, ti * half, half, 1)
        return both_halves(jnp.concatenate(gather_blocks(mine, "ctx", nc), axis=0), 1)

    def reduce_ctx(value):
        low = value.astype(BF)
        keep = cut(low, ti * half, half, 1)
        send = cut(low, (1 - ti) * half, half, 1)
        both = (keep.astype(F32) + swap(send, "tp", nt, 1).astype(F32)).astype(BF)
        got = all_to_all_blocks(list(both.reshape(nc, rows, half)), "ctx", nc)
        return sum(block.astype(F32) for block in got)

    gate_full = lax.all_gather(cut(w_gate, ci * units, units, 1), "fsdp", axis=0, tiled=True)
    up_full = lax.all_gather(cut(w_up, ci * units, units, 1), "fsdp", axis=0, tiled=True)
    down_full = lax.all_gather(
        cut(w_down, ci * units, units, 0).T, "fsdp", axis=0, tiled=True
    )

    gains = jnp.stack([gain_attn, gain_ffn])
    gains = absolute(gather_blocks(gains, "fsdp", nf), fi, 1).astype(F32)
    gain_one, gain_two = gains[0], gains[1]
    inputs = tokens[0].astype(F32)
    incoming = cotangent[0]

    segment_row = segment_ids[0]
    offset = ci * rows
    local_segment = lax.dynamic_slice_in_dim(segment_row, offset, rows, 0)
    local_index = offset + jnp.arange(rows, dtype=jnp.int32)
    earlier = jnp.sum((segment_row[None, :] < local_segment[:, None]).astype(jnp.int32), axis=1)
    position = (local_index - earlier).astype(F32)
    freqs = 10000.0 ** (-(jnp.arange(HD // 4, dtype=F32) * 2.0 / (HD // 2)))
    angle = position[:, None] * freqs[None, :]
    cosine = jnp.cos(angle)
    sine = jnp.sin(angle)

    normed_attn = rms_scale(inputs, gain_one).astype(BF)
    normed_slab = rows_to_slabs(normed_attn)
    kv_half = cut(w_keyval, ti * HD, HD, 1)
    partial = jnp.concatenate(
        [matmul(normed_slab, w_query).astype(BF), matmul(normed_slab, kv_half).astype(BF)], axis=1
    )
    projected = reduce_rows(partial, qcols + HD)
    query = projected[:, :qcols].reshape(rows, heads, HD)
    keyval = projected[:, qcols:]
    query_rows = (
        rotate(query, cosine[:, None, :], sine[:, None, :]).reshape(rows * heads, HD).astype(BF)
    )
    keyval = jnp.where(ti == 0, rotate(keyval, cosine, sine), keyval).astype(BF)
    kv_all = jnp.concatenate(gather_blocks(keyval, "ctx", nc), axis=0)
    kv_other = swap(kv_all, "tp", nt, 1)
    key_all = jnp.where(ti == 0, kv_all, kv_other)
    value_all = jnp.where(ti == 0, kv_other, kv_all)

    key_index = jnp.concatenate(
        [(ci ^ k) * rows + jnp.arange(rows, dtype=jnp.int32) for k in range(nc)]
    )
    key_segment = jnp.concatenate(
        [lax.dynamic_slice_in_dim(segment_row, (ci ^ k) * rows, rows, 0) for k in range(nc)]
    )
    row_index = jnp.repeat(local_index, heads)
    row_segment = jnp.repeat(local_segment, heads)
    mask = (row_segment[:, None] == key_segment[None, :]) & (
        key_index[None, :] <= row_index[:, None]
    )
    scores = jnp.where(mask, times_transposed(query_rows, key_all) * scale, NEGATIVE)
    peak = jnp.max(scores, axis=1, keepdims=True)
    terms = jnp.exp(scores - peak)
    probs = terms / jnp.sum(terms, axis=1, keepdims=True)
    probs_low = probs.astype(BF)
    attended = matmul(probs_low, value_all).reshape(rows, qcols).astype(BF)

    attended_plane = gather_rows(attended)
    branch = tp_sum(matmul(attended_plane, w_out)).astype(BF)
    hidden_state = inputs + slabs_to_rows(branch).astype(F32)
    normed_ffn = rms_scale(hidden_state, gain_two).astype(BF)

    normed_all = gather_ctx(normed_ffn)
    incoming_all = gather_ctx(incoming)
    gate = matmul(normed_all, gate_full)
    upward = matmul(normed_all, up_full)
    d_hidden = matmul(incoming_all, down_full)
    hidden, geglu_pull = jax.vjp(geglu, gate, upward)
    hidden = hidden.astype(BF)
    d_gate, d_up = geglu_pull(d_hidden)
    d_gate = d_gate.astype(BF)
    d_up = d_up.astype(BF)

    def finish(grad, axis):
        low = grad.astype(BF)
        blocks = [cut(low, (fi ^ k) * slab, slab, axis) for k in range(nf)]
        got = all_to_all_blocks(blocks, "fsdp", nf)
        return sum(block.astype(F32) for block in got).astype(BF)

    shard_down = finish(transposed_times(hidden, incoming_all), 1)
    grad_down = lax.all_gather(shard_down, "ctx", axis=0, tiled=True).astype(F32)
    shard_gate = finish(transposed_times(normed_all, d_gate), 0)
    grad_gate = lax.all_gather(shard_gate, "ctx", axis=0, tiled=False)
    shard_up = finish(transposed_times(normed_all, d_up), 0)
    grad_up = lax.all_gather(shard_up, "ctx", axis=0, tiled=False)

    def spread(value):
        return jnp.concatenate([value[j] for j in range(nc)], axis=1).astype(F32)

    grad_gate = spread(grad_gate)
    grad_up = spread(grad_up)

    d_normed_ffn = reduce_ctx(
        times_transposed(d_gate, gate_full) + times_transposed(d_up, up_full)
    ).astype(BF)
    d_normed_ffn = both_halves(d_normed_ffn, 1).astype(F32)
    feed = reduce_ctx(times_transposed(hidden, down_full))
    output = both_halves((cut(hidden_state, ti * half, half, 1) + feed).astype(BF), 1)

    unused, norm_pull = jax.vjp(rms_scale, hidden_state, gain_two)
    d_state_norm, grad_gain_two = norm_pull(d_normed_ffn)
    d_state = incoming.astype(F32) + d_state_norm
    d_branch_slab = rows_to_slabs(d_state.astype(BF))
    grad_out = transposed_times(attended_plane, d_branch_slab)
    d_attended = reduce_rows(times_transposed(d_branch_slab, w_out).astype(BF), qcols)
    d_attended = d_attended.astype(BF).reshape(rows * heads, HD)
    d_probs = times_transposed(d_attended, value_all)
    delta = jnp.sum(probs * d_probs, axis=1, keepdims=True)
    d_scores = (probs * (d_probs - delta)).astype(BF)
    d_rows = matmul(d_scores, key_all) * scale
    d_key = transposed_times(d_scores, query_rows) * scale
    d_value = transposed_times(probs_low, d_attended)
    d_key, d_value = d_key.astype(BF), d_value.astype(BF)
    keep = jnp.where(ti == 0, d_key, d_value)
    send = jnp.where(ti == 0, d_value, d_key)
    d_kv = (keep.astype(F32) + swap(send, "tp", nt, 1).astype(F32)).astype(BF)
    d_kv = sum(
        block.astype(F32)
        for block in all_to_all_blocks(list(d_kv.reshape(nc, rows, HD)), "ctx", nc)
    )
    d_kv = jnp.where(ti == 0, unrotate(d_kv, cosine, sine), d_kv).astype(BF)
    d_query = unrotate(d_rows.reshape(rows, heads, HD), cosine[:, None, :], sine[:, None, :])
    d_query = d_query.reshape(rows, qcols).astype(BF)
    d_plane = gather_rows(jnp.concatenate([d_query, d_kv], axis=1))
    d_query_plane = d_plane[:, :qcols]
    d_kv_plane = d_plane[:, qcols:]
    d_normed = tp_sum(
        times_transposed(d_query_plane, w_query) + times_transposed(d_kv_plane, kv_half)
    ).astype(BF)
    d_normed_attn = slabs_to_rows(d_normed).astype(F32)
    grad_query = transposed_times(normed_slab, d_query_plane)
    grad_kv = transposed_times(normed_slab, d_kv_plane)
    unused, norm_pull_one = jax.vjp(rms_scale, inputs, gain_one)
    d_input_norm, grad_gain_one = norm_pull_one(d_normed_attn)
    grad_inputs = d_state + d_input_norm

    grad_out = lax.psum(grad_out.astype(BF), "ctx").astype(F32)
    grad_query = lax.psum(grad_query.astype(BF), "ctx").astype(F32)
    grad_kv = lax.psum(grad_kv.astype(BF), "ctx")
    grad_kv = both_halves(grad_kv, 1).astype(F32)
    gain_grads = jnp.stack([grad_gain_one, grad_gain_two])
    gain_blocks = [cut(gain_grads, (fi ^ k) * slab, slab, 1) for k in range(nf)]
    gain_grads = sum(all_to_all_blocks(gain_blocks, "fsdp", nf))
    step = 1
    while step < nc:
        gain_grads = gain_grads + swap(gain_grads, "ctx", nc, step)
        step *= 2
    return (
        output[None],
        grad_inputs[None],
        grad_query,
        grad_kv,
        grad_out,
        grad_gate,
        grad_up,
        grad_down,
        gain_grads[0],
        gain_grads[1],
    )


def partners(axis, size):
    me = lax.axis_index(axis)
    flip = me + 1 - 2 * lax.rem(me, 2)
    return [me, flip, lax.rem(me + 2, size), size - 1 - me]


class Wire:
    def __init__(self, send, recv):
        self.send, self.recv, self.count, self.live = send, recv, 0, []

    def __call__(self, src, dst, axis, peer):
        slot = self.count
        self.count += 1
        copy = pltpu.make_async_remote_copy(
            src_ref=src,
            dst_ref=dst,
            send_sem=self.send.at[slot],
            recv_sem=self.recv.at[slot],
            device_id={axis: peer},
            device_id_type=MESH,
        )
        copy.start()
        self.live.append(copy)
        return copy

    def settle(self, copies):
        for copy in copies:
            copy.wait_send()
            self.live = [each for each in self.live if each is not copy]

    def finish(self):
        for copy in self.live:
            copy.wait_send()


def greet(peers):
    barrier = pltpu.get_barrier_semaphore()
    for axis, peer in peers:
        pl.semaphore_signal(barrier, inc=1, device_id={axis: peer}, device_id_type=MESH)
    pl.semaphore_wait(barrier, len(peers))


def wide(value, columns):
    return jnp.concatenate([value] * (columns // value.shape[1]), axis=1)


def nt_dot(left, right):
    return lax.dot_general(left, right, (((1,), (1,)), ((), ())), preferred_element_type=F32)


def tn_dot(left, right):
    return lax.dot_general(left, right, (((0,), (0,)), ((), ())), preferred_element_type=F32)


class Gather:
    def __init__(self, wire, fs, pieces, height, place, own=None):
        self.wire, self.fs, self.pieces, self.height = wire, fs, pieces, height
        self.place, self.own = place, own
        self.arrivals = {}

    def strip(self, p):
        return pl.ds(p * self.height, self.height)

    def send(self, m, p, k):
        target = self.place(m, self.fs[0], self.strip(p))
        source = self.own.at[self.strip(p), :] if self.own is not None else target
        self.arrivals[m, p, k] = self.wire(source, target, "fsdp", self.fs[k])

    def pass_on(self, m, p, k, to):
        self.arrivals.pop((m, p, k)).wait_recv()
        target = self.place(m, self.fs[k], self.strip(p))
        self.arrivals[m, p, 3] = self.wire(target, target, "fsdp", self.fs[to])

    def steps(self, which, prepare):
        half = self.pieces // 2
        for m in which:
            prepare(m)
            for i in range(half):
                self.send(m, i, 1)
                self.send(m, half + i, 2)
                yield
            for i in range(half):
                self.pass_on(m, half + i, 2, 1)
                self.pass_on(m, i, 1, 2)
                yield
            for i in range(half):
                self.send(m, half + i, 1)
                self.send(m, i, 2)
                yield

    def settle(self):
        for copy in self.arrivals.values():
            copy.wait_recv()


def middle_kernel(
    w_down,
    shard_down,
    cot_in,
    normed_in,
    gate_in,
    up_in,
    hidden_in,
    gate_w_in,
    up_w_in,
    d_up,
    dn,
    part,
    shard_gate,
    down_all,
    dfull,
    cot,
    normed,
    gate,
    upward,
    hidden,
    gate_w,
    up_w,
    dh,
    d_gate,
    parts,
    near,
    far,
    sums,
    sems,
    send,
    recv,
    local,
):
    fs, cs = partners("fsdp", 4), partners("ctx", 4)
    ci = lax.axis_index("ctx")
    units, slab = dfull.shape[1:]
    length, _ = cot.shape
    loads = [
        pltpu.make_async_copy(source, target, local.at[n])
        for n, (source, target) in enumerate(
            (
                (w_down.at[pl.ds(pl.multiple_of(ci * units, 64), units), :], dfull.at[fs[0]]),
                (cot_in, cot),
                (gate_in, gate),
                (up_in, upward),
                (normed_in, normed),
                (gate_w_in, gate_w),
                (up_w_in, up_w),
                (hidden_in, hidden),
            )
        )
    ]
    loads[0].start()
    greet([("fsdp", fs[1]), ("fsdp", fs[2]), ("ctx", cs[1]), ("ctx", cs[3])])
    for load in loads[1:]:
        load.start()
    wire = Wire(send, recv)
    spread = Spread(shard_down, down_all, PIECES, *sems)
    spread.begin()
    for p in range(PIECES):
        spread.give(p)
    gather = Gather(wire, fs, 10, units // 10, lambda m, index, at: dfull.at[index, at, :])

    def prepare(m):
        loads[0].wait()

    def lanes(index):
        return pl.ds(pl.multiple_of(index * slab, slab), slab)

    for n, _ in enumerate(gather.steps((0,), prepare)):
        if n == 3:
            loads[1].wait()
            dh[...] = nt_dot(cot[:, lanes(fs[0])], dfull[fs[0]])
        if n >= 15 - PIECES:
            spread.hand_on(n - 15 + PIECES)
    for load in loads[2:]:
        load.wait()
    gather.settle()
    for k in (1, 2, 3):
        dh[...] += nt_dot(cot[:, lanes(fs[k])], dfull[fs[k]])
    step = 128
    for n in range(length // step):
        at = slice(n * step, (n + 1) * step)
        v, d = gate[at, :], dh[at, :]
        square = v * v
        t = jnp.tanh(0.7978845608028654 * (v + 0.044715 * (square * v)))
        cdf = 0.5 * (1.0 + t)
        slope = cdf + (0.5 * v) * (1.0 - t * t) * (
            0.7978845608028654 * (1.0 + 0.134145 * square)
        )
        d_gate[at, :] = (d * upward[at, :] * slope).astype(BF)
        d_up[at, :] = (d * (v * cdf)).astype(BF)
    product = Product(wire, True, d_gate, normed, shard_gate, parts, near, far, sums)
    product.start()
    for p in range(PIECES // 2):
        spread.hand_far(p)

    def turn_back(j, carry):
        block = jnp.dot(d_gate[...], gate_w[j], preferred_element_type=F32)
        block += jnp.dot(d_up[...], up_w[j], preferred_element_type=F32)
        dn[:, lanes(j)] = block.astype(BF)
        return carry

    lax.fori_loop(0, 4, turn_back, 0)
    product.middle()
    for p in range(PIECES // 2, PIECES):
        spread.hand_far(p)

    def feed(j, carry):
        block = jnp.dot(hidden[...], dfull[j], preferred_element_type=F32)
        part[:, lanes(j)] = block.astype(BF)
        return carry

    lax.fori_loop(0, 4, feed, 0)
    product.end()
    spread.close()
    wire.finish()


def call_middle(w_down, shard_down, cot, normed, gate, upward, hidden, gate_w, up_w):
    units, slab = shard_down.shape
    length, depth = cot.shape
    sizes = product_sizes(True, slab, units)
    pair = [pltpu.VMEM((2, *size), BF) for size in sizes]
    single = [pltpu.VMEM(size, BF) for size in sizes]
    shape = jax.ShapeDtypeStruct
    vmem = pl.BlockSpec(memory_space=pltpu.VMEM)
    hbm = pl.BlockSpec(memory_space=pl.ANY)
    return pl.pallas_call(
        middle_kernel,
        out_shape=[
            shape((length, units), BF),
            shape((length, depth), BF),
            shape((length, depth), BF),
            shape((units, slab), BF),
            shape((4, units, slab), BF),
        ],
        in_specs=[hbm] * 9,
        out_specs=[vmem] * 4 + [hbm],
        scratch_shapes=[
            pltpu.VMEM((4, units, slab), BF),
            pltpu.VMEM((length, depth), BF),
            pltpu.VMEM((length, depth), BF),
            pltpu.VMEM((length, units), F32),
            pltpu.VMEM((length, units), F32),
            pltpu.VMEM((length, units), BF),
            pltpu.VMEM((4, units, slab), BF),
            pltpu.VMEM((4, units, slab), BF),
            pltpu.VMEM((length, units), F32),
            pltpu.VMEM((length, units), BF),
            list(pair),
            list(pair),
            list(single),
            list(single),
            spread_scratch(PIECES),
            pltpu.SemaphoreType.DMA((40,)),
            pltpu.SemaphoreType.DMA((40,)),
            pltpu.SemaphoreType.DMA((8,)),
        ],
        compiler_params=pltpu.CompilerParams(
            collective_id=2, has_side_effects=True, vmem_limit_bytes=67_043_328
        ),
        cost_estimate=pl.CostEstimate(
            flops=12 * length * depth * units, bytes_accessed=300_000_000, transcendentals=0
        ),
        name="feed_forward_backward",
    )(w_down, shard_down, cot, normed, gate, upward, hidden, gate_w, up_w)


def forward_kernel(
    heads,
    tok,
    cot,
    seg,
    freq,
    gain_a,
    gain_f,
    w_q,
    w_kv,
    w_o,
    w_gate,
    w_up,
    q_rot,
    kv_out,
    probs,
    state,
    gains_all,
    normed_all,
    cot_all,
    gate_full,
    up_full,
    normed_slab,
    att_plane,
    gate,
    upward,
    hidden,
    shard,
    cos,
    sin,
    xbuf,
    rbuf,
    part,
    precv,
    kvbuf,
    attbuf,
    obuf,
    orecv,
    bbuf,
    brecv,
    nown,
    grel,
    window,
    wfull,
    nall,
    call,
    parts,
    near,
    far,
    sums,
    keep,
    send,
    recv,
    local,
):
    fs, cs = partners("fsdp", 4), partners("ctx", 4)
    ci, ti = lax.axis_index("ctx"), lax.axis_index("tp")
    other = 1 - ti
    rows, depth = tok.shape
    slab = depth // 4
    hrows = rows // 2
    qcols = heads * HD
    units = gate_full.shape[1]
    scale = HD ** (-0.5)
    wire = Wire(send, recv)
    locals_ = []

    def keep_local(src, dst):
        copy = pltpu.make_async_copy(src, dst, local.at[len(locals_)])
        copy.start()
        locals_.append(copy)
        return copy

    def lanes(index):
        return pl.ds(pl.multiple_of(index * slab, slab), slab)

    mine = pl.ds(pl.multiple_of(ti * hrows, hrows), hrows)
    first = pl.ds(pl.multiple_of(((ci * units) // 128) * 128, 128), window.shape[2])
    win = [
        keep_local(w_gate.at[:, first], window.at[0]),
        keep_local(w_up.at[:, first], window.at[1]),
    ]
    greet(
        [("fsdp", fs[k]) for k in (1, 2, 3)]
        + [("ctx", cs[k]) for k in (1, 2, 3)]
        + [("tp", other)]
    )

    x_in = [None] * 4
    for k in (1, 2, 3):
        x_in[k] = wire(tok.at[mine, lanes(fs[k])], xbuf.at[k, mine, :], "fsdp", fs[k])
    grel[0] = jnp.zeros((8, slab), F32)
    grel[0, 0:1, :] = gain_a[...].astype(F32)
    grel[0, 1:2, :] = gain_f[...].astype(F32)
    g_in = [None] * 4
    for k in (1, 2, 3):
        g_in[k] = wire(grel.at[0], grel.at[k], "fsdp", fs[k])
    xbuf[0] = tok[:, lanes(fs[0])]
    x = tok[...].astype(F32)
    r = lax.rsqrt(jnp.sum(x * x, axis=1, keepdims=True) * (1.0 / depth) + 1e-06)
    rbuf[0] = jnp.broadcast_to(r, (rows, 128))
    r_in = [None] * 4
    for k in (1, 2, 3):
        r_in[k] = wire(rbuf.at[0, mine, :], rbuf.at[k, mine, :], "fsdp", fs[k])
    c_in = [None] * 4
    for k in (1, 2, 3):
        c_in[k] = wire(cot.at[mine, :], call.at[ci, ti], "ctx", cs[k])
    for half in (0, 1):
        call[ci, half] = cot[half * hrows : (half + 1) * hrows, :]

    odd = units % 128
    pieces = 10
    height = units // pieces

    def prepare(m):
        win[m].wait()
        if odd:

            @pl.when(lax.rem(ci, 2) == 0)
            def _():
                wfull[m, fs[0]] = window[m, :, 0:units].T

            @pl.when(lax.rem(ci, 2) == 1)
            def _():
                wfull[m, fs[0]] = window[m, :, odd : odd + units].T
        else:
            wfull[m, fs[0]] = window[m, :, 0:units].T

    gather = Gather(wire, fs, pieces, height, lambda m, index, at: wfull.at[m, index, at, :])
    schedule = gather.steps((0, 1), prepare)

    def bulk(count):
        for _ in range(count):
            next(schedule, None)

    bulk(BULK[0])
    gain_one = grel[0, 0:1, :]
    kv_half = w_kv[:, pl.ds(pl.multiple_of(ti * HD, HD), HD)]
    p_in = [None] * 4
    pass_x = {}
    for k in range(4):
        if k == 1:
            for j in (1, 2, 3):
                x_in[j].wait_recv()
                r_in[j].wait_recv()
                for buffer in (xbuf, rbuf):
                    half = buffer.at[j, mine, :]
                    pass_x[j, buffer is rbuf] = wire(half, half, "tp", other)
        if k:
            pass_x[k, False].wait_recv()
            pass_x[k, True].wait_recv()
        normed = (xbuf[k].astype(F32) * wide(rbuf[k], slab) * gain_one).astype(BF)
        normed_slab[k] = normed
        part[k, :, 0:qcols] = jnp.dot(normed, w_q[...], preferred_element_type=F32).astype(BF)
        part[k, :, qcols:] = jnp.dot(normed, kv_half, preferred_element_type=F32).astype(BF)
        if k:
            p_in[k] = wire(part.at[k], precv.at[k], "fsdp", fs[k])
    bulk(BULK[1])

    def segment(index):
        at = pl.ds(pl.multiple_of(index * rows, rows), rows)
        return jnp.broadcast_to(seg[:, at].astype(F32), (rows, rows))

    mine_segment = segment(ci).T
    row_index = lax.broadcasted_iota(jnp.int32, (rows, rows), 0) + ci * rows
    lane = lax.broadcasted_iota(jnp.int32, (rows, rows), 1)
    earlier = jnp.zeros((rows, 1), F32)
    for k in range(4):
        theirs = segment(cs[k])
        earlier += jnp.sum(jnp.where(theirs < mine_segment, 1.0, 0.0), axis=1, keepdims=True)
        inside = jnp.logical_and(theirs == mine_segment, lane + cs[k] * rows <= row_index)
        keep[:, k * rows : (k + 1) * rows] = jnp.where(inside, 1.0, 0.0)
    angle = (row_index.astype(F32) - earlier) * freq[...]
    cos[...] = jnp.cos(angle)
    turned = jnp.sin(angle)
    sin[...] = jnp.where(lane < HD // 4, -turned, turned)
    for k in (1, 2, 3):
        p_in[k].wait_recv()

    def total(start, size):
        out = part[0, :, start : start + size].astype(F32)
        for k in (1, 2, 3):
            out += precv[k, :, start : start + size].astype(F32)
        return out

    c, s = cos[...], sin[...]
    zero = (1 - ti).astype(F32)
    kvbuf[ti, 0] = turn(total(qcols, HD), c * zero + (1.0 - zero), s * zero).astype(BF)
    kv_in = [None] * 4
    for k in (1, 2, 3):
        kv_in[k] = wire(kvbuf.at[ti, 0], kvbuf.at[ti, k], "ctx", cs[k])
    kv_side = [wire(kvbuf.at[ti, 0], kvbuf.at[ti, 0], "tp", other)]
    for h in range(heads):
        q_rot[:, h * HD : (h + 1) * HD] = turn(total(h * HD, HD), c, s).astype(BF)
    bulk(BULK[2])
    for k in (1, 2, 3):
        kv_in[k].wait_recv()
        kv_side.append(wire(kvbuf.at[ti, k], kvbuf.at[ti, k], "tp", other))
    for copy in kv_side:
        copy.wait_recv()
    length = 4 * rows
    keys = kvbuf[0].reshape(length, HD)
    values = kvbuf[1].reshape(length, HD)
    kv_out[...] = kvbuf[...]
    seen = keep[...] > 0.5
    for h in range(heads):
        sc = nt_dot(q_rot[:, h * HD : (h + 1) * HD], keys) * scale
        sc = jnp.where(seen, sc, NEGATIVE)
        e = jnp.exp(sc - jnp.max(sc, axis=1, keepdims=True))
        p = e / jnp.sum(e, axis=1, keepdims=True)
        probs[h] = p
        attbuf[0, :, h * HD : (h + 1) * HD] = jnp.dot(
            p.astype(BF), values, preferred_element_type=F32
        ).astype(BF)
    a_in = {}
    for k in (1, 2):
        a_in[k] = wire(attbuf.at[0], attbuf.at[k], "fsdp", fs[k])
    bulk(BULK[3])
    c_side = []
    for k in (1, 2, 3):
        c_in[k].wait_recv()
        c_side.append(wire(call.at[cs[k], ti], call.at[cs[k], ti], "tp", other))
    o_in = []
    for k in range(4):
        if k == 1:
            for j, to, start in ((1, 2, 0), (2, 1, hrows)):
                a_in[j].wait_recv()
                a_in[3, j] = wire(
                    attbuf.at[j, pl.ds(start, hrows), :],
                    attbuf.at[3, pl.ds(start, hrows), :],
                    "fsdp",
                    fs[to],
                )
        if k == 3:
            a_in[3, 1].wait_recv()
            a_in[3, 2].wait_recv()
        att_plane[k] = attbuf[k]
        block = jnp.dot(attbuf[k], w_o[...], preferred_element_type=F32).astype(BF)
        obuf[k, 0] = block[0:hrows]
        obuf[k, 1] = block[hrows:rows]
        o_in.append(wire(obuf.at[k, other], orecv.at[k], "tp", other))
    b_in = [None] * 4
    for k in (1, 2, 3, 0):
        o_in[k].wait_recv()
        both = (obuf[k, ti].astype(F32) + orecv[k].astype(F32)).astype(BF)
        if k:
            bbuf[k] = both
            b_in[k] = wire(bbuf.at[k], brecv.at[k], "fsdp", fs[k])
        else:
            brecv[0] = both
    bulk(BULK[4])
    for k in (1, 2, 3):
        g_in[k].wait_recv()
    gains_all[...] = grel[...]
    squares = jnp.zeros((hrows, 1), F32)
    for k in range(4):
        if k:
            b_in[k].wait_recv()
        h_new = tok[mine, lanes(fs[k])].astype(F32) + brecv[k].astype(F32)
        state[:, lanes(fs[k])] = h_new
        squares += jnp.sum(h_new * h_new, axis=1, keepdims=True)
    r2 = lax.rsqrt(squares * (1.0 / depth) + 1e-06)
    for k in range(4):
        nown[:, lanes(fs[k])] = (state[:, lanes(fs[k])] * r2 * grel[k, 1:2, :]).astype(BF)
    n_in = [None] * 4
    for k in (1, 2, 3):
        n_in[k] = wire(nown, nall.at[ci, ti], "ctx", cs[k])
    n_side = [wire(nown, nall.at[ci, ti], "tp", other)]
    nall[ci, ti] = nown[...]
    bulk(BULK[5])
    for k in (1, 2, 3):
        n_in[k].wait_recv()
        n_side.append(wire(nall.at[cs[k], ti], nall.at[cs[k], ti], "tp", other))
        bulk(BULK[6])
    bulk(1000)
    for copy in n_side:
        copy.wait_recv()

    def project(f):
        x = nall[:, :, :, lanes(f)].reshape(length, slab)
        return nt_dot(x, wfull[0, f]), nt_dot(x, wfull[1, f])

    gate[...], upward[...] = project(fs[0])
    gather.settle()
    keep_local(wfull.at[0], gate_full)
    keep_local(wfull.at[1], up_full)
    for k in (1, 2, 3):
        g, u = project(fs[k])
        gate[...] += g
        upward[...] += u
    for k in range(4):
        at = slice(k * rows, (k + 1) * rows)
        g = gate[at, :]
        cdf = 0.5 * (1.0 + jnp.tanh(0.7978845608028654 * (g + 0.044715 * (g * g * g))))
        hidden[at, :] = (g * cdf * upward[at, :]).astype(BF)
    keep_local(nall, normed_all)
    for copy in c_side:
        copy.wait_recv()
    keep_local(call, cot_all)
    product = Product(wire, True, hidden, call, shard, parts, near, far, sums)
    product.start()
    product.middle()
    product.end()
    for copy in locals_[2:]:
        copy.wait()
    wire.finish()


BULK = (4, 5, 4, 4, 4, 7, 1)


def call_forward(heads, tok, cot, seg, freq, gain_a, gain_f, w_q, w_kv, w_o, w_gate, w_up):
    rows, depth = tok.shape
    slab, hrows, qcols, length = depth // 4, rows // 2, heads * HD, 4 * rows
    units = w_gate.shape[1] // 4
    reach = -(-(units + units % 128) // 128) * 128
    shape = jax.ShapeDtypeStruct
    vmem = pl.BlockSpec(memory_space=pltpu.VMEM)
    hbm = pl.BlockSpec(memory_space=pl.ANY)
    pcols = qcols + HD
    sizes = product_sizes(True, slab, units)
    pair = [pltpu.VMEM((2, *size), BF) for size in sizes]
    single = [pltpu.VMEM(size, BF) for size in sizes]
    return pl.pallas_call(
        functools.partial(forward_kernel, heads),
        out_shape=[
            shape((rows, qcols), BF),
            shape((2, 4, rows, HD), BF),
            shape((heads, rows, length), F32),
            shape((hrows, depth), F32),
            shape((4, 8, slab), F32),
            shape((4, 2, hrows, depth), BF),
            shape((4, 2, hrows, depth), BF),
            shape((4, units, slab), BF),
            shape((4, units, slab), BF),
            shape((4, rows, slab), BF),
            shape((4, rows, qcols), BF),
            shape((length, units), F32),
            shape((length, units), F32),
            shape((length, units), BF),
            shape((units, slab), BF),
            shape((rows, 128), F32),
            shape((rows, 128), F32),
        ],
        in_specs=[vmem] * 9 + [hbm] * 2,
        out_specs=[vmem] * 5 + [hbm] * 4 + [vmem] * 8,
        scratch_shapes=[
            pltpu.VMEM((4, rows, slab), BF),
            pltpu.VMEM((4, rows, 128), F32),
            pltpu.VMEM((4, rows, pcols), BF),
            pltpu.VMEM((4, rows, pcols), BF),
            pltpu.VMEM((2, 4, rows, HD), BF),
            pltpu.VMEM((4, rows, qcols), BF),
            pltpu.VMEM((4, 2, hrows, slab), BF),
            pltpu.VMEM((4, hrows, slab), BF),
            pltpu.VMEM((4, hrows, slab), BF),
            pltpu.VMEM((4, hrows, slab), BF),
            pltpu.VMEM((hrows, depth), BF),
            pltpu.VMEM((4, 8, slab), F32),
            pltpu.VMEM((2, slab, reach), BF),
            pltpu.VMEM((2, 4, units, slab), BF),
            pltpu.VMEM((4, 2, hrows, depth), BF),
            pltpu.VMEM((4, 2, hrows, depth), BF),
            list(pair),
            list(pair),
            list(single),
            list(single),
            pltpu.VMEM((rows, length), F32),
            pltpu.SemaphoreType.DMA((132,)),
            pltpu.SemaphoreType.DMA((132,)),
            pltpu.SemaphoreType.DMA((12,)),
        ],
        compiler_params=pltpu.CompilerParams(
            collective_id=1, has_side_effects=True, vmem_limit_bytes=67_043_328
        ),
        cost_estimate=pl.CostEstimate(
            flops=2 * length * slab * (2 * qcols + HD), bytes_accessed=400_000_000, transcendentals=0
        ),
        name="attention_forward",
    )(tok, cot, seg, freq, gain_a, gain_f, w_q, w_kv, w_o, w_gate, w_up)


class Product:
    def __init__(self, wire, flip, left, right, shard, mine, near, far, sums):
        self.wire, self.flip, self.left, self.right, self.shard = wire, flip, left, right, shard
        self.mine, self.near, self.far, self.sums = mine, near, far, sums
        self.fs = partners("fsdp", 4)
        self.slab = shard.shape[1] if flip else shard.shape[0]
        units = shard.shape[0] if flip else shard.shape[1]
        cut = 128 * ((units + 255) // 256)
        self.spans = ((0, cut), (cut, units - cut))
        self.first, self.second = (1, 2), (2, 1)
        self.one, self.two = {}, {}

    def piece(self, k, half):
        start, size = self.spans[half]
        block = pl.ds(pl.multiple_of(self.fs[k] * self.slab, self.slab), self.slab)
        if self.flip:
            right = self.right[..., block]
            right = right.reshape(-1, right.shape[-1])
            return tn_dot(self.left[:, start : start + size], right)
        return tn_dot(self.left[:, block], self.right[:, start : start + size])

    def start(self):
        for slot in (0, 1):
            for half in (0, 1):
                k = 3 if slot == 0 else self.first[half]
                self.mine[half][slot] = self.piece(k, half).astype(BF)
                self.one[half, slot] = self.wire(
                    self.mine[half].at[slot],
                    self.near[half].at[slot],
                    "fsdp",
                    self.fs[self.first[half]],
                )

    def middle(self):
        for half in (0, 1):
            own = self.piece(self.second[half], half)
            self.one[half, 0].wait_recv()
            self.sums[half][...] = (own + self.near[half][0].astype(F32)).astype(BF)
            self.two[half] = self.wire(
                self.sums[half], self.far[half], "fsdp", self.fs[self.second[half]]
            )

    def end(self):
        for half in (0, 1):
            start, size = self.spans[half]
            own = self.piece(0, half)
            self.one[half, 1].wait_recv()
            own += self.near[half][1].astype(F32)
            self.two[half].wait_recv()
            own += self.far[half][...].astype(F32)
            if self.flip:
                self.shard[start : start + size, :] = own.astype(BF)
            else:
                self.shard[:, start : start + size] = own.astype(BF)


def product_sizes(flip, slab, units):
    cut = 128 * ((units + 255) // 256)
    return [(size, slab) if flip else (slab, size) for size in (cut, units - cut)]


def turn(value, c, s):
    front = value[:, 0:128]
    return jnp.concatenate(
        [front * c + pltpu.roll(front, 64, 1) * s, value[:, 128:256]], axis=1
    )


class Line:
    def __init__(self, own, inbox, outbox, total, send, recv):
        self.own, self.inbox, self.outbox, self.total = own, inbox, outbox, total
        self.send, self.recv = send, recv
        self.ci = lax.axis_index("ctx")

    def copy(self, way, u):
        step = 1 if way == 0 else 3
        return pltpu.make_async_remote_copy(
            src_ref=self.outbox.at[way, u - 1 + way],
            dst_ref=self.inbox.at[way, u - 1 + way],
            send_sem=self.send.at[way, u - 1 + way],
            recv_sem=self.recv.at[way, u - 1 + way],
            device_id={"ctx": lax.rem(self.ci + step, 4)},
            device_id_type=MESH,
        )

    def sends(self, way, u):
        return self.ci < u if way == 0 else self.ci > u

    def fed(self, way):
        return self.ci > 0 if way == 0 else self.ci < 3

    def lead(self):
        for step in range(3):
            for way, u in ((0, 3 - step), (1, step)):

                @pl.when(jnp.logical_and(self.sends(way, u), jnp.logical_not(self.fed(way))))
                def _():
                    self.outbox[way, u - 1 + way] = self.own(u).astype(BF)
                    self.copy(way, u).start()

    def hop(self, way, u):
        self.copy(way, u).wait_recv()
        slot = u - 1 + way
        self.outbox[way, slot] = (self.own(u) + self.inbox[way, slot].astype(F32)).astype(BF)
        self.copy(way, u).start()

    def push_near(self, steps=(0, 1)):
        for step in steps:

            @pl.when(self.ci == 1)
            def _():
                self.hop(0, 3 - step)

            @pl.when(self.ci == 2)
            def _():
                self.hop(1, step)

    def push_far(self):
        @pl.when(self.ci == 1)
        def _():
            self.hop(1, 0)

        @pl.when(self.ci == 2)
        def _():
            self.hop(0, 3)

    def collect(self):
        self.total[...] = self.own(self.ci)
        for way in (0, 1):

            @pl.when(self.fed(way))
            def _():
                self.copy(way, self.ci).wait_recv()
                self.total[...] += self.inbox[way, self.ci - 1 + way].astype(F32)

    def drain(self):
        for way in (0, 1):
            for u in range(1 - way, 4 - way):

                @pl.when(self.sends(way, u))
                def _():
                    self.copy(way, u).wait_send()


def line_scratch(*form):
    return [
        pltpu.VMEM((2, 3, *form), BF),
        pltpu.VMEM((2, 3, *form), BF),
        pltpu.VMEM(form, F32),
        pltpu.SemaphoreType.DMA((2, 3)),
        pltpu.SemaphoreType.DMA((2, 3)),
    ]


class Spread:
    def __init__(self, own, full, pieces, send, recv, local, height=None):
        self.own, self.full, self.pieces = own, full, pieces
        self.send, self.recv = send, recv
        self.height = height or own.shape[0] // pieces
        self.cs = partners("ctx", 4)
        self.ci = self.cs[0]
        self.inner = jnp.logical_and(self.ci > 0, self.ci < 3)
        self.local = local

    def strip(self, p):
        return pl.ds(p * self.height, self.height)

    def copy(self, kind, p, source, peer):
        place = self.full.at[source, self.strip(p), :]
        src = self.own.at[self.strip(p), :] if kind < 2 else place
        slot = (0, 1, 2, 1, 2)[kind]
        return pltpu.make_async_remote_copy(
            src_ref=src,
            dst_ref=place,
            send_sem=self.send.at[kind, p],
            recv_sem=self.recv.at[slot, p],
            device_id={"ctx": peer},
            device_id_type=MESH,
        )

    def out(self, kind, p):
        cs = self.cs
        source = (cs[0], cs[0], cs[1], cs[3], cs[2])[kind]
        peer = (cs[1], cs[3], cs[3], cs[1], cs[1])[kind]
        return self.copy(kind, p, source, peer)

    def arrived(self, slot, p):
        self.copy((0, 1, 2)[slot], p, self.ci, self.cs[1]).wait_recv()

    def keep(self):
        return pltpu.make_async_copy(self.own, self.full.at[self.ci], self.local)

    def begin(self):
        self.keep().start()

    def give(self, p):
        self.out(0, p).start()

        @pl.when(self.inner)
        def _():
            self.out(1, p).start()

    def hand_on(self, p):
        @pl.when(self.inner)
        def _():
            self.arrived(0, p)
            self.out(2, p).start()
            self.arrived(1, p)
            self.out(3, p).start()

    def hand_far(self, p):
        @pl.when(self.inner)
        def _():
            self.arrived(2, p)
            self.out(4, p).start()

    def close(self, near=True, far=True):
        for p in range(self.pieces):

            @pl.when(jnp.logical_not(self.inner))
            def _():
                for slot in range(0 if near else 2, 3 if far else 2):
                    self.arrived(slot, p)

            if near:
                self.out(0, p).wait_send()

            @pl.when(self.inner)
            def _():
                if near and not far:
                    self.arrived(2, p)
                for kind in range(1 if near else 4, 5 if far else 4):
                    self.out(kind, p).wait_send()

        if near:
            self.keep().wait()

    def hand_again(self, p):
        @pl.when(self.inner)
        def _():
            self.out(4, p).start()


def spread_scratch(pieces):
    return [
        pltpu.SemaphoreType.DMA((5, pieces)),
        pltpu.SemaphoreType.DMA((3, pieces)),
        pltpu.SemaphoreType.DMA,
    ]


def units_line(wire, part, side, line_refs, ti):
    other = 1 - ti
    side_in = [wire(part.at[u, other], side.at[u], "tp", other) for u in range(4)]
    for copy in side_in:
        copy.wait_recv()
    return Line(lambda u: part[u, ti].astype(F32) + side[u].astype(F32), *line_refs)


def backward_kernel(
    heads,
    dn,
    cot_in,
    state,
    gains_all,
    probs_in,
    q_rot_in,
    kv_in,
    cos,
    sin,
    w_o_in,
    normed_in,
    att_in,
    normed_all,
    shard_gate,
    d_up,
    part_in,
    tok_in,
    w_q_in,
    w_kv_in,
    out,
    grad_tok,
    gain_grads,
    gate_all,
    up_all,
    weights_all,
    kv_side,
    side,
    dbuf,
    dslab,
    dpart,
    dfar,
    dkv2,
    kvt,
    zk,
    zfar,
    dqbuf,
    dkvbuf,
    dk_acc,
    dv_acc,
    own_out,
    own_query,
    row_refs,
    out_refs,
    query_refs,
    parts,
    sums,
    product_recv,
    shard_up,
    gate_sems,
    up_sems,
    gpart,
    weight_grads,
    weight_sems,
    last_sems,
    obuf,
    gbuf,
    pbuf,
    pside,
    nbuf,
    nrow,
    gfar,
    gsum,
    gnear,
    gall,
    late,
    late_sems,
    send,
    recv,
    local,
):
    fs, cs = partners("fsdp", 4), partners("ctx", 4)
    ci, ti = lax.axis_index("ctx"), lax.axis_index("tp")
    other = 1 - ti
    hrows, depth = state.shape
    rows = 2 * hrows
    slab = depth // 4
    length = 4 * rows
    scale = HD ** (-0.5)
    sources = (cot_in, probs_in, q_rot_in, kv_in, w_o_in, normed_in, att_in, part_in, tok_in, w_q_in, w_kv_in)
    cot, probs, q_rot, kv, w_o, normed, att, part, tok, w_q, w_kv = late
    loads = [
        pltpu.make_async_copy(source, target, late_sems.at[n])
        for n, (source, target) in enumerate(zip(sources, late))
    ]
    greet(
        [("fsdp", fs[k]) for k in (1, 2, 3)]
        + [("ctx", cs[k]) for k in (1, 2, 3)]
        + [("tp", other)]
    )
    wire = Wire(send, recv)
    mine = pl.ds(pl.multiple_of(ti * hrows, hrows), hrows)

    def lanes(index):
        return pl.ds(pl.multiple_of(index * slab, slab), slab)

    up = Product(wire, True, d_up, normed_all, shard_up, parts, *product_recv, sums)
    gate_line = Spread(shard_gate, gate_all, PIECES, *gate_sems)
    up_line = Spread(shard_up, up_all, PIECES, *up_sems)
    line = units_line(wire, dn, side, row_refs, ti)
    line.lead()
    gate_line.begin()
    for p in range(PIECES // 2):
        gate_line.give(p)
    for load in loads:
        load.start()
    up.start()
    squares = jnp.zeros((hrows, 1), F32)
    for k in range(4):
        u = state[:, lanes(fs[k])]
        squares += jnp.sum(u * u, axis=1, keepdims=True)
    r = lax.rsqrt(squares * (1.0 / depth) + 1e-06)
    line.push_near()
    line.push_far()
    for p in range(PIECES // 2, PIECES):
        gate_line.give(p)
    line.collect()
    for load in loads:
        load.wait()
    inner = jnp.zeros((hrows, 1), F32)
    for k in range(4):
        at = lanes(fs[k])
        inner += jnp.sum(
            state[:, at] * gains_all[k, 1:2, :] * line.total[:, at], axis=1, keepdims=True
        )
    pull = r * r * r * (inner * (1.0 / depth))
    d_in = {}
    d_side = {}
    gpart[...] = jnp.zeros_like(gpart)
    for k in (1, 2, 3, 0):
        at = lanes(fs[k])
        u, d = state[:, at], line.total[:, at]
        ds = cot[mine, at].astype(F32) + (r * (gains_all[k, 1:2, :] * d) - u * pull)
        gbuf[ti, :, at] = ds
        if k:
            dbuf[k] = ds.astype(BF)
            d_in[k] = wire(dbuf.at[k], dslab.at[k, ti], "fsdp", fs[k])
        else:
            dslab[0, ti] = ds.astype(BF)
            d_side[0] = wire(dslab.at[0, ti], dslab.at[0, ti], "tp", other)
        gpart[k, 1:2, :] = jnp.sum(u * r * d, axis=0, keepdims=True)
    up.middle()
    for k in (1, 2, 3):
        d_in[k].wait_recv()
        d_side[k] = wire(dslab.at[k, ti], dslab.at[k, ti], "tp", other)
    for p in range(PIECES // 2):
        gate_line.hand_on(p)
    a_in = {}
    for k in (1, 2, 3, 0):
        d_side[k].wait_recv()
        block = dslab[k].reshape(rows, slab)
        dpart[k] = nt_dot(block, w_o[...]).astype(BF)
        if k:
            a_in[k] = wire(dpart.at[k], dfar.at[k], "fsdp", fs[k])
    for p in range(PIECES // 2, PIECES):
        gate_line.hand_on(p)
    up.end()
    keys = kv[0].reshape(length, HD)
    values = kv[1].reshape(length, HD)
    c, s = cos[...], sin[...]
    quarter = heads * HD // 4
    branch = dslab[...].reshape(length, slab)
    for u in range(4):
        columns = att[:, :, u * quarter : (u + 1) * quarter].reshape(length, quarter)
        own_out[u] = tn_dot(columns, branch).astype(BF)
    out_line = Line(lambda u: own_out[u].astype(F32), *out_refs)
    for k in (1, 2, 3):
        a_in[k].wait_recv()
    for h in range(heads):
        at = slice(h * HD, (h + 1) * HD)
        d = dpart[0, :, at].astype(F32)
        for k in (1, 2, 3):
            d += dfar[k, :, at].astype(F32)
        d = d.astype(BF)
        p = probs[h]
        dp = nt_dot(d, values)
        delta = jnp.sum(p * dp, axis=1, keepdims=True)
        dsc = (p * (dp - delta)).astype(BF)
        dq = jnp.dot(dsc, keys, preferred_element_type=F32) * scale
        dqbuf[0, :, at] = turn(dq, c, -s).astype(BF)
        dk = tn_dot(dsc, q_rot[:, at])
        dv = tn_dot(p.astype(BF), d)
        if h == 0:
            dk_acc[...] = dk
            dv_acc[...] = dv
        else:
            dk_acc[...] += dk
            dv_acc[...] += dv
    for p in range(PIECES // 2):
        gate_line.hand_far(p)
    dkv2[0] = (dk_acc[...] * scale).astype(BF).reshape(4, rows, HD)
    dkv2[1] = dv_acc[...].astype(BF).reshape(4, rows, HD)
    k_side = wire(dkv2.at[other], kvt, "tp", other)
    q_in = {}
    for k in (1, 2, 3):
        q_in[k] = wire(dqbuf.at[0], dqbuf.at[k], "fsdp", fs[k])
    k_side.wait_recv()
    z_in = {}
    for k in (1, 2, 3):
        zk[k] = (dkv2[ti, k].astype(F32) + kvt[k].astype(F32)).astype(BF)
        z_in[k] = wire(zk.at[k], zfar.at[k], "ctx", cs[k])
    out_line.lead()
    for p in range(PIECES // 2, PIECES):
        gate_line.hand_far(p)
    own = dkv2[ti, 0].astype(F32) + kvt[0].astype(F32)
    for k in (1, 2, 3):
        z_in[k].wait_recv()
        own += zfar[k].astype(F32)
    zero = (1 - ti).astype(F32)
    dkvbuf[0] = turn(own, c * zero + (1.0 - zero), -s * zero).astype(BF)
    v_in = {}
    for k in (1, 2, 3):
        v_in[k] = wire(dkvbuf.at[0], dkvbuf.at[k], "fsdp", fs[k])
    out_line.push_near()
    up_line.begin()
    for p in range(PIECES):
        up_line.give(p)
    for k in (1, 2, 3):
        q_in[k].wait_recv()
    slabs = normed[...].reshape(length, slab)
    for u in (3, 0, 2, 1):
        columns = dqbuf[:, :, u * quarter : (u + 1) * quarter].reshape(length, quarter)
        own_query[u, 0:quarter] = tn_dot(columns, slabs).astype(BF)
    for k in (1, 2, 3):
        v_in[k].wait_recv()
    for u in (3, 0, 2, 1):
        columns = dkvbuf[:, :, u * (HD // 4) : (u + 1) * (HD // 4)].reshape(length, HD // 4)
        own_query[u, quarter:] = tn_dot(columns, slabs).astype(BF)
    query_line = Line(lambda u: own_query[u].astype(F32), *query_refs)
    kv_half = w_kv[:, pl.ds(pl.multiple_of(ti * HD, HD), HD)]
    p_in = {}
    for k in (1, 2, 3, 0):
        block = (nt_dot(dqbuf[k], w_q[...]) + nt_dot(dkvbuf[k], kv_half)).astype(BF)
        pbuf[k, 0] = block[0:hrows]
        pbuf[k, 1] = block[hrows:rows]
        p_in[k] = wire(pbuf.at[k, other], pside.at[k], "tp", other)
    out_line.push_far()
    query_line.lead()
    n_in = {}
    for k in (1, 2, 3, 0):
        p_in[k].wait_recv()
        both = (pbuf[k, ti].astype(F32) + pside[k].astype(F32)).astype(BF)
        if k:
            nbuf[k] = both
            n_in[k] = wire(nbuf.at[k], nrow.at[k], "fsdp", fs[k])
        else:
            nrow[0] = both
    squares = jnp.zeros((hrows, 1), F32)
    for k in range(4):
        u = tok[mine, lanes(fs[k])].astype(F32)
        squares += jnp.sum(u * u, axis=1, keepdims=True)
    r = lax.rsqrt(squares * (1.0 / depth) + 1e-06)
    for p in range(PIECES):
        up_line.hand_on(p)
    query_line.push_near((0,))
    inner = jnp.zeros((hrows, 1), F32)
    for k in range(4):
        if k:
            n_in[k].wait_recv()
        u = tok[mine, lanes(fs[k])].astype(F32)
        inner += jnp.sum(u * gains_all[k, 0:1, :] * nrow[k].astype(F32), axis=1, keepdims=True)
    pull = r * r * r * (inner * (1.0 / depth))
    for k in range(4):
        at = lanes(fs[k])
        u, d = tok[mine, at].astype(F32), nrow[k].astype(F32)
        gbuf[ti, :, at] += (r * (gains_all[k, 0:1, :] * d) - u * pull)
        gpart[k, 0:1, :] = jnp.sum(u * r * d, axis=0, keepdims=True)
    t_side = wire(gbuf.at[ti], gbuf.at[ti], "tp", other)
    g_in = {}
    for k in (1, 2, 3):
        g_in[k] = wire(gpart.at[k], gfar.at[k], "fsdp", fs[k])
    for p in range(PIECES // 2):
        up_line.hand_far(p)
    query_line.push_far()
    query_line.push_near((1,))
    for p in range(PIECES // 2, PIECES):
        up_line.hand_far(p)
    gain_sum = gpart[0]
    for k in (1, 2, 3):
        g_in[k].wait_recv()
        gain_sum += gfar[k]
    gsum[...] = gain_sum
    near_gain = wire(gsum, gnear, "tp", other)
    near_gain.wait_recv()
    gall[ci] = gain_sum + gnear[...]
    all_gain = [wire(gall.at[ci], gall.at[ci], "ctx", cs[k]) for k in (1, 2, 3)]
    out_line.collect()
    weight_grads[0:quarter, :] = out_line.total[...].astype(BF)
    query_line.collect()
    weight_grads[quarter:, :] = query_line.total[...].astype(BF)
    weight_line = Spread(weight_grads, weights_all, PIECES, *weight_sems)
    weight_line.begin()
    for p in range(PIECES):
        weight_line.give(p)
    line.drain()
    last = units_line(wire, part, side, [*row_refs[:3], *last_sems], ti)
    last.lead()
    for p in range(PIECES):
        weight_line.hand_on(p)
    for p in range(PIECES // 2):
        weight_line.hand_far(p)
    last.push_near()
    last.push_far()
    for p in range(PIECES // 2, PIECES):
        weight_line.hand_far(p)
    last.collect()
    obuf[ti] = (state[...] + last.total[...]).astype(BF)
    o_side = wire(obuf.at[ti], obuf.at[ti], "tp", other)
    t_side.wait_recv()
    keep_t = pltpu.make_async_copy(gbuf, grad_tok, local.at[0])
    keep_t.start()
    o_side.wait_recv()
    keep_o = pltpu.make_async_copy(obuf, out, local.at[1])
    keep_o.start()
    for copy in all_gain:
        copy.wait_recv()
    gain_grads[...] = gall[0] + gall[1] + gall[2] + gall[3]
    gate_line.close()
    up_line.close()
    weight_line.close()
    tail = pl.ds(2 * quarter, HD // 4)
    kv_last = wire(weights_all.at[:, tail, :], kv_side, "tp", other)
    kv_last.wait_recv()
    for each in (last, out_line, query_line):
        each.drain()
    keep_t.wait()
    keep_o.wait()
    wire.finish()


PIECES = 4


def call_backward(
    heads, dn, cot, state, gains_all, probs, q_rot, kv, cos, sin, w_o, normed, att, normed_all, shard_gate, d_up, part, tok, w_q, w_kv
):
    hrows, depth = state.shape
    rows, slab, qcols = 2 * hrows, depth // 4, heads * HD
    length = 4 * rows
    units = d_up.shape[1]
    late = (cot, probs, q_rot, kv, w_o, normed, att, part, tok, w_q, w_kv)
    sizes = product_sizes(True, slab, units)
    pair = [pltpu.VMEM((2, *size), BF) for size in sizes]
    single = [pltpu.VMEM(size, BF) for size in sizes]
    shape = jax.ShapeDtypeStruct
    vmem = pl.BlockSpec(memory_space=pltpu.VMEM)
    hbm = pl.BlockSpec(memory_space=pl.ANY)
    return pl.pallas_call(
        functools.partial(backward_kernel, heads),
        out_shape=[
            shape((2, hrows, depth), BF),
            shape((2, hrows, depth), F32),
            shape((8, slab), F32),
            shape((4, units, slab), BF),
            shape((4, units, slab), BF),
            shape((4, qcols // 2 + HD // 4, slab), BF),
            shape((4, HD // 4, slab), BF),
        ],
        in_specs=[vmem, hbm, vmem, vmem, hbm, hbm, hbm, vmem, vmem]
        + [hbm] * 3
        + [vmem, hbm, vmem]
        + [hbm] * 4,
        out_specs=[hbm] * 2 + [vmem] + [hbm] * 4,
        scratch_shapes=[
            pltpu.VMEM((4, hrows, depth), BF),
            pltpu.VMEM((4, hrows, slab), BF),
            pltpu.VMEM((4, 2, hrows, slab), BF),
            pltpu.VMEM((4, rows, qcols), BF),
            pltpu.VMEM((4, rows, qcols), BF),
            pltpu.VMEM((2, 4, rows, HD), BF),
            pltpu.VMEM((4, rows, HD), BF),
            pltpu.VMEM((4, rows, HD), BF),
            pltpu.VMEM((4, rows, HD), BF),
            pltpu.VMEM((4, rows, qcols), BF),
            pltpu.VMEM((4, rows, HD), BF),
            pltpu.VMEM((length, HD), F32),
            pltpu.VMEM((length, HD), F32),
            pltpu.VMEM((4, qcols // 4, slab), BF),
            pltpu.VMEM((4, (qcols + HD) // 4, slab), BF),
            line_scratch(hrows, depth),
            line_scratch(qcols // 4, slab),
            line_scratch((qcols + HD) // 4, slab),
            list(pair),
            list(single),
            [list(pair), list(single)],
            pltpu.VMEM((units, slab), BF),
            spread_scratch(PIECES),
            spread_scratch(PIECES),
            pltpu.VMEM((4, 8, slab), F32),
            pltpu.VMEM((qcols // 2 + HD // 4, slab), BF),
            spread_scratch(PIECES),
            [pltpu.SemaphoreType.DMA((2, 3)), pltpu.SemaphoreType.DMA((2, 3))],
            pltpu.VMEM((2, hrows, depth), BF),
            pltpu.VMEM((2, hrows, depth), F32),
            pltpu.VMEM((4, 2, hrows, slab), BF),
            pltpu.VMEM((4, hrows, slab), BF),
            pltpu.VMEM((4, hrows, slab), BF),
            pltpu.VMEM((4, hrows, slab), BF),
            pltpu.VMEM((4, 8, slab), F32),
            pltpu.VMEM((8, slab), F32),
            pltpu.VMEM((8, slab), F32),
            pltpu.VMEM((4, 8, slab), F32),
            [pltpu.VMEM(each.shape, each.dtype) for each in late],
            pltpu.SemaphoreType.DMA((len(late),)),
            pltpu.SemaphoreType.DMA((64,)),
            pltpu.SemaphoreType.DMA((64,)),
            pltpu.SemaphoreType.DMA((2,)),
        ],
        compiler_params=pltpu.CompilerParams(
            collective_id=5, has_side_effects=True, vmem_limit_bytes=67_043_328
        ),
        cost_estimate=pl.CostEstimate(
            flops=2 * length * slab * qcols, bytes_accessed=300_000_000, transcendentals=0
        ),
        name="attention_backward",
    )(dn, cot, state, gains_all, probs, q_rot, kv, cos, sin, w_o, normed, att, normed_all, shard_gate, d_up, part, tok, w_q, w_kv)


STRIP = 128


def convert_kernel(
    gate_all,
    up_all,
    down_all,
    weights_all,
    kv_side,
    out_in,
    tok_in,
    grad_gate,
    grad_up,
    grad_down,
    grad_out,
    grad_query,
    grad_kv,
    out,
    grad_tok,
    wide_in,
    wide_out,
    tall_in,
    tall_out,
    turn_in,
    turn_out,
    kv_in,
    kv_out,
    same_out,
    same_tok,
    in_sems,
    out_sems,
):
    ti = lax.axis_index("tp")
    units, slab = gate_all.shape[1:]
    quarter = grad_query.shape[1] // 4
    loads, works, stores = [], [], []

    def job(sources, work, target_from, target):
        n = len(loads)
        slot = n % 3
        loads.append(
            [
                pltpu.make_async_copy(source, place(slot), in_sems.at[slot, m])
                for m, (source, place) in enumerate(sources)
            ]
        )
        works.append(lambda: work(slot))
        stores.append(pltpu.make_async_copy(target_from(slot), target, out_sems.at[slot]))

    def strips(source, target):
        for p in range(slab // STRIP):
            rows = pl.ds(p * STRIP, STRIP)

            def work(slot):
                block = wide_in[slot].reshape(4 * units, STRIP)
                for j in range(6):
                    at = slice(j * 4 * units // 6, (j + 1) * 4 * units // 6)
                    wide_out[slot, :, at] = block[at].T.astype(F32)

            job(
                [(source.at[:, :, rows], lambda slot: wide_in.at[slot])],
                work,
                lambda slot: wide_out.at[slot],
                target.at[rows, :],
            )

    def tall_work(slot):
        tall_out[slot] = tall_in[slot].astype(F32)

    def low_work(slot):
        tall_out[slot, 0:quarter] = tall_in[slot, 0:quarter].astype(F32)

    strips(gate_all, grad_gate)
    strips(up_all, grad_up)
    high = tall_in.shape[1]
    for p in range(4 * units // high):
        rows = pl.ds(p * high, high)
        job(
            [(down_all.at[rows, :], lambda slot: tall_in.at[slot])],
            tall_work,
            lambda slot: tall_out.at[slot],
            grad_down.at[rows, :],
        )
    for j in range(4):
        part = pl.ds(0, quarter)
        job(
            [(weights_all.at[j, part, :], lambda slot: tall_in.at[slot, part, :])],
            low_work,
            lambda slot: tall_out.at[slot, part, :],
            grad_out.at[pl.ds(j * quarter, quarter), :],
        )
    early = [
        pltpu.make_async_copy(
            weights_all.at[j, pl.ds(quarter, quarter), :],
            turn_in.at[pl.ds(j * quarter, quarter), :],
            in_sems.at[3, j],
        )
        for j in range(4)
    ] + [
        pltpu.make_async_copy(
            weights_all.at[:, pl.ds(2 * quarter, HD // 4), :], kv_in.at[0], in_sems.at[4, 0]
        ),
        pltpu.make_async_copy(kv_side, kv_in.at[1], in_sems.at[4, 1]),
    ]
    same = [
        pltpu.make_async_copy(out_in, same_out, in_sems.at[4, 2]),
        pltpu.make_async_copy(tok_in, same_tok, in_sems.at[4, 3]),
    ]
    for copy in loads[0] + loads[1] + early + same:
        copy.start()
    for n in range(len(loads)):
        if n + 2 < len(loads):
            for copy in loads[n + 2]:
                copy.start()
        for copy in loads[n]:
            copy.wait()
        if n >= 3:
            stores[n - 3].wait()
        works[n]()
        stores[n].start()
    late = []
    for n, (copy, source, target) in enumerate(
        ((same[0], same_out, out), (same[1], same_tok, grad_tok))
    ):
        copy.wait()
        late.append(pltpu.make_async_copy(source, target, out_sems.at[3 + n]))
        late[-1].start()
    for copy in early:
        copy.wait()
    for i in range(4 * quarter // 256):
        turn_out[:, i * 256 : (i + 1) * 256] = turn_in[i * 256 : (i + 1) * 256, :].T.astype(F32)
    late.append(pltpu.make_async_copy(turn_out, grad_query, out_sems.at[5]))
    late[-1].start()
    for n, place in ((0, ti), (1, 1 - ti)):
        at = pl.ds(pl.multiple_of(place * HD, HD), HD)
        kv_out[:, at] = kv_in[n].reshape(HD, slab).T.astype(F32)
    late.append(pltpu.make_async_copy(kv_out, grad_kv, out_sems.at[6]))
    late[-1].start()
    for copy in stores[-3:] + late:
        copy.wait()


def call_convert(gate_all, up_all, down_all, weights_all, kv_side, out, grad_tok):
    units, slab = gate_all.shape[1:]
    quarter = (weights_all.shape[1] - HD // 4) // 2
    shape = jax.ShapeDtypeStruct
    hbm = pl.BlockSpec(memory_space=pl.ANY)
    return pl.pallas_call(
        convert_kernel,
        out_shape=[
            shape((slab, 4 * units), F32),
            shape((slab, 4 * units), F32),
            shape((4 * units, slab), F32),
            shape((4 * quarter, slab), F32),
            shape((slab, 4 * quarter), F32),
            shape((slab, 2 * HD), F32),
            shape(out.shape, out.dtype),
            shape(grad_tok.shape, grad_tok.dtype),
        ],
        in_specs=[hbm] * 7,
        out_specs=[hbm] * 8,
        scratch_shapes=[
            pltpu.VMEM((3, 4, units, STRIP), BF),
            pltpu.VMEM((3, STRIP, 4 * units), F32),
            pltpu.VMEM((3, units, slab), BF),
            pltpu.VMEM((3, units, slab), F32),
            pltpu.VMEM((4 * quarter, slab), BF),
            pltpu.VMEM((slab, 4 * quarter), F32),
            pltpu.VMEM((2, 4, HD // 4, slab), BF),
            pltpu.VMEM((slab, 2 * HD), F32),
            pltpu.VMEM(out.shape, out.dtype),
            pltpu.VMEM(grad_tok.shape, grad_tok.dtype),
            pltpu.SemaphoreType.DMA((5, 4)),
            pltpu.SemaphoreType.DMA((7,)),
        ],
        compiler_params=pltpu.CompilerParams(vmem_limit_bytes=67_043_328),
        cost_estimate=pl.CostEstimate(
            flops=0, bytes_accessed=20 * slab * 4 * units, transcendentals=0
        ),
        name="convert",
    )(gate_all, up_all, down_all, weights_all, kv_side, out, grad_tok)


def fast_device(
    tokens,
    segment_ids,
    w_query,
    w_keyval,
    w_out,
    w_gate,
    w_up,
    w_down,
    gain_attn,
    gain_ffn,
    cotangent,
):
    tok, cot = tokens[0], cotangent[0]
    rows, depth = tok.shape
    hrows, slab = rows // 2, depth // 4
    length = segment_ids.shape[1]
    heads = w_query.shape[1] // HD
    units = w_gate.shape[1] // 4

    freqs = 10000.0 ** (-(jnp.arange(HD // 4, dtype=F32) * 2.0 / (HD // 2)))
    freqs = jnp.concatenate([freqs, freqs])[None]

    (
        q_rot,
        kv,
        probs,
        state,
        gains_all,
        normed_all,
        cot_all,
        gate_full,
        up_full,
        normed_slab,
        att_plane,
        gate,
        upward,
        hidden,
        shard_down,
        cos,
        sin,
    ) = call_forward(
        heads,
        tok,
        cot,
        segment_ids,
        freqs,
        gain_attn[None],
        gain_ffn[None],
        w_query,
        w_keyval,
        w_out,
        w_gate,
        w_up,
    )
    normed_all = normed_all.reshape(length, depth)
    cot_all = cot_all.reshape(length, depth)
    d_up, dn, part, shard_gate, down_all = call_middle(
        w_down, shard_down, cot_all, normed_all, gate, upward, hidden, gate_full, up_full
    )
    dn = dn.reshape(4, 2, hrows, depth)
    part = part.reshape(4, 2, hrows, depth)
    out, grad_tok, gain_grads, gate_all, up_all, weight_grads, kv_side = call_backward(
        heads,
        dn,
        cot,
        state,
        gains_all,
        probs,
        q_rot,
        kv,
        cos,
        sin,
        w_out,
        normed_slab,
        att_plane,
        normed_all,
        shard_gate,
        d_up,
        part,
        tok,
        w_query,
        w_keyval,
    )
    (
        grad_gate,
        grad_up,
        grad_down,
        grad_out,
        grad_query,
        grad_kv,
        out,
        grad_tok,
    ) = call_convert(
        gate_all,
        up_all,
        down_all.reshape(4 * units, slab),
        weight_grads,
        kv_side,
        out,
        grad_tok,
    )

    return (
        out.reshape(1, rows, depth),
        grad_tok.reshape(1, rows, depth),
        grad_query,
        grad_kv,
        grad_out,
        grad_gate,
        grad_up,
        grad_down,
        gain_grads[0],
        gain_grads[1],
    )


def solution(mesh):
    sizes = (mesh.shape["fsdp"], mesh.shape["ctx"], mesh.shape["tp"])
    in_specs = (
        P("fsdp", "ctx", None),
        P("fsdp", None),
        P("fsdp", "tp"),
        P("fsdp", None),
        P("tp", "fsdp"),
        P("fsdp", "tp"),
        P("fsdp", "tp"),
        P("tp", "fsdp"),
        P("fsdp"),
        P("fsdp"),
        P("fsdp", "ctx", None),
    )
    out_specs = (
        P("fsdp", "ctx", None),
        P("fsdp", "ctx", None),
        P("fsdp", "tp"),
        P("fsdp", None),
        P("tp", "fsdp"),
        P("fsdp", "tp"),
        P("fsdp", "tp"),
        P("tp", "fsdp"),
        P("fsdp"),
        P("fsdp"),
    )

    def body(*args):
        rows, depth = args[0].shape[1:]
        fits = sizes == (4, 4, 2) and depth % 512 == 0 and rows == 128
        if fits:
            return fast_device(*args)
        return per_device(sizes, *args)

    return jax.shard_map(
        body, mesh=mesh, in_specs=in_specs, out_specs=out_specs, check_vma=False
    )
```
